32 devices in a mesh: gz: 32 (over z, y, x, core).
Axes of the slice: x: 2, y: 2, z: 4, core: 2. Of those that a mesh axis runs over, the one named last changes fastest.
Arguments:
- density: float32 [2, 32, 256, 256], P(None, 'gz'), may hold values from 0.02 to 0.8
- kernel_hat: float32 [64, 512, 512], P(None, 'gz'), may hold values from 0.37 to 7, as said below
Outputs:
- potential: float32 [2, 32, 256, 256], P(None, 'gz')
- energies: float32 [2], replicated
The draws below stay inside these ranges and needn't reach their ends.
Inputs may be any that keep to these rules, and one draw needn't show every extreme that they name: kernel_hat at (a, b, c) equals kernel_hat at ((-a) mod 64, (-b) mod 512, (-c) mod 512).
All inputs are finite; a program needn't handle non-finite values.
Results may differ from the reference program's by a relative error of at most 0.00015.
Values sent between devices are 32-bit elements; how exact they have to be, the bound alone decides.
A program may use at most 64 MiB of HBM per device.

```python
import math
import jax
import jax.numpy as jnp
from jax import lax

NX = 256
NY = 256
NZ = 32
MX = 512
MY = 512
MZ = 64


SCREEN = 0.01


STRENGTH = 0.02


CONTACT = 1.5


def draw_density(key, part):
    height = jnp.arange(NZ, dtype=jnp.float32)[None, :, None, None] / max(NZ - 1, 1)
    uniform_draw = jax.random.uniform(key, (2, NZ, NY, NX), jnp.float32)
    ramp_values = 0.1 * jnp.exp(math.log(4.5) * height)
    return ramp_values * 0.3 * jnp.exp(math.log(5.0) * uniform_draw)


def symbol(length_cells):
    indices = jnp.arange(length_cells, dtype=jnp.int32)
    folded = jnp.minimum(indices, length_cells - indices).astype(jnp.float32)
    return (2.0 * jnp.sin(math.pi * folded / length_cells)) ** 2


def draw_kernel_hat(key, part):
    laplace = symbol(MZ)[:, None, None] + symbol(MY)[None, :, None] + symbol(MX)[None, None, :]
    uniform_draw = jax.random.uniform(key, (MZ, MY, MX), jnp.float32)
    roughness = jnp.exp(math.log(0.5) + math.log(4.0) * uniform_draw)
    mirrored = roughness
    for direction in range(3):
        mirrored = jnp.roll(jnp.flip(mirrored, direction), 1, direction)
    return (STRENGTH / (laplace + SCREEN) + CONTACT) * (0.5 * (roughness + mirrored))


def setup_inputs(seed: int = 0) -> dict:
    key_list = jax.random.split(jax.random.key(seed), 3)
    density = draw_density(jax.random.fold_in(key_list[2], 71), 0)
    kernel_hat = draw_kernel_hat(jax.random.fold_in(key_list[2], 71), 0)
    return {"density": density, "kernel_hat": kernel_hat}


HGRID = 0.35
STENCIL = (0.8, -0.2, 4.0 / 105.0, -1.0 / 280.0)
KAPPA = 0.804
MU_X = 0.2195149727645171
BETA_C = 0.06672455060314922
GAMMA_C = 0.031090690869654894
FZ_CURV = 1.709921
PARAMS_UNPOL = (0.031091, 0.2137, 7.5957, 3.5876, 1.6382, 0.49294)
PARAMS_POL = (0.015545, 0.20548, 14.1189, 6.1977, 3.3662, 0.62517)
PARAMS_STIFF = (0.016887, 0.11125, 10.357, 3.6231, 0.88026, 0.49671)

def inner_slope(extended, direction):
    stencil_reach = len(STENCIL)
    length_out = extended.shape[direction] - 2 * stencil_reach
    result = 0.0
    for offset, weight in enumerate(STENCIL):
        upper_part = lax.slice_in_dim(extended, stencil_reach + offset + 1, stencil_reach + offset + 1 + length_out, axis=direction)
        lower_part = lax.slice_in_dim(extended, stencil_reach - offset - 1, stencil_reach - offset - 1 + length_out, axis=direction)
        result = result + weight * (upper_part - lower_part)
    return result / HGRID

def plane_slope(field, direction):
    stencil_reach = len(STENCIL)
    widths = [(0, 0)] * field.ndim
    widths[direction] = (stencil_reach, stencil_reach)
    return inner_slope(jnp.pad(field, widths), direction)

def pw_piece(radius, params):
    half_root = jnp.sqrt(radius)
    series = params[2] * half_root + params[3] * radius + params[4] * radius * half_root + params[5] * radius * radius
    return -2.0 * params[0] * (1.0 + params[1] * radius) * jnp.log1p(1.0 / (2.0 * params[0] * series))

def exchange_part(doubled, sigma_four):
    cube_root = jnp.cbrt(doubled)
    uniform_part = -0.75 * (3.0 / math.pi) ** (1.0 / 3.0) * cube_root
    reduced = sigma_four / (4.0 * (3.0 * math.pi ** 2) ** (2.0 / 3.0) * doubled ** 2 * cube_root ** 2)
    enhance = 1.0 + KAPPA - KAPPA / (1.0 + MU_X * reduced / KAPPA)
    return doubled * uniform_part * enhance

def energy_density(dens_up, dens_down, sigma_uu, sigma_ud, sigma_dd):
    exchange_term = 0.5 * exchange_part(2.0 * dens_up, 4.0 * sigma_uu) + 0.5 * exchange_part(2.0 * dens_down, 4.0 * sigma_dd)
    density_sum = dens_up + dens_down
    polarization = (dens_up - dens_down) / density_sum
    radius = jnp.cbrt(3.0 / (4.0 * math.pi * density_sum))
    plus_side = 1.0 + polarization
    minus_side = 1.0 - polarization
    plus_cube = jnp.cbrt(plus_side)
    minus_cube = jnp.cbrt(minus_side)
    spin_weight = (plus_side * plus_cube + minus_side * minus_cube - 2.0) / (2.0 ** (4.0 / 3.0) - 2.0)
    unpolar = pw_piece(radius, PARAMS_UNPOL)
    polarized = pw_piece(radius, PARAMS_POL)
    stiffness = pw_piece(radius, PARAMS_STIFF)
    polar_four = polarization ** 4
    local_corr = unpolar - stiffness * spin_weight * (1.0 - polar_four) / FZ_CURV + (polarized - unpolar) * spin_weight * polar_four
    phi_factor = 0.5 * (plus_cube ** 2 + minus_cube ** 2)
    phi_cubed = phi_factor ** 3
    screening_sq = 4.0 * jnp.cbrt(3.0 * math.pi ** 2 * density_sum) / math.pi
    sigma_total = sigma_uu + 2.0 * sigma_ud + sigma_dd
    scaled_sq = sigma_total / (4.0 * phi_factor ** 2 * screening_sq * density_sum ** 2)
    weight_a = BETA_C / GAMMA_C / jnp.expm1(-local_corr / (GAMMA_C * phi_cubed))
    gradient_term = GAMMA_C * phi_cubed * jnp.log1p(BETA_C / GAMMA_C * scaled_sq * (1.0 + weight_a * scaled_sq) / (1.0 + weight_a * scaled_sq + weight_a ** 2 * scaled_sq ** 2))
    return exchange_term + density_sum * (local_corr + gradient_term)

def flux_pair(deriv_uu, deriv_ud, deriv_dd, gradient):
    return jnp.stack([2.0 * deriv_uu * gradient[0] + deriv_ud * gradient[1], 2.0 * deriv_dd * gradient[1] + deriv_ud * gradient[0]])

def xc_fields(dens, grad_z, grad_y, grad_x):
    sigma_uu = grad_z[0] * grad_z[0] + grad_y[0] * grad_y[0] + grad_x[0] * grad_x[0]
    sigma_ud = grad_z[0] * grad_z[1] + grad_y[0] * grad_y[1] + grad_x[0] * grad_x[1]
    sigma_dd = grad_z[1] * grad_z[1] + grad_y[1] * grad_y[1] + grad_x[1] * grad_x[1]
    energy, pullback = jax.vjp(energy_density, dens[0], dens[1], sigma_uu, sigma_ud, sigma_dd)
    d_up, d_down, d_uu, d_ud, d_dd = pullback(jnp.ones_like(energy))
    return (energy, jnp.stack([d_up, d_down]), flux_pair(d_uu, d_ud, d_dd, grad_z), flux_pair(d_uu, d_ud, d_dd, grad_y), flux_pair(d_uu, d_ud, d_dd, grad_x))

def plane_terms(slices):
    density_plane, grad_z, grad_y, grad_x = slices
    return xc_fields(density_plane, grad_z, grad_y, grad_x)

def reference(density, kernel_hat):
    grad_z = plane_slope(density, 1)
    grad_y = plane_slope(density, 2)
    grad_x = plane_slope(density, 3)
    moved = tuple((jnp.moveaxis(array_item, 1, 0) for array_item in (density, grad_z, grad_y, grad_x)))
    energy, d_dens, flux_z, flux_y, flux_x = lax.map(plane_terms, moved)
    d_dens = jnp.moveaxis(d_dens, 0, 1)
    flux_z = jnp.moveaxis(flux_z, 0, 1)
    flux_y = jnp.moveaxis(flux_y, 0, 1)
    flux_x = jnp.moveaxis(flux_x, 0, 1)
    v_xc = d_dens - (plane_slope(flux_z, 1) + plane_slope(flux_y, 2) + plane_slope(flux_x, 3))
    density_sum = density[0] + density[1]
    padded = jnp.pad(density_sum, ((0, NZ), (0, NY), (0, NX)))
    spectrum = jnp.fft.rfftn(padded)
    filtered = jnp.fft.irfftn(spectrum * kernel_hat[:, :, :NX + 1], s=padded.shape)
    hartree = filtered[:NZ, :NY, :NX]
    potential = v_xc + hartree[None]
    energies = jnp.stack([jnp.mean(energy), 0.5 * jnp.mean(density_sum * hartree)])
    return (potential, energies)
```

```python
import functools
import math

import jax
import jax.numpy as jnp
import numpy as np
from jax import lax
from jax.experimental import pallas as pl
from jax.experimental.pallas import tpu as pltpu
from jax.sharding import PartitionSpec as P

HGRID = 0.35
STENCIL_WHOLE = (672.0, -168.0, 32.0, -3.0)
STENCIL_SCALE = 1.0 / (840.0 * HGRID)
REACH = len(STENCIL_WHOLE)
KAPPA = 0.804
MU_X = 0.2195149727645171
BETA_C = 0.06672455060314922
GAMMA_C = 0.031090690869654894
FZ_CURV = 1.709921
PARAMS_UNPOL = (0.031091, 0.2137, 7.5957, 3.5876, 1.6382, 0.49294)
PARAMS_POL = (0.015545, 0.20548, 14.1189, 6.1977, 3.3662, 0.62517)
PARAMS_STIFF = (0.016887, 0.11125, 10.357, 3.6231, 0.88026, 0.49671)

MESH = pl.DeviceIdType.MESH
LANES = 128
SUBLANES = 8
VMEM_SPEC = pl.BlockSpec(memory_space=pltpu.VMEM)
ANY_SPEC = pl.BlockSpec(memory_space=pl.ANY)
VMEM_BYTES = 60 * 1024 * 1024


def exchange_spin(dens, log_dens, sigma):
    factor = -0.75 * (3.0 / math.pi) ** (1.0 / 3.0) * 2.0 ** (1.0 / 3.0)
    scale = (3.0 * math.pi**2) ** (2.0 / 3.0) * 2.0 ** (8.0 / 3.0)
    inverse_cube = jnp.exp(log_dens * (-1.0 / 3.0))
    cube = dens * inverse_cube * inverse_cube
    product = dens * cube
    weight = product * product
    bent = (MU_X / (KAPPA * scale)) * sigma
    inverse = 1.0 / (weight + bent)
    share = weight * inverse
    rest = KAPPA * bent * inverse
    enhance = 1.0 + rest
    energy = factor * product * enhance
    by_dens = factor * cube * ((4.0 / 3.0) * enhance - (8.0 / 3.0) * rest * share)
    square = dens * dens * inverse
    by_sigma = (factor * MU_X / scale) * square * square
    return energy, by_dens, by_sigma, cube, inverse_cube


def pw_piece(root, square, params):
    amp, alpha, b1, b2, b3, b4 = params
    doubled = 2.0 * amp
    series = root * (doubled * b1 + root * (doubled * b2 + root * (doubled * b3 + root * (doubled * b4))))
    slope = doubled * b1 + root * (
        2.0 * doubled * b2 + root * (3.0 * doubled * b3 + root * (4.0 * doubled * b4))
    )
    above = series + 1.0
    inverse = 1.0 / (series * above)
    logarithm = jnp.log(above * above * inverse)
    front = -doubled - (doubled * alpha) * square
    value = front * logarithm
    by_root = (-2.0 * doubled * alpha) * root * logarithm - front * slope * inverse
    return value, by_root


def xc_point(up, down, sigma_uu, sigma_ud, sigma_dd):
    energy_u, vx_u, by_uu, cube_u, inverse_u = exchange_spin(up, jnp.log(up), sigma_uu)
    energy_d, vx_d, by_dd, cube_d, inverse_d = exchange_spin(down, jnp.log(down), sigma_dd)
    total = up + down
    sixth = jnp.exp(jnp.log(total) * (-1.0 / 6.0))
    inverse_cube = sixth * sixth
    wigner = (3.0 / (4.0 * math.pi)) ** (1.0 / 3.0)
    root = math.sqrt(wigner) * sixth
    square = wigner * inverse_cube
    inverse_square = inverse_cube * inverse_cube
    inverse_total = inverse_square * inverse_cube
    cube = total * inverse_square
    zeta = (up - down) * inverse_total
    plus = 1.0 + zeta
    minus = 1.0 - zeta
    third = 2.0 ** (1.0 / 3.0)
    plus_cube = third * cube_u * inverse_cube
    minus_cube = third * cube_d * inverse_cube
    spin = 1.0 / (2.0 ** (4.0 / 3.0) - 2.0)
    weight = (plus * plus_cube + minus * minus_cube - 2.0) * spin
    by_weight = (4.0 / 3.0 * spin) * (plus_cube - minus_cube)
    unpol, unpol_root = pw_piece(root, square, PARAMS_UNPOL)
    pol, pol_root = pw_piece(root, square, PARAMS_POL)
    stiff, stiff_root = pw_piece(root, square, PARAMS_STIFF)
    stiff = stiff * (-1.0 / FZ_CURV)
    stiff_root = stiff_root * (-1.0 / FZ_CURV)
    zeta_two = zeta * zeta
    zeta_four = zeta_two * zeta_two
    gap = pol - unpol - stiff
    mixed = stiff + gap * zeta_four
    mixed_root = stiff_root + (pol_root - unpol_root - stiff_root) * zeta_four
    local = unpol + weight * mixed
    local_root = unpol_root + weight * mixed_root
    local_zeta = by_weight * mixed + weight * gap * (4.0 * zeta_two * zeta)
    phi = 0.5 * (plus_cube * plus_cube + minus_cube * minus_cube)
    by_phi = (2.0 ** (-1.0 / 3.0) / 3.0) * cube * (inverse_u - inverse_d)
    inverse_phi = 1.0 / phi
    phi_square = inverse_phi * inverse_phi
    inverse_gamma = phi_square * inverse_phi * (1.0 / GAMMA_C)
    gamma_phi = GAMMA_C * phi * phi * phi
    ratio = BETA_C / GAMMA_C
    expo = -local * inverse_gamma
    weight_a = ratio / (jnp.exp(expo) - 1.0)
    scale = math.pi / (16.0 * (3.0 * math.pi**2) ** (1.0 / 3.0))
    to_t = scale * phi_square * (inverse_square * inverse_cube) * (inverse_square * inverse_square)
    sigma = sigma_uu + 2.0 * sigma_ud + sigma_dd
    tee = sigma * to_t
    why = weight_a * tee
    numer = 1.0 + why
    denom = 1.0 + why * numer
    scaled = ratio * tee
    upper = denom + scaled * numer
    inverse = 1.0 / (denom * upper)
    gradient = gamma_phi * jnp.log(upper * upper * inverse)
    shared = gamma_phi * inverse
    by_tee = ratio * shared * (numer + why)
    by_a = shared * scaled * tee * why * (numer + 1.0)
    chain = by_a * weight_a * (1.0 + weight_a * (1.0 / ratio))
    by_local = 1.0 - chain * inverse_gamma
    tee_part = tee * by_tee
    phi_part = (3.0 * gradient - 3.0 * expo * chain - 2.0 * tee_part) * inverse_phi
    corr = local + gradient
    by_total = corr - (1.0 / 6.0) * root * local_root * by_local - (7.0 / 3.0) * tee_part
    by_zeta = by_local * local_zeta + phi_part * by_phi
    by_sigma = total * by_tee * to_t
    energy = energy_u + energy_d + total * corr
    return (
        energy,
        vx_u + by_total + by_zeta * minus,
        vx_d + by_total - by_zeta * plus,
        by_uu + by_sigma,
        2.0 * by_sigma,
        by_dd + by_sigma,
    )


def np_split(table):
    table = np.asarray(table, np.float32)
    high = table.astype(jnp.bfloat16)
    low = (table - high.astype(np.float32)).astype(jnp.bfloat16)
    return high, low


def y_tables(width_y, devices, scale):
    period = 2 * width_y
    count = period // devices
    half = count // 2
    slots = max(half, SUBLANES)
    device = np.arange(devices)[:, None]
    ky = device * count + np.arange(half)[None, :] + (device >= devices // 2)
    space = np.arange(width_y)
    angle = (ky[:, :, None] * space % period) * (2.0 * np.pi / period)
    both = np.stack([np.cos(angle), -np.sin(angle)], axis=1)
    both[0, 1, 0] = (-1.0) ** space
    weight = np.full((devices, 2, half, 1), 2.0)
    weight[0, :, 0] = 1.0
    pad = [(0, 0), (0, 0), (0, slots - half), (0, 0)]
    forward = np.pad(both, pad).reshape(devices * 2 * slots, width_y)
    back = np.pad(both * weight, pad).reshape(devices * 2 * slots, width_y)
    return *np_split(forward), *np_split(back.T * scale)


def x_tables(width_x):
    index = np.outer(np.arange(width_x), np.arange(width_x)) % (2 * width_x)
    angle = index * (np.pi / width_x)
    cos, sin = np.cos(angle), np.sin(angle)
    sin[:, 0] = (-1.0) ** np.arange(width_x)
    fore = np.concatenate([cos, sin], axis=1)
    back = np.concatenate([cos, sin.T], axis=0)
    return *np_split(fore), *np_split(back)


def stencil_matrix(size):
    table = np.zeros((size, size + 2 * REACH), np.float32)
    for row in range(size):
        for step, weight in enumerate(STENCIL_WHOLE, 1):
            table[row, row + REACH + step] = weight
            table[row, row + REACH - step] = -weight
    return table


def slope_tables(width_x, rows):
    wide = stencil_matrix(width_x)[:, REACH : REACH + width_x].T
    table = stencil_matrix(rows)
    inner = table[:, REACH : REACH + rows]
    below, above = table[:, :REACH], table[:, REACH + rows :]
    pad = np.zeros((rows, -(rows + 2 * REACH) % 16), np.float32)
    tall = np.concatenate([inner, above, below, pad], axis=1)
    tall = np.concatenate([tall] * 3, axis=1)
    return wide.astype(jnp.bfloat16), tall.astype(jnp.bfloat16)


def turn_table(width_x):
    table = np.zeros((width_x, width_x), np.float32)
    lanes = np.arange(width_x)
    table[(width_x - lanes) % width_x, lanes] = 1.0
    return table.astype(jnp.bfloat16)


def dot(left, right):
    return jnp.dot(left, right, preferred_element_type=jnp.float32)


def split(value):
    high = value.astype(jnp.bfloat16)
    low = (value - high.astype(jnp.float32)).astype(jnp.bfloat16)
    return high, low


def split_three(value):
    high = value.astype(jnp.bfloat16)
    rest = value - high.astype(jnp.float32)
    middle = rest.astype(jnp.bfloat16)
    low = (rest - middle.astype(jnp.float32)).astype(jnp.bfloat16)
    return high, middle, low


def dot_exact(value, table):
    high, middle, low = split_three(value)
    return dot(high, table) + (dot(middle, table) + dot(low, table))


def add(left, right):
    if left is None or right is None:
        return left if right is None else right
    return left[0] + right[0], left[1] + right[1]


def sub(left, right):
    if right is None:
        return left
    return left[0] - right[0], left[1] - right[1]


def turn(value, numer, denom, sign):
    if value is None:
        return None
    numer = numer * sign % denom
    eighth = numer * 8
    re, im = value
    if eighth % (2 * denom) == 0:
        quarter = eighth // (2 * denom)
        return ((re, im), (-im, re), (-re, -im), (im, -re))[quarter]
    if eighth % denom == 0:
        root = math.sqrt(0.5)
        plus, minus = root * (re + im), root * (re - im)
        return {1: (minus, plus), 3: (-plus, minus), 5: (-minus, -plus), 7: (plus, -minus)}[eighth // denom]
    cos = math.cos(2.0 * math.pi * numer / denom)
    sin = math.sin(2.0 * math.pi * numer / denom)
    return cos * re - sin * im, sin * re + cos * im


def small_dft(values, sign, first_half=False):
    count = len(values)
    if count == 1:
        return values
    even = small_dft(values[0::2], sign)
    odd = small_dft(values[1::2], sign)
    odd = [turn(value, k, count, sign) for k, value in enumerate(odd)]
    out = [add(e, o) for e, o in zip(even, odd)]
    if not first_half:
        out += [sub(e, o) for e, o in zip(even, odd)]
    return out


class Copies:
    def __init__(self, sends, receives, index=None):
        self.sends, self.receives = sends, receives

    def make(self, source, target, send, receive, peer):
        return pltpu.make_async_remote_copy(
            src_ref=source,
            dst_ref=target,
            send_sem=self.sends.at[send],
            recv_sem=self.receives.at[receive],
            device_id=(peer,),
            device_id_type=MESH,
        )


def mega_kernel(
    devices,
    group,
    half,
    dens,
    ty_high,
    ty_low,
    khat_hbm,
    tb_high_hbm,
    tb_low_hbm,
    tx_high,
    tx_low,
    tr_high,
    tr_low,
    t_wide,
    t_tall,
    t_turn,
    out,
    e_out,
    khat,
    tb_high,
    tb_low,
    spec_out,
    spec_in,
    halo_out,
    halo_in,
    main,
    grad_x,
    grad_y,
    grad_z,
    flux_z,
    flux_out,
    flux_in,
    v_own,
    v_all,
    edge_out,
    edge_in,
    k_raw,
    k_self,
    k_cross,
    z_in,
    z_mid,
    h_spec,
    x_in,
    back_out,
    back_in,
    partial,
    sums,
    local_sems,
    spec_s,
    spec_r,
    back_s,
    back_r,
    part_s,
    part_r,
    main_s,
    main_r,
    halo_s,
    halo_r,
    fz_s,
    fz_r,
    fy_s,
    fy_r,
    v_s,
    v_r,
    edge_s,
    edge_r,
):
    me = lax.axis_index("gz")
    level, member = lax.div(me, group), lax.rem(me, group)
    levels = devices // group
    base = level * group
    width_y, width_x = dens.shape[1:]
    rows = width_y // group
    tiles = width_x // LANES
    depth = devices
    slots = spec_out.shape[1] // 2
    first_device, edge_device = 0, devices // 2
    cells = depth * width_y * width_x

    barrier = pltpu.get_barrier_semaphore()

    def greet(step, carry):
        pl.semaphore_signal(
            barrier, inc=1, device_id=(lax.rem(me + step, devices),), device_id_type=MESH
        )
        return carry

    lax.fori_loop(1, devices, greet, 0)

    locals_ = [
        pltpu.make_async_copy(source, target, local_sems.at[i])
        for i, (source, target) in enumerate(
            [(khat_hbm, khat), (tb_high_hbm, tb_high), (tb_low_hbm, tb_low)]
        )
    ]
    for copy in locals_:
        copy.start()

    def remote(source, target, send, receive, peer):
        return pltpu.make_async_remote_copy(
            src_ref=source,
            dst_ref=target,
            send_sem=send,
            recv_sem=receive,
            device_id=(peer,),
            device_id_type=MESH,
        )

    sub_row = lax.broadcasted_iota(jnp.int32, (1, SUBLANES, width_x), 1)
    for b in range(group):
        above = dens[:, (b + 1) * rows : (b + 1) * rows + SUBLANES] if b < group - 1 else 0.0
        below = dens[:, b * rows - SUBLANES : b * rows] if b else 0.0
        halo_out[b] = jnp.where(sub_row < REACH, above, below)

    total = dens[0] + dens[1]
    high, low = split(total)
    values = dot(ty_high[...], high) + (dot(ty_high[...], low) + dot(ty_low[...], high))
    spec_out[...] = values.reshape(spec_out.shape)

    pl.semaphore_wait(barrier, devices - 1)

    up = member >= group - REACH
    near = jnp.where(up, level + 1, level - 1)
    has_near = jnp.logical_and(near >= 0, near < levels)
    near_slot = jnp.where(up, member - (group - REACH), REACH + group + member)

    def block(b):
        return pl.ds(pl.multiple_of(b * rows, rows), rows)

    def main_copy(b, peer, slot, which):
        return remote(
            dens.at[:, block(b)], main.at[:, slot], main_s.at[which, b], main_r.at[slot], peer
        )

    def halo_copy(b, peer, source):
        return remote(
            halo_out.at[b], halo_in.at[source], halo_s.at[b], halo_r.at[source], peer
        )

    def in_group(act):
        def body(step, carry):
            b = lax.rem(member + step, group)
            act(b, base + b)
            return carry

        lax.fori_loop(1, group, body, 0)

    def start_main(b, peer):
        main_copy(b, peer, REACH + member, 0).start()
        halo_copy(b, peer, member).start()

    in_group(start_main)

    def near_each(act):
        @pl.when(has_near)
        def _():
            def body(step, carry):
                b = lax.rem(member + step, group)
                act(main_copy(b, near * group + b, near_slot, 1))
                return carry

            lax.fori_loop(0, group, body, 0)

    near_each(lambda copy: copy.start())

    def spec_copy(step, peer, slot):
        return remote(
            spec_out.at[peer], spec_in.at[slot], spec_s.at[step], spec_r.at[step], peer
        )

    def around(act):
        def body(step, carry):
            act(step, lax.rem(me + step, devices), lax.rem(me - step + devices, devices))
            return carry

        lax.fori_loop(1, devices, body, 0)

    around(lambda step, peer, origin: spec_copy(step, peer, me).start())
    main[:, REACH + member] = dens[:, block(member)]
    halo_in[member] = halo_out[member]
    spec_in[me] = spec_out[me]

    zero_planes = jnp.zeros((2, REACH, rows, width_x), jnp.float32)

    @pl.when(level == 0)
    def _():
        main[:, :REACH] = zero_planes
        flux_z[:, :REACH] = zero_planes

    @pl.when(level == levels - 1)
    def _():
        main[:, REACH + group :] = zero_planes
        flux_z[:, REACH + group :] = zero_planes

    locals_[0].wait()

    @pl.when(me == edge_device)
    def _():
        edge_out[...] = khat[:, 0, :]
        remote(edge_out, edge_in, edge_s, edge_r, first_device).start()

    lower = me < edge_device
    planes_k = khat.shape[0]
    if slots > half:
        k_raw[...] = jnp.ones(k_raw.shape, jnp.float32)

    def pick(kz, carry):
        row = jnp.where(lower, khat[kz, :half], khat[kz, 1 : half + 1])
        for t in range(tiles):
            k_self[kz, t, :half] = row[:, t * LANES : (t + 1) * LANES]
        k_raw[kz, :half] = row[:, width_x:]
        if slots > half:
            for t in range(tiles):
                k_self[kz, t, half:] = jnp.ones((slots - half, LANES), jnp.float32)
        return carry

    lax.fori_loop(0, planes_k, pick, 0)
    turned = dot_exact(k_raw[...].reshape(planes_k * slots, width_x), t_turn[...])
    turned = turned.reshape(planes_k, slots, width_x)
    for t in range(tiles):
        k_self[:, tiles + t] = turned[:, :, t * LANES : (t + 1) * LANES]

    def clear(kz, carry):
        k_cross[kz] = jnp.zeros(k_cross.shape[1:], jnp.float32)
        return carry

    lax.fori_loop(0, planes_k, clear, 0)

    @pl.when(me == first_device)
    def _():
        remote(edge_out, edge_in, edge_s, edge_r, edge_device).wait_recv()
        edge_out[:, :width_x] = edge_in[:, :width_x]
        edge_out[:, width_x:] = dot_exact(edge_in[:, width_x:], t_turn[...])
        top = lax.broadcasted_iota(jnp.int32, (slots, LANES), 0) == 0

        def mix(kz, carry):
            other = edge_out[pl.ds(kz, 1), :]
            for t in range(2 * tiles):
                mine = k_self[kz, t]
                theirs = other[:, t * LANES : (t + 1) * LANES]
                k_self[kz, t] = jnp.where(top, 0.5 * (mine + theirs), mine)
                k_cross[kz, t] = jnp.where(top, 0.5 * (mine - theirs), 0.0)
            return carry

        lax.fori_loop(0, planes_k, mix, 0)

    def finish_main(b, peer):
        main_copy(b, peer, REACH + b, 0).wait_recv()
        halo_copy(b, peer, b).wait_recv()

    in_group(finish_main)

    def near_wait(first):
        def body(step, carry):
            main_copy(member, me, first + step, 1).wait_recv()
            return carry

        lax.fori_loop(0, REACH, body, 0)

    @pl.when(level > 0)
    def _():
        near_wait(0)

    @pl.when(level < levels - 1)
    def _():
        near_wait(REACH + group)

    def slope_z(field, spin, plane):
        result = 0.0
        for step, weight in enumerate(STENCIL_WHOLE, 1):
            result = result + (weight * STENCIL_SCALE) * (
                field[spin, plane + REACH + step] - field[spin, plane + REACH - step]
            )
        return result

    pad_rows = t_tall.shape[1] // 3 - rows - SUBLANES

    def slope_y(inner, outer):
        parts = [inner, outer]
        if pad_rows:
            parts.append(jnp.zeros((pad_rows, width_x), jnp.float32))
        stacked = jnp.concatenate(split_three(jnp.concatenate(parts, axis=0)), axis=0)
        return dot(t_tall[...], stacked) * STENCIL_SCALE

    def slope_x(field):
        value = field.reshape(group * rows, width_x)
        return (dot_exact(value, t_wide[...]) * STENCIL_SCALE).reshape(group, rows, width_x)

    for spin in range(2):
        grad_x[spin] = slope_x(main[spin, REACH : REACH + group])

    def gradients(plane, carry):
        for spin in range(2):
            grad_z[spin, plane] = slope_z(main, spin, plane)
            grad_y[spin, plane] = slope_y(main[spin, REACH + plane], halo_in[plane, spin])
        return carry

    lax.fori_loop(0, group, gradients, 0)

    chunk = SUBLANES

    def point(index, acc):
        plane = lax.div(index, rows // chunk)
        at = pl.ds(pl.multiple_of(lax.rem(index, rows // chunk) * chunk, chunk), chunk)
        uz, uy, ux = grad_z[0, plane, at], grad_y[0, plane, at], grad_x[0, plane, at]
        dz, dy, dx = grad_z[1, plane, at], grad_y[1, plane, at], grad_x[1, plane, at]
        energy, d_up, d_down, d_uu, d_ud, d_dd = xc_point(
            main[0, REACH + plane, at],
            main[1, REACH + plane, at],
            uz * uz + uy * uy + ux * ux,
            uz * dz + uy * dy + ux * dx,
            dz * dz + dy * dy + dx * dx,
        )
        v_own[0, plane, at] = d_up
        v_own[1, plane, at] = d_down
        d_uu = 2.0 * d_uu
        d_dd = 2.0 * d_dd
        flux_z[0, REACH + plane, at] = d_uu * uz + d_ud * dz
        flux_z[1, REACH + plane, at] = d_dd * dz + d_ud * uz
        grad_y[0, plane, at] = d_uu * uy + d_ud * dy
        grad_y[1, plane, at] = d_dd * dy + d_ud * uy
        grad_x[0, plane, at] = d_uu * ux + d_ud * dx
        grad_x[1, plane, at] = d_dd * dx + d_ud * ux
        return acc + energy

    energy_acc = lax.fori_loop(
        0, group * rows // chunk, point, jnp.zeros((chunk, width_x), jnp.float32)
    )
    energy_xc = jnp.sum(energy_acc) * (1.0 / cells)

    def flux_z_copy(side, peer):
        source = (slice(group, group + REACH), slice(REACH, 2 * REACH))[side]
        target = (slice(0, REACH), slice(REACH + group, 2 * REACH + group))[side]
        return remote(
            flux_z.at[:, source], flux_z.at[:, target], fz_s.at[side], fz_r.at[side], peer
        )

    def flux_y_copy(side, peer):
        return remote(flux_out, flux_in.at[side], fy_s.at[side], fy_r.at[side], peer)

    exists_up, exists_down = level < levels - 1, level > 0
    right, left = member < group - 1, member > 0

    @pl.when(exists_up)
    def _():
        flux_z_copy(0, me + group).start()

    @pl.when(exists_down)
    def _():
        flux_z_copy(1, me - group).start()

    for spin in range(2):
        flux_out[:, spin] = jnp.where(
            sub_row < REACH, grad_y[spin, :, :SUBLANES], grad_y[spin, :, rows - SUBLANES :]
        )

    @pl.when(right)
    def _():
        flux_y_copy(0, me + 1).start()

    @pl.when(left)
    def _():
        flux_y_copy(1, me - 1).start()

    around(lambda step, peer, origin: spec_copy(step, peer, origin).wait_recv())
    lane = lax.broadcasted_iota(jnp.int32, (1, 1, width_x), 2)
    first = lane == 0
    high, low = split(spec_in[...].reshape(depth * 2 * slots, width_x))
    wide = dot(high, tx_high[...]) + (dot(low, tx_high[...]) + dot(high, tx_low[...]))
    wide = wide.reshape(depth, 2, slots, 2 * width_x)
    cos_re, cos_im = wide[:, 0, :, :width_x], wide[:, 1, :, :width_x]
    sin_re, sin_im = wide[:, 0, :, width_x:], wide[:, 1, :, width_x:]
    fields = (
        (jnp.where(first, cos_re, cos_re + sin_im), jnp.where(first, cos_im, cos_im - sin_re)),
        (jnp.where(first, sin_re, cos_re - sin_im), jnp.where(first, sin_im, cos_im + sin_re)),
    )
    for sign in range(2):
        for part in range(2):
            for t in range(tiles):
                z_in[:, part, sign * tiles + t] = fields[sign][part][
                    :, :, t * LANES : (t + 1) * LANES
                ]

    n1, n2 = z_mid.shape[:2]
    full = n1 * n2

    def load(ref, *at):
        return ref[at[0], 0, at[1]], ref[at[0], 1, at[1]]

    def fore(col, carry):
        for j in range(n2):
            given = [load(z_in, n2 * i + j, col) for i in range(n1 // 2)]
            for k, value in enumerate(small_dft(given + [None] * (n1 // 2), -1)):
                re, im = turn(value, k * j, full, -1)
                z_mid[k, j, 0] = re
                z_mid[k, j, 1] = im
        for k in range(n1):
            given = [(z_mid[k, j, 0], z_mid[k, j, 1]) for j in range(n2)]
            for m, (re, im) in enumerate(small_dft(given, -1)):
                h_spec[k + n1 * m, 0, col] = re
                h_spec[k + n1 * m, 1, col] = im
        return carry

    lax.fori_loop(0, 2 * tiles, fore, 0)
    lane = lax.broadcasted_iota(jnp.int32, (slots, LANES), 1)

    def back(col, carry):
        other = lax.rem(col + tiles, 2 * tiles)
        alone = jnp.logical_and(lane == 0, lax.rem(col, tiles) == 0)
        for k in range(n1):
            given = []
            for m in range(n2):
                kz = k + n1 * m
                flip = (full - kz) % full
                re, im = load(h_spec, kz, col)
                own_re, own_im = load(h_spec, flip, col)
                far_re, far_im = load(h_spec, flip, other)
                far_re = jnp.where(alone, own_re, far_re)
                far_im = jnp.where(alone, own_im, far_im)
                direct, cross = k_self[kz, col], k_cross[kz, col]
                given.append((direct * re + cross * far_re, direct * im - cross * far_im))
            for j, value in enumerate(small_dft(given, 1)):
                re, im = turn(value, k * j, full, 1)
                z_mid[k, j, 0] = re
                z_mid[k, j, 1] = im
        for j in range(n2):
            given = [(z_mid[k, j, 0], z_mid[k, j, 1]) for k in range(n1)]
            for i, (re, im) in enumerate(small_dft(given, 1, first_half=True)):
                z_in[n2 * i + j, 0, col] = re
                z_in[n2 * i + j, 1, col] = im
        return carry

    lax.fori_loop(0, 2 * tiles, back, 0)
    for t in range(tiles):
        keep = lax.broadcasted_iota(jnp.int32, (1, 1, LANES), 2) + t * LANES == 0
        plus_re, plus_im = z_in[:, 0, t], z_in[:, 1, t]
        minus_re, minus_im = z_in[:, 0, tiles + t], z_in[:, 1, tiles + t]
        here = slice(t * LANES, (t + 1) * LANES)
        there = slice(width_x + t * LANES, width_x + (t + 1) * LANES)
        x_in[:, 0, :, here] = jnp.where(keep, plus_re, plus_re + minus_re)
        x_in[:, 1, :, here] = jnp.where(keep, plus_im, plus_im + minus_im)
        x_in[:, 0, :, there] = jnp.where(keep, minus_re, minus_im - plus_im)
        x_in[:, 1, :, there] = jnp.where(keep, minus_im, plus_re - minus_re)
    high, low = split(x_in[...].reshape(depth * 2 * slots, 2 * width_x))
    values = dot(high, tr_high[...]) + (dot(low, tr_high[...]) + dot(high, tr_low[...]))
    back_out[...] = values.reshape(back_out.shape)

    def back_copy(step, peer, slot):
        return remote(
            back_out.at[peer], back_in.at[slot], back_s.at[step], back_r.at[step], peer
        )

    around(lambda step, peer, origin: back_copy(step, peer, me).start())
    back_in[me] = back_out[me]

    acc = jnp.sum(spec_in[...] * back_out[...], axis=0)
    row = lax.broadcasted_iota(jnp.int32, acc.shape, 0)
    single = jnp.logical_and(me == first_device, lax.rem(row, slots) == 0)
    energy_h = jnp.sum(jnp.where(single, acc, 2.0 * acc)) * (0.5 / (8.0 * cells) / cells)
    row = lax.broadcasted_iota(jnp.int32, partial.shape, 0)
    partial[...] = jnp.where(row == 0, energy_xc, energy_h)

    def part_copy(step, peer, slot):
        return remote(partial, sums.at[slot], part_s.at[step], part_r.at[step], peer)

    around(lambda step, peer, origin: part_copy(step, peer, me).start())
    sums[me] = partial[...]

    @pl.when(exists_down)
    def _():
        flux_z_copy(0, me).wait_recv()

    @pl.when(exists_up)
    def _():
        flux_z_copy(1, me).wait_recv()

    @pl.when(left)
    def _():
        flux_y_copy(0, me).wait_recv()

    @pl.when(right)
    def _():
        flux_y_copy(1, me).wait_recv()

    @pl.when(jnp.logical_not(left))
    def _():
        flux_in[0] = jnp.zeros(flux_in.shape[1:], jnp.float32)

    @pl.when(jnp.logical_not(right))
    def _():
        flux_in[1] = jnp.zeros(flux_in.shape[1:], jnp.float32)

    for spin in range(2):
        v_own[spin] = v_own[spin] - slope_x(grad_x[spin])

    def divergence(plane, carry):
        for spin in range(2):
            outer = jnp.where(sub_row[0] < REACH, flux_in[1, plane, spin], flux_in[0, plane, spin])
            v_own[spin, plane] = v_own[spin, plane] - (
                slope_z(flux_z, spin, plane) + slope_y(grad_y[spin, plane], outer)
            )
        return carry

    lax.fori_loop(0, group, divergence, 0)

    def v_copy(b, peer, source):
        return remote(
            v_own.at[:, b], v_all.at[:, block(source)], v_s.at[b], v_r.at[source], peer
        )

    in_group(lambda b, peer: v_copy(b, peer, member).start())
    v_all[:, block(member)] = v_own[:, member]

    locals_[1].wait()
    locals_[2].wait()
    around(lambda step, peer, origin: back_copy(step, peer, origin).wait_recv())
    high, low = split(back_in[...].reshape(depth * 2 * slots, width_x))
    hartree = dot(tb_high[...], high) + (dot(tb_high[...], low) + dot(tb_low[...], high))
    in_group(lambda b, peer: v_copy(b, peer, b).wait_recv())
    out[0] = hartree + v_all[0]
    out[1] = hartree + v_all[1]
    around(lambda step, peer, origin: part_copy(step, peer, origin).wait_recv())
    e_out[...] = jnp.sum(sums[...], axis=0)

    def sent(b, peer):
        main_copy(b, peer, REACH + member, 0).wait_send()
        halo_copy(b, peer, member).wait_send()
        v_copy(b, peer, member).wait_send()

    in_group(sent)
    near_each(lambda copy: copy.wait_send())

    def sent_around(step, peer, origin):
        spec_copy(step, peer, me).wait_send()
        back_copy(step, peer, me).wait_send()
        part_copy(step, peer, me).wait_send()

    around(sent_around)

    @pl.when(exists_up)
    def _():
        flux_z_copy(0, me + group).wait_send()

    @pl.when(exists_down)
    def _():
        flux_z_copy(1, me - group).wait_send()

    @pl.when(right)
    def _():
        flux_y_copy(0, me + 1).wait_send()

    @pl.when(left)
    def _():
        flux_y_copy(1, me - 1).wait_send()

    @pl.when(me == edge_device)
    def _():
        remote(edge_out, edge_in, edge_s, edge_r, first_device).wait_send()


def per_device(density, kernel_hat):
    planes, width_y, width_x = density.shape[1:]
    devices = lax.axis_size("gz")
    assert planes == 1
    group = 2 * REACH
    rows = width_y // group
    cells = devices * width_y * width_x
    count = kernel_hat.shape[1]
    half = count // 2
    slots = max(half, SUBLANES)
    tiles = width_x // LANES
    full = 2 * devices
    n1 = 1 << (full.bit_length() // 2)
    ty_high, ty_low, tb_high, tb_low = y_tables(width_y, devices, 1.0 / (8 * cells))
    x_parts = x_tables(width_x)
    t_wide, t_tall = slope_tables(width_x, rows)
    spec_shape = (devices, 2 * slots, width_x)
    tile_shape = (2, group, rows, width_x)
    tall_shape = (2, group + 2 * REACH, rows, width_x)
    f32 = functools.partial(pltpu.VMEM, dtype=jnp.float32)
    dma = pltpu.SemaphoreType.DMA
    scratch = [
        f32(kernel_hat.shape),
        pltpu.VMEM(tb_high.shape, jnp.bfloat16),
        pltpu.VMEM(tb_low.shape, jnp.bfloat16),
        f32(spec_shape),
        f32(spec_shape),
        f32((group, 2, SUBLANES, width_x)),
        f32((group, 2, SUBLANES, width_x)),
        f32(tall_shape),
        f32(tile_shape),
        f32(tile_shape),
        f32(tile_shape),
        f32(tall_shape),
        f32((group, 2, SUBLANES, width_x)),
        f32((2, group, 2, SUBLANES, width_x)),
        f32(tile_shape),
        f32((2, width_y, width_x)),
        f32((full, 2 * width_x)),
        f32((full, 2 * width_x)),
        f32((full, slots, width_x)),
        f32((full, 2 * tiles, slots, LANES)),
        f32((full, 2 * tiles, slots, LANES)),
        f32((devices, 2, 2 * tiles, slots, LANES)),
        f32((n1, full // n1, 2, slots, LANES)),
        f32((full, 2, 2 * tiles, slots, LANES)),
        f32((devices, 2, slots, 2 * width_x)),
        f32(spec_shape),
        f32(spec_shape),
        f32((SUBLANES, LANES)),
        f32((devices, SUBLANES, LANES)),
        dma((3,)),
        dma((devices,)),
        dma((devices,)),
        dma((devices,)),
        dma((devices,)),
        dma((devices,)),
        dma((devices,)),
        dma((2, group)),
        dma((group + 2 * REACH,)),
        dma((group,)),
        dma((group,)),
        dma((2,)),
        dma((2,)),
        dma((2,)),
        dma((2,)),
        dma((group,)),
        dma((group,)),
        dma,
        dma,
    ]
    potential, energies = pl.pallas_call(
        functools.partial(mega_kernel, devices, group, half),
        out_shape=(
            jax.ShapeDtypeStruct((2, width_y, width_x), jnp.float32),
            jax.ShapeDtypeStruct((SUBLANES, LANES), jnp.float32),
        ),
        in_specs=[VMEM_SPEC] * 3 + [ANY_SPEC] * 3 + [VMEM_SPEC] * 7,
        out_specs=(VMEM_SPEC, VMEM_SPEC),
        scratch_shapes=scratch,
        compiler_params=pltpu.CompilerParams(
            collective_id=0, has_side_effects=True, vmem_limit_bytes=VMEM_BYTES
        ),
        name="potential",
    )(
        density.reshape(2, width_y, width_x),
        ty_high,
        ty_low,
        kernel_hat,
        tb_high,
        tb_low,
        *x_parts,
        t_wide,
        t_tall,
        turn_table(width_x),
    )
    return potential.reshape(density.shape), energies[:2, 0]


def solution(mesh):
    placed = (P(None, "gz", None, None), P(None, "gz", None))
    return jax.shard_map(
        per_device,
        mesh=mesh,
        in_specs=placed,
        out_specs=(P(None, "gz", None, None), P()),
        check_vma=False,
    )
```

```python
import functools
import math

import jax
import jax.numpy as jnp
import numpy as np
from jax import lax
from jax.experimental import pallas as pl
from jax.experimental.pallas import tpu as pltpu
from jax.sharding import PartitionSpec as P

HGRID = 0.35
STENCIL_WHOLE = (672.0, -168.0, 32.0, -3.0)
STENCIL_SCALE = 1.0 / (840.0 * HGRID)
REACH = len(STENCIL_WHOLE)
KAPPA = 0.804
MU_X = 0.2195149727645171
BETA_C = 0.06672455060314922
GAMMA_C = 0.031090690869654894
FZ_CURV = 1.709921
PARAMS_UNPOL = (0.031091, 0.2137, 7.5957, 3.5876, 1.6382, 0.49294)
PARAMS_POL = (0.015545, 0.20548, 14.1189, 6.1977, 3.3662, 0.62517)
PARAMS_STIFF = (0.016887, 0.11125, 10.357, 3.6231, 0.88026, 0.49671)

MESH = pl.DeviceIdType.MESH
LANES = 128
SUBLANES = 8
PACK = 256
VMEM_SPEC = pl.BlockSpec(memory_space=pltpu.VMEM)
HBM_SPEC = pl.BlockSpec(memory_space=pltpu.HBM)
VMEM_BYTES = 52 * 1024 * 1024
VMEM_MOST = 63 * 1024 * 1024
EARLY = 8


def exchange_spin(dens, log_dens, sigma):
    factor = -0.75 * (3.0 / math.pi) ** (1.0 / 3.0) * 2.0 ** (1.0 / 3.0)
    scale = (3.0 * math.pi**2) ** (2.0 / 3.0) * 2.0 ** (8.0 / 3.0)
    inverse_cube = jnp.exp(log_dens * (-1.0 / 3.0))
    cube = dens * inverse_cube * inverse_cube
    product = dens * cube
    weight = product * product
    bent = (MU_X / (KAPPA * scale)) * sigma
    inverse = 1.0 / (weight + bent)
    share = weight * inverse
    rest = KAPPA * bent * inverse
    enhance = 1.0 + rest
    energy = factor * product * enhance
    by_dens = factor * cube * ((4.0 / 3.0) * enhance - (8.0 / 3.0) * rest * share)
    square = dens * dens * inverse
    by_sigma = (factor * MU_X / scale) * square * square
    return energy, by_dens, by_sigma, cube, inverse_cube


def pw_piece(root, square, params):
    amp, alpha, b1, b2, b3, b4 = params
    doubled = 2.0 * amp
    series = root * (doubled * b1 + root * (doubled * b2 + root * (doubled * b3 + root * (doubled * b4))))
    slope = doubled * b1 + root * (
        2.0 * doubled * b2 + root * (3.0 * doubled * b3 + root * (4.0 * doubled * b4))
    )
    above = series + 1.0
    inverse = 1.0 / (series * above)
    logarithm = jnp.log(above * above * inverse)
    front = -doubled - (doubled * alpha) * square
    value = front * logarithm
    by_root = (-2.0 * doubled * alpha) * root * logarithm - front * slope * inverse
    return value, by_root


def xc_point(up, down, sigma_uu, sigma_ud, sigma_dd):
    energy_u, vx_u, by_uu, cube_u, inverse_u = exchange_spin(up, jnp.log(up), sigma_uu)
    energy_d, vx_d, by_dd, cube_d, inverse_d = exchange_spin(down, jnp.log(down), sigma_dd)
    total = up + down
    sixth = jnp.exp(jnp.log(total) * (-1.0 / 6.0))
    inverse_cube = sixth * sixth
    wigner = (3.0 / (4.0 * math.pi)) ** (1.0 / 3.0)
    root = math.sqrt(wigner) * sixth
    square = wigner * inverse_cube
    inverse_square = inverse_cube * inverse_cube
    inverse_total = inverse_square * inverse_cube
    cube = total * inverse_square
    zeta = (up - down) * inverse_total
    plus = 1.0 + zeta
    minus = 1.0 - zeta
    third = 2.0 ** (1.0 / 3.0)
    plus_cube = third * cube_u * inverse_cube
    minus_cube = third * cube_d * inverse_cube
    spin = 1.0 / (2.0 ** (4.0 / 3.0) - 2.0)
    weight = (plus * plus_cube + minus * minus_cube - 2.0) * spin
    by_weight = (4.0 / 3.0 * spin) * (plus_cube - minus_cube)
    unpol, unpol_root = pw_piece(root, square, PARAMS_UNPOL)
    pol, pol_root = pw_piece(root, square, PARAMS_POL)
    stiff, stiff_root = pw_piece(root, square, PARAMS_STIFF)
    stiff = stiff * (-1.0 / FZ_CURV)
    stiff_root = stiff_root * (-1.0 / FZ_CURV)
    zeta_two = zeta * zeta
    zeta_four = zeta_two * zeta_two
    gap = pol - unpol - stiff
    mixed = stiff + gap * zeta_four
    mixed_root = stiff_root + (pol_root - unpol_root - stiff_root) * zeta_four
    local = unpol + weight * mixed
    local_root = unpol_root + weight * mixed_root
    local_zeta = by_weight * mixed + weight * gap * (4.0 * zeta_two * zeta)
    phi = 0.5 * (plus_cube * plus_cube + minus_cube * minus_cube)
    by_phi = (2.0 ** (-1.0 / 3.0) / 3.0) * cube * (inverse_u - inverse_d)
    inverse_phi = 1.0 / phi
    phi_square = inverse_phi * inverse_phi
    inverse_gamma = phi_square * inverse_phi * (1.0 / GAMMA_C)
    gamma_phi = GAMMA_C * phi * phi * phi
    ratio = BETA_C / GAMMA_C
    expo = -local * inverse_gamma
    weight_a = ratio / (jnp.exp(expo) - 1.0)
    scale = math.pi / (16.0 * (3.0 * math.pi**2) ** (1.0 / 3.0))
    to_t = scale * phi_square * (inverse_square * inverse_cube) * (inverse_square * inverse_square)
    sigma = sigma_uu + 2.0 * sigma_ud + sigma_dd
    tee = sigma * to_t
    why = weight_a * tee
    numer = 1.0 + why
    denom = 1.0 + why * numer
    scaled = ratio * tee
    upper = denom + scaled * numer
    inverse = 1.0 / (denom * upper)
    gradient = gamma_phi * jnp.log(upper * upper * inverse)
    shared = gamma_phi * inverse
    by_tee = ratio * shared * (numer + why)
    by_a = shared * scaled * tee * why * (numer + 1.0)
    chain = by_a * weight_a * (1.0 + weight_a * (1.0 / ratio))
    by_local = 1.0 - chain * inverse_gamma
    tee_part = tee * by_tee
    phi_part = (3.0 * gradient - 3.0 * expo * chain - 2.0 * tee_part) * inverse_phi
    corr = local + gradient
    by_total = corr - (1.0 / 6.0) * root * local_root * by_local - (7.0 / 3.0) * tee_part
    by_zeta = by_local * local_zeta + phi_part * by_phi
    by_sigma = total * by_tee * to_t
    energy = energy_u + energy_d + total * corr
    return (
        energy,
        vx_u + by_total + by_zeta * minus,
        vx_d + by_total - by_zeta * plus,
        by_uu + by_sigma,
        2.0 * by_sigma,
        by_dd + by_sigma,
    )


def np_split(table):
    table = np.asarray(table, np.float32)
    high = table.astype(jnp.bfloat16)
    low = (table - high.astype(np.float32)).astype(jnp.bfloat16)
    return high, low


def y_tables(width_y, devices, scale):
    period = 2 * width_y
    count = period // devices
    half = count // 2
    slots = max(half, SUBLANES)
    device = np.arange(devices)[:, None]
    ky = device * count + np.arange(half)[None, :] + (device >= devices // 2)
    space = np.arange(width_y)
    angle = (ky[:, :, None] * space % period) * (2.0 * np.pi / period)
    both = np.stack([np.cos(angle), -np.sin(angle)], axis=1)
    both[0, 1, 0] = (-1.0) ** space
    weight = np.full((devices, 2, half, 1), 2.0)
    weight[0, :, 0] = 1.0
    pad = [(0, 0), (0, 0), (0, slots - half), (0, 0)]
    forward = np.pad(both, pad).reshape(devices * 2 * slots, width_y)
    back = np.pad(both * weight, pad).reshape(devices * 2 * slots, width_y)
    return *np_split(forward), *np_split(back.T * scale)


def x_tables(width_x):
    index = np.outer(np.arange(width_x), np.arange(width_x)) % (2 * width_x)
    angle = index * (np.pi / width_x)
    cos, sin = np.cos(angle), np.sin(angle)
    sin[:, 0] = (-1.0) ** np.arange(width_x)
    fore = np.concatenate([cos, sin], axis=1)
    back = np.concatenate([cos, sin.T], axis=0)
    return *np_split(fore), *np_split(back)


def stencil_matrix(size):
    table = np.zeros((size, size + 2 * REACH), np.float32)
    for row in range(size):
        for step, weight in enumerate(STENCIL_WHOLE, 1):
            table[row, row + REACH + step] = weight
            table[row, row + REACH - step] = -weight
    return table


def slope_tables(width_x, rows):
    wide = stencil_matrix(width_x)[:, REACH : REACH + width_x].T
    table = stencil_matrix(rows)
    inner = table[:, REACH : REACH + rows]
    below, above = table[:, :REACH], table[:, REACH + rows :]
    pad = np.zeros((rows, -(rows + 2 * REACH) % 16), np.float32)
    tall = np.concatenate([inner, above, below, pad], axis=1)
    tall = np.concatenate([tall] * 3, axis=1)
    tall = np.pad(tall, [(0, 0), (0, -tall.shape[1] % PACK)])
    return wide.astype(jnp.bfloat16), tall.astype(jnp.bfloat16)


def turn_table(width_x):
    table = np.zeros((width_x, width_x), np.float32)
    lanes = np.arange(width_x)
    table[(width_x - lanes) % width_x, lanes] = 1.0
    return table.astype(jnp.bfloat16)


def pack(tables):
    blocks, places, row = [], [], 0
    for table in tables:
        starts = []
        for column in range(0, table.shape[1], PACK):
            starts.append(row)
            blocks.append(table[:, column : column + PACK])
            row += table.shape[0]
        places.append((table.shape[0], tuple(starts)))
    return np.concatenate(blocks, axis=0), tuple(places)


def dot(left, right):
    return jnp.dot(left, right, preferred_element_type=jnp.float32)


def split(value):
    high = value.astype(jnp.bfloat16)
    low = (value - high.astype(jnp.float32)).astype(jnp.bfloat16)
    return high, low


def split_three(value):
    high = value.astype(jnp.bfloat16)
    rest = value - high.astype(jnp.float32)
    middle = rest.astype(jnp.bfloat16)
    low = (rest - middle.astype(jnp.float32)).astype(jnp.bfloat16)
    return high, middle, low


def dot_exact(value, table):
    high, middle, low = split_three(value)
    return dot(high, table) + (dot(middle, table) + dot(low, table))


def add(left, right):
    if left is None or right is None:
        return left if right is None else right
    return left[0] + right[0], left[1] + right[1]


def sub(left, right):
    if right is None:
        return left
    return left[0] - right[0], left[1] - right[1]


def turn(value, numer, denom, sign):
    if value is None:
        return None
    numer = numer * sign % denom
    eighth = numer * 8
    re, im = value
    if eighth % (2 * denom) == 0:
        quarter = eighth // (2 * denom)
        return ((re, im), (-im, re), (-re, -im), (im, -re))[quarter]
    if eighth % denom == 0:
        root = math.sqrt(0.5)
        plus, minus = root * (re + im), root * (re - im)
        return {1: (minus, plus), 3: (-plus, minus), 5: (-minus, -plus), 7: (plus, -minus)}[eighth // denom]
    cos = math.cos(2.0 * math.pi * numer / denom)
    sin = math.sin(2.0 * math.pi * numer / denom)
    return cos * re - sin * im, sin * re + cos * im


def small_dft(values, sign, first_half=False):
    count = len(values)
    if count == 1:
        return values
    even = small_dft(values[0::2], sign)
    odd = small_dft(values[1::2], sign)
    odd = [turn(value, k, count, sign) for k, value in enumerate(odd)]
    out = [add(e, o) for e, o in zip(even, odd)]
    if not first_half:
        out += [sub(e, o) for e, o in zip(even, odd)]
    return out


def mega_kernel(
    devices,
    group,
    half,
    places,
    *refs,
):
    dens_hbm, khat_hbm, table_hbm, hartree, v_all, sums, dens, khat, table = refs[:9]
    (
        spec_out,
        spec_in,
        halo_out,
        halo_in,
        main,
        grad_x,
        grad_y,
        grad_z,
        flux_z,
        flux_out,
        flux_in,
        v_own,
        edge_out,
        edge_in,
        k_raw,
        k_self,
        k_cross,
        z_in,
        z_mid,
        h_spec,
        x_in,
        back_out,
        back_in,
        partial,
        local_sems,
        spec_s,
        spec_r,
        back_s,
        back_r,
        part_s,
        part_r,
        main_s,
        main_r,
        relay_s,
        halo_s,
        halo_r,
        fz_s,
        fz_r,
        fy_s,
        fy_r,
        v_s,
        v_r,
        edge_s,
        edge_r,
    ) = refs[9:]
    me = lax.axis_index("gz")
    level, member = lax.div(me, group), lax.rem(me, group)
    levels = devices // group
    base = level * group
    width_y, width_x = dens.shape[1:]
    rows = width_y // group
    tiles = width_x // LANES
    depth = devices
    slots = spec_out.shape[1] // 2
    first_device, edge_device = 0, devices // 2
    cells = depth * width_y * width_x

    barrier = pltpu.get_barrier_semaphore()

    def greet(step, carry):
        pl.semaphore_signal(
            barrier, inc=1, device_id=(lax.rem(me + step, devices),), device_id_type=MESH
        )
        return carry

    lax.fori_loop(1, devices, greet, 0)

    cuts = (0, places[2][1][0], places[5][1][0], table.shape[0])
    pairs = [(dens_hbm, dens)]
    pairs += [
        (table_hbm.at[low:high], table.at[low:high]) for low, high in zip(cuts, cuts[1:])
    ]
    pairs.insert(2, (khat_hbm, khat))
    loads = [
        pltpu.make_async_copy(source, target, local_sems.at[i])
        for i, (source, target) in enumerate(pairs)
    ]
    for copy in loads:
        copy.start()

    def blocks(index):
        count, starts = places[index]
        return [table[start : start + count] for start in starts]

    def from_left(index, high, low):
        result = 0.0
        for k, (t_high, t_low) in enumerate(zip(blocks(index), blocks(index + 1))):
            part = slice(k * PACK, k * PACK + t_high.shape[1])
            upper, lower = high[part], low[part]
            result = result + (dot(t_high, upper) + (dot(t_high, lower) + dot(t_low, upper)))
        return result

    def from_right(index, high, low):
        return [
            dot(high, t_high) + (dot(low, t_high) + dot(high, t_low))
            for t_high, t_low in zip(blocks(index), blocks(index + 1))
        ]

    def remote(source, target, send, receive, peer):
        return pltpu.make_async_remote_copy(
            src_ref=source,
            dst_ref=target,
            send_sem=send,
            recv_sem=receive,
            device_id=(peer,),
            device_id_type=MESH,
        )

    loads[0].wait()
    sub_row = lax.broadcasted_iota(jnp.int32, (1, SUBLANES, width_x), 1)
    for b in range(group):
        above = dens[:, (b + 1) * rows : (b + 1) * rows + SUBLANES] if b < group - 1 else 0.0
        below = dens[:, b * rows - SUBLANES : b * rows] if b else 0.0
        halo_out[b] = jnp.where(sub_row < REACH, above, below)

    pl.semaphore_wait(barrier, devices - 1)

    upper = member >= REACH
    own_half = jnp.where(upper, REACH, 0)
    far_half = REACH - own_half
    near = jnp.where(upper, level + 1, level - 1)
    relay = jnp.where(upper, level - 1, level + 1)
    has_near = jnp.logical_and(near >= 0, near < levels)
    has_relay = jnp.logical_and(relay >= 0, relay < levels)

    def beyond(plane):
        return jnp.where(plane >= REACH, plane - (group - REACH), REACH + group + plane)

    def block(b):
        return pl.ds(pl.multiple_of(b * rows, rows), rows)

    def main_copy(b, peer, slot, which):
        return remote(
            dens.at[:, block(b)], main.at[:, slot], main_s.at[which], main_r.at[slot], peer
        )

    def halo_copy(b, peer, source):
        return remote(
            halo_out.at[b], halo_in.at[source], halo_s, halo_r, peer
        )

    def in_group(act):
        def body(step, carry):
            b = lax.rem(member + step, group)
            act(b, base + b)
            return carry

        lax.fori_loop(1, group, body, 0)

    def start_main(b, peer):
        main_copy(b, peer, REACH + member, 0).start()
        halo_copy(b, peer, member).start()

    def near_each(act):
        @pl.when(has_near)
        def _():
            def body(step, carry):
                b = own_half + lax.rem(member + step, REACH)
                act(main_copy(b, near * group + b, beyond(member), 1))
                return carry

            lax.fori_loop(0, REACH, body, 0)

    def relay_copy(step):
        plane = far_half + lax.rem(member + REACH - step, REACH)
        return plane, remote(
            main.at[:, REACH + plane],
            main.at[:, beyond(plane)],
            relay_s,
            main_r.at[beyond(plane)],
            relay * group + member,
        )

    near_each(lambda copy: copy.start())

    def start_far(step, carry):
        b = far_half + lax.rem(member + step, REACH)
        start_main(b, base + b)
        return carry

    def start_own(step, carry):
        b = own_half + lax.rem(member + step, REACH)
        start_main(b, base + b)
        return carry

    lax.fori_loop(0, REACH, start_far, 0)
    lax.fori_loop(1, REACH, start_own, 0)

    loads[1].wait()
    high, low = split(dens[0] + dens[1])
    spec_out[...] = from_left(0, high, low).reshape(spec_out.shape)
    loads[2].wait()

    @pl.when(me == edge_device)
    def _():
        edge_out[...] = khat[:, 0, :]
        remote(edge_out, edge_in, edge_s, edge_r, first_device).start()

    def spec_copy(step, peer, slot):
        return remote(
            spec_out.at[peer], spec_in.at[slot], spec_s, spec_r, peer
        )

    def around(act, first=1, last=devices):
        def body(index, carry):
            away = lax.div(index, 2)
            step = devices // 2 + jnp.where(lax.rem(index, 2) == 0, away, -away)
            act(step, lax.rem(me + step, devices), lax.rem(me - step + devices, devices))
            return carry

        lax.fori_loop(first, last, body, 0)

    def start_spec(step, peer, origin):
        spec_copy(step, peer, me).start()

    around(start_spec, last=1 + EARLY)
    main[:, REACH + member] = dens[:, block(member)]
    halo_in[member] = halo_out[member]
    spec_in[me] = spec_out[me]

    zero_planes = jnp.zeros((2, REACH, rows, width_x), jnp.float32)

    @pl.when(level == 0)
    def _():
        main[:, :REACH] = zero_planes
        flux_z[:, :REACH] = zero_planes

    @pl.when(level == levels - 1)
    def _():
        main[:, REACH + group :] = zero_planes
        flux_z[:, REACH + group :] = zero_planes

    loads[3].wait()
    (t_turn,), (t_wide,), (t_tall,) = blocks(2), blocks(3), blocks(4)
    lower = me < edge_device
    planes_k = khat.shape[0]
    if slots > half:
        k_raw[...] = jnp.ones(k_raw.shape, jnp.float32)

    def pick(kz, carry):
        row = jnp.where(lower, khat[kz, :half], khat[kz, 1 : half + 1])
        for t in range(tiles):
            k_self[kz, t, :half] = row[:, t * LANES : (t + 1) * LANES]
        k_raw[kz, :half] = row[:, width_x:]
        if slots > half:
            for t in range(tiles):
                k_self[kz, t, half:] = jnp.ones((slots - half, LANES), jnp.float32)
        return carry

    lax.fori_loop(0, planes_k, pick, 0)
    turned = dot_exact(k_raw[...].reshape(planes_k * slots, width_x), t_turn)
    turned = turned.reshape(planes_k, slots, width_x)
    for t in range(tiles):
        k_self[:, tiles + t] = turned[:, :, t * LANES : (t + 1) * LANES]

    def clear(kz, carry):
        k_cross[kz] = jnp.zeros(k_cross.shape[1:], jnp.float32)
        return carry

    lax.fori_loop(0, planes_k, clear, 0)

    def finish_main(b, peer):
        main_copy(b, peer, REACH + b, 0).wait_recv()

    def finish_far(step, carry):
        plane, copy = relay_copy(step)
        finish_main(plane, base + plane)

        @pl.when(has_relay)
        def _():
            copy.start()

        return carry

    lax.fori_loop(0, REACH, finish_far, 0)
    around(start_spec, first=1 + EARLY)

    def finish_own(step, carry):
        b = own_half + lax.rem(member + step, REACH)
        finish_main(b, base + b)
        return carry

    lax.fori_loop(1, REACH, finish_own, 0)
    mates = pl.ds(0, group - 1)
    remote(halo_out.at[mates], halo_in.at[mates], halo_s, halo_r, me).wait_recv()

    def slope_z(field, spin, plane):
        result = 0.0
        for step, weight in enumerate(STENCIL_WHOLE, 1):
            result = result + (weight * STENCIL_SCALE) * (
                field[spin, plane + REACH + step] - field[spin, plane + REACH - step]
            )
        return result

    pad_rows = -(rows + SUBLANES) % 16
    tall = 3 * (rows + SUBLANES + pad_rows)

    def slope_y(inner, outer):
        parts = [inner, outer]
        if pad_rows:
            parts.append(jnp.zeros((pad_rows, width_x), jnp.float32))
        stacked = jnp.concatenate(split_three(jnp.concatenate(parts, axis=0)), axis=0)
        return dot(t_tall[:, :tall], stacked) * STENCIL_SCALE

    def slope_x(field):
        value = field.reshape(group * rows, width_x)
        return (dot_exact(value, t_wide) * STENCIL_SCALE).reshape(group, rows, width_x)

    for spin in range(2):
        grad_x[spin] = slope_x(main[spin, REACH : REACH + group])

    def gradients(plane, carry):
        for spin in range(2):
            grad_y[spin, plane] = slope_y(main[spin, REACH + plane], halo_in[plane, spin])
        return carry

    lax.fori_loop(0, group, gradients, 0)
    def near_wait(first):
        def body(step, carry):
            main_copy(member, me, first + step, 1).wait_recv()
            return carry

        lax.fori_loop(0, REACH, body, 0)

    @pl.when(level > 0)
    def _():
        near_wait(0)

    @pl.when(level < levels - 1)
    def _():
        near_wait(REACH + group)


    def gradients_z(plane, carry):
        for spin in range(2):
            grad_z[spin, plane] = slope_z(main, spin, plane)
        return carry

    lax.fori_loop(0, group, gradients_z, 0)

    chunk = SUBLANES

    def point(index, acc):
        plane = lax.div(index, rows // chunk)
        at = pl.ds(pl.multiple_of(lax.rem(index, rows // chunk) * chunk, chunk), chunk)
        uz, uy, ux = grad_z[0, plane, at], grad_y[0, plane, at], grad_x[0, plane, at]
        dz, dy, dx = grad_z[1, plane, at], grad_y[1, plane, at], grad_x[1, plane, at]
        energy, d_up, d_down, d_uu, d_ud, d_dd = xc_point(
            main[0, REACH + plane, at],
            main[1, REACH + plane, at],
            uz * uz + uy * uy + ux * ux,
            uz * dz + uy * dy + ux * dx,
            dz * dz + dy * dy + dx * dx,
        )
        v_own[0, plane, at] = d_up
        v_own[1, plane, at] = d_down
        d_uu = 2.0 * d_uu
        d_dd = 2.0 * d_dd
        flux_z[0, REACH + plane, at] = d_uu * uz + d_ud * dz
        flux_z[1, REACH + plane, at] = d_dd * dz + d_ud * uz
        grad_y[0, plane, at] = d_uu * uy + d_ud * dy
        grad_y[1, plane, at] = d_dd * dy + d_ud * uy
        grad_x[0, plane, at] = d_uu * ux + d_ud * dx
        grad_x[1, plane, at] = d_dd * dx + d_ud * ux
        return acc + energy

    energy_acc = lax.fori_loop(
        0, group * rows // chunk, point, jnp.zeros((chunk, width_x), jnp.float32)
    )
    energy_xc = jnp.sum(energy_acc) * (1.0 / cells)

    def flux_z_copy(side, peer):
        source = (slice(group, group + REACH), slice(REACH, 2 * REACH))[side]
        target = (slice(0, REACH), slice(REACH + group, 2 * REACH + group))[side]
        return remote(
            flux_z.at[:, source], flux_z.at[:, target], fz_s.at[side], fz_r.at[side], peer
        )

    def flux_y_copy(side, peer):
        return remote(flux_out, flux_in.at[side], fy_s.at[side], fy_r.at[side], peer)

    exists_up, exists_down = level < levels - 1, level > 0
    right, left = member < group - 1, member > 0

    @pl.when(exists_up)
    def _():
        flux_z_copy(0, me + group).start()

    @pl.when(exists_down)
    def _():
        flux_z_copy(1, me - group).start()

    for spin in range(2):
        flux_out[:, spin] = jnp.where(
            sub_row < REACH, grad_y[spin, :, :SUBLANES], grad_y[spin, :, rows - SUBLANES :]
        )

    @pl.when(right)
    def _():
        flux_y_copy(0, me + 1).start()

    @pl.when(left)
    def _():
        flux_y_copy(1, me - 1).start()

    @pl.when(me == first_device)
    def _():
        remote(edge_out, edge_in, edge_s, edge_r, edge_device).wait_recv()
        edge_out[:, :width_x] = edge_in[:, :width_x]
        edge_out[:, width_x:] = dot_exact(edge_in[:, width_x:], t_turn)
        top = lax.broadcasted_iota(jnp.int32, (slots, LANES), 0) == 0

        def mix(kz, carry):
            other = edge_out[pl.ds(kz, 1), :]
            for t in range(2 * tiles):
                mine = k_self[kz, t]
                theirs = other[:, t * LANES : (t + 1) * LANES]
                k_self[kz, t] = jnp.where(top, 0.5 * (mine + theirs), mine)
                k_cross[kz, t] = jnp.where(top, 0.5 * (mine - theirs), 0.0)
            return carry

        lax.fori_loop(0, planes_k, mix, 0)

    loads[4].wait()
    others = pl.ds(0, devices - 1)
    remote(spec_out.at[others], spec_in.at[others], spec_s, spec_r, me).wait_recv()
    lane = lax.broadcasted_iota(jnp.int32, (1, 1, width_x), 2)
    first = lane == 0
    high, low = split(spec_in[...].reshape(depth * 2 * slots, width_x))
    wide = jnp.concatenate(from_right(5, high, low), axis=1)
    wide = wide.reshape(depth, 2, slots, 2 * width_x)
    cos_re, cos_im = wide[:, 0, :, :width_x], wide[:, 1, :, :width_x]
    sin_re, sin_im = wide[:, 0, :, width_x:], wide[:, 1, :, width_x:]
    fields = (
        (jnp.where(first, cos_re, cos_re + sin_im), jnp.where(first, cos_im, cos_im - sin_re)),
        (jnp.where(first, sin_re, cos_re - sin_im), jnp.where(first, sin_im, cos_im + sin_re)),
    )
    for sign in range(2):
        for part in range(2):
            for t in range(tiles):
                z_in[:, part, sign * tiles + t] = fields[sign][part][
                    :, :, t * LANES : (t + 1) * LANES
                ]

    n1, n2 = z_mid.shape[:2]
    full = n1 * n2

    def load(ref, *at):
        return ref[at[0], 0, at[1]], ref[at[0], 1, at[1]]

    def fore(col, carry):
        for j in range(n2):
            given = [load(z_in, n2 * i + j, col) for i in range(n1 // 2)]
            for k, value in enumerate(small_dft(given + [None] * (n1 // 2), -1)):
                re, im = turn(value, k * j, full, -1)
                z_mid[k, j, 0] = re
                z_mid[k, j, 1] = im
        for k in range(n1):
            given = [(z_mid[k, j, 0], z_mid[k, j, 1]) for j in range(n2)]
            for m, (re, im) in enumerate(small_dft(given, -1)):
                h_spec[k + n1 * m, 0, col] = re
                h_spec[k + n1 * m, 1, col] = im
        return carry

    lax.fori_loop(0, 2 * tiles, fore, 0)
    lane = lax.broadcasted_iota(jnp.int32, (slots, LANES), 1)

    def back(col, carry):
        other = lax.rem(col + tiles, 2 * tiles)
        alone = jnp.logical_and(lane == 0, lax.rem(col, tiles) == 0)
        for k in range(n1):
            given = []
            for m in range(n2):
                kz = k + n1 * m
                flip = (full - kz) % full
                re, im = load(h_spec, kz, col)
                own_re, own_im = load(h_spec, flip, col)
                far_re, far_im = load(h_spec, flip, other)
                far_re = jnp.where(alone, own_re, far_re)
                far_im = jnp.where(alone, own_im, far_im)
                direct, cross = k_self[kz, col], k_cross[kz, col]
                given.append((direct * re + cross * far_re, direct * im - cross * far_im))
            for j, value in enumerate(small_dft(given, 1)):
                re, im = turn(value, k * j, full, 1)
                z_mid[k, j, 0] = re
                z_mid[k, j, 1] = im
        for j in range(n2):
            given = [(z_mid[k, j, 0], z_mid[k, j, 1]) for k in range(n1)]
            for i, (re, im) in enumerate(small_dft(given, 1, first_half=True)):
                z_in[n2 * i + j, 0, col] = re
                z_in[n2 * i + j, 1, col] = im
        return carry

    lax.fori_loop(0, 2 * tiles, back, 0)
    for t in range(tiles):
        keep = lax.broadcasted_iota(jnp.int32, (1, 1, LANES), 2) + t * LANES == 0
        plus_re, plus_im = z_in[:, 0, t], z_in[:, 1, t]
        minus_re, minus_im = z_in[:, 0, tiles + t], z_in[:, 1, tiles + t]
        here = slice(t * LANES, (t + 1) * LANES)
        there = slice(width_x + t * LANES, width_x + (t + 1) * LANES)
        x_in[:, 0, :, here] = jnp.where(keep, plus_re, plus_re + minus_re)
        x_in[:, 1, :, here] = jnp.where(keep, plus_im, plus_im + minus_im)
        x_in[:, 0, :, there] = jnp.where(keep, minus_re, minus_im - plus_im)
        x_in[:, 1, :, there] = jnp.where(keep, minus_im, plus_re - minus_re)
    high, low = split(x_in[...].reshape(depth * 2 * slots, 2 * width_x))
    back_out[...] = jnp.concatenate(from_right(7, high, low), axis=1).reshape(back_out.shape)

    def back_copy(step, peer, slot):
        return remote(
            back_out.at[peer], back_in.at[slot], back_s, back_r, peer
        )

    around(lambda step, peer, origin: back_copy(step, peer, me).start())
    back_in[me] = back_out[me]

    acc = jnp.sum(spec_in[...] * back_out[...], axis=0)
    row = lax.broadcasted_iota(jnp.int32, acc.shape, 0)
    single = jnp.logical_and(me == first_device, lax.rem(row, slots) == 0)
    energy_h = jnp.sum(jnp.where(single, acc, 2.0 * acc)) * (0.5 / (8.0 * cells) / cells)
    lane = lax.broadcasted_iota(jnp.int32, partial.shape, 1)
    partial[...] = jnp.where(lane == 0, energy_xc, energy_h)

    def part_copy(step, peer, slot):
        return remote(partial, sums.at[slot], part_s, part_r, peer)

    around(lambda step, peer, origin: part_copy(step, peer, me).start())
    sums[me] = partial[...]

    @pl.when(exists_down)
    def _():
        flux_z_copy(0, me).wait_recv()

    @pl.when(exists_up)
    def _():
        flux_z_copy(1, me).wait_recv()

    @pl.when(left)
    def _():
        flux_y_copy(0, me).wait_recv()

    @pl.when(right)
    def _():
        flux_y_copy(1, me).wait_recv()

    @pl.when(jnp.logical_not(left))
    def _():
        flux_in[0] = jnp.zeros(flux_in.shape[1:], jnp.float32)

    @pl.when(jnp.logical_not(right))
    def _():
        flux_in[1] = jnp.zeros(flux_in.shape[1:], jnp.float32)

    for spin in range(2):
        v_own[spin] = v_own[spin] - slope_x(grad_x[spin])

    def divergence(plane, carry):
        for spin in range(2):
            outer = jnp.where(sub_row[0] < REACH, flux_in[1, plane, spin], flux_in[0, plane, spin])
            v_own[spin, plane] = v_own[spin, plane] - (
                slope_z(flux_z, spin, plane) + slope_y(grad_y[spin, plane], outer)
            )
        return carry

    lax.fori_loop(0, group, divergence, 0)

    def v_copy(b, peer, source):
        return remote(
            v_own.at[:, b], v_all.at[:, block(source)], v_s, v_r, peer
        )

    in_group(lambda b, peer: v_copy(b, peer, member).start())
    v_all[:, block(member)] = v_own[:, member]

    remote(back_out.at[others], back_in.at[others], back_s, back_r, me).wait_recv()
    high, low = split(back_in[...].reshape(depth * 2 * slots, width_x))
    hartree[...] = from_left(9, high, low)
    remote(v_own.at[:, mates], v_own.at[:, mates], v_s, v_r, me).wait_recv()
    remote(sums.at[others], sums.at[others], part_s, part_r, me).wait_recv()

    seven = main.at[:, mates]
    remote(seven, seven, main_s.at[0], main_r.at[0], me).wait_send()
    remote(halo_out.at[mates], halo_in.at[mates], halo_s, halo_r, me).wait_send()
    remote(seven, seven, v_s, v_r, me).wait_send()
    four = main.at[:, pl.ds(0, REACH)]

    @pl.when(has_near)
    def _():
        remote(four, four, main_s.at[1], main_r.at[0], me).wait_send()

    @pl.when(has_relay)
    def _():
        remote(four, four, relay_s, main_r.at[0], me).wait_send()

    remote(spec_out.at[others], spec_in.at[others], spec_s, spec_r, me).wait_send()
    remote(back_out.at[others], back_in.at[others], back_s, back_r, me).wait_send()
    remote(sums.at[others], sums.at[others], part_s, part_r, me).wait_send()

    @pl.when(exists_up)
    def _():
        flux_z_copy(0, me + group).wait_send()

    @pl.when(exists_down)
    def _():
        flux_z_copy(1, me - group).wait_send()

    @pl.when(right)
    def _():
        flux_y_copy(0, me + 1).wait_send()

    @pl.when(left)
    def _():
        flux_y_copy(1, me - 1).wait_send()

    @pl.when(me == edge_device)
    def _():
        remote(edge_out, edge_in, edge_s, edge_r, first_device).wait_send()


def join_kernel(hartree, v_all, sums, out, energies):
    out[0] = hartree[...] + v_all[0]
    out[1] = hartree[...] + v_all[1]
    both = jnp.sum(sums[...], axis=0)
    lane = lax.broadcasted_iota(jnp.int32, both.shape, 1)
    energies[0] = jnp.sum(jnp.where(lane == 0, both, 0.0))
    energies[1] = jnp.sum(jnp.where(lane == 1, both, 0.0))


def per_device(density, kernel_hat):
    planes, width_y, width_x = density.shape[1:]
    devices = lax.axis_size("gz")
    assert planes == 1
    group = 2 * REACH
    rows = width_y // group
    cells = devices * width_y * width_x
    count = kernel_hat.shape[1]
    half = count // 2
    slots = max(half, SUBLANES)
    tiles = width_x // LANES
    full = 2 * devices
    n1 = 1 << (full.bit_length() // 2)
    ty_high, ty_low, tb_high, tb_low = y_tables(width_y, devices, 1.0 / (8 * cells))
    tables = (
        ty_high,
        ty_low,
        turn_table(width_x),
        *slope_tables(width_x, rows),
        *x_tables(width_x),
        tb_high,
        tb_low,
    )
    packed, places = pack(tables)
    spec_shape = (devices, 2 * slots, width_x)
    tile_shape = (2, group, rows, width_x)
    tall_shape = (2, group + 2 * REACH, rows, width_x)
    f32 = functools.partial(pltpu.VMEM, dtype=jnp.float32)
    dma = pltpu.SemaphoreType.DMA
    scratch = [
        f32((2, width_y, width_x)),
        f32(kernel_hat.shape),
        pltpu.VMEM(packed.shape, packed.dtype),
        f32(spec_shape),
        f32(spec_shape),
        f32((group, 2, SUBLANES, width_x)),
        f32((group, 2, SUBLANES, width_x)),
        f32(tall_shape),
        f32(tile_shape),
        f32(tile_shape),
        f32(tile_shape),
        f32(tall_shape),
        f32((group, 2, SUBLANES, width_x)),
        f32((2, group, 2, SUBLANES, width_x)),
        f32(tile_shape),
        f32((full, 2 * width_x)),
        f32((full, 2 * width_x)),
        f32((full, slots, width_x)),
        f32((full, 2 * tiles, slots, LANES)),
        f32((full, 2 * tiles, slots, LANES)),
        f32((devices, 2, 2 * tiles, slots, LANES)),
        f32((n1, full // n1, 2, slots, LANES)),
        f32((full, 2, 2 * tiles, slots, LANES)),
        f32((devices, 2, slots, 2 * width_x)),
        f32(spec_shape),
        f32(spec_shape),
        f32((1, LANES)),
        dma((5,)),
        *[dma] * 6,
        dma((2,)),
        dma((group + 2 * REACH,)),
        *[dma] * 3,
        *[dma((2,))] * 4,
        *[dma] * 4,
    ]
    held = sum(math.prod(part.shape) for part in scratch if hasattr(part, "memory_space"))
    limit = max(VMEM_BYTES, min(VMEM_MOST, 8 * held))
    pieces = pl.pallas_call(
        functools.partial(mega_kernel, devices, group, half, places),
        out_shape=(
            jax.ShapeDtypeStruct((width_y, width_x), jnp.float32),
            jax.ShapeDtypeStruct((2, width_y, width_x), jnp.float32),
            jax.ShapeDtypeStruct((devices, 1, LANES), jnp.float32),
        ),
        in_specs=[HBM_SPEC] * 3,
        out_specs=(VMEM_SPEC,) * 3,
        scratch_shapes=scratch,
        compiler_params=pltpu.CompilerParams(
            collective_id=0, has_side_effects=True, vmem_limit_bytes=limit
        ),
        name="potential",
    )(density.reshape(2, width_y, width_x), kernel_hat, packed)
    potential, energies = pl.pallas_call(
        join_kernel,
        out_shape=(
            jax.ShapeDtypeStruct((2, width_y, width_x), jnp.float32),
            jax.ShapeDtypeStruct((2,), jnp.float32),
        ),
        in_specs=[VMEM_SPEC] * 3,
        out_specs=(VMEM_SPEC, pl.BlockSpec(memory_space=pltpu.SMEM)),
        compiler_params=pltpu.CompilerParams(vmem_limit_bytes=8 << 20),
        name="join",
    )(*pieces)
    return potential.reshape(density.shape), energies


def solution(mesh):
    placed = (P(None, "gz", None, None), P(None, "gz", None))
    return jax.shard_map(
        per_device,
        mesh=mesh,
        in_specs=placed,
        out_specs=(P(None, "gz", None, None), P()),
        check_vma=False,
    )
```

```python
import functools
import math

import jax
import jax.numpy as jnp
import numpy as np
from jax import lax
from jax.experimental import pallas as pl
from jax.experimental.pallas import tpu as pltpu
from jax.sharding import PartitionSpec as P

HGRID = 0.35
STENCIL_WHOLE = (672.0, -168.0, 32.0, -3.0)
STENCIL_SCALE = 1.0 / (840.0 * HGRID)
REACH = len(STENCIL_WHOLE)
KAPPA = 0.804
MU_X = 0.2195149727645171
BETA_C = 0.06672455060314922
GAMMA_C = 0.031090690869654894
FZ_CURV = 1.709921
PARAMS_UNPOL = (0.031091, 0.2137, 7.5957, 3.5876, 1.6382, 0.49294)
PARAMS_POL = (0.015545, 0.20548, 14.1189, 6.1977, 3.3662, 0.62517)
PARAMS_STIFF = (0.016887, 0.11125, 10.357, 3.6231, 0.88026, 0.49671)

MESH = pl.DeviceIdType.MESH
LANES = 128
SUBLANES = 8
PACK = 256
VMEM_SPEC = pl.BlockSpec(memory_space=pltpu.VMEM)
HBM_SPEC = pl.BlockSpec(memory_space=pltpu.HBM)
VMEM_BYTES = 53 * 1024 * 1024
VMEM_MOST = 63 * 1024 * 1024
EARLY = 12


def exchange_spin(dens, log_dens, sigma):
    factor = -0.75 * (3.0 / math.pi) ** (1.0 / 3.0) * 2.0 ** (1.0 / 3.0)
    scale = (3.0 * math.pi**2) ** (2.0 / 3.0) * 2.0 ** (8.0 / 3.0)
    inverse_cube = jnp.exp(log_dens * (-1.0 / 3.0))
    cube = dens * inverse_cube * inverse_cube
    product = dens * cube
    weight = product * product
    bent = (MU_X / (KAPPA * scale)) * sigma
    inverse = 1.0 / (weight + bent)
    share = weight * inverse
    rest = KAPPA * bent * inverse
    enhance = 1.0 + rest
    energy = factor * product * enhance
    by_dens = factor * cube * ((4.0 / 3.0) * enhance - (8.0 / 3.0) * rest * share)
    square = dens * dens * inverse
    by_sigma = (factor * MU_X / scale) * square * square
    return energy, by_dens, by_sigma, cube, inverse_cube


def pw_piece(root, square, params):
    amp, alpha, b1, b2, b3, b4 = params
    doubled = 2.0 * amp
    series = root * (doubled * b1 + root * (doubled * b2 + root * (doubled * b3 + root * (doubled * b4))))
    slope = doubled * b1 + root * (
        2.0 * doubled * b2 + root * (3.0 * doubled * b3 + root * (4.0 * doubled * b4))
    )
    above = series + 1.0
    inverse = 1.0 / (series * above)
    logarithm = jnp.log(above * above * inverse)
    front = -doubled - (doubled * alpha) * square
    value = front * logarithm
    by_root = (-2.0 * doubled * alpha) * root * logarithm - front * slope * inverse
    return value, by_root


def xc_point(up, down, sigma_uu, sigma_ud, sigma_dd):
    energy_u, vx_u, by_uu, cube_u, inverse_u = exchange_spin(up, jnp.log(up), sigma_uu)
    energy_d, vx_d, by_dd, cube_d, inverse_d = exchange_spin(down, jnp.log(down), sigma_dd)
    total = up + down
    sixth = jnp.exp(jnp.log(total) * (-1.0 / 6.0))
    inverse_cube = sixth * sixth
    wigner = (3.0 / (4.0 * math.pi)) ** (1.0 / 3.0)
    root = math.sqrt(wigner) * sixth
    square = wigner * inverse_cube
    inverse_square = inverse_cube * inverse_cube
    inverse_total = inverse_square * inverse_cube
    cube = total * inverse_square
    zeta = (up - down) * inverse_total
    plus = 1.0 + zeta
    minus = 1.0 - zeta
    third = 2.0 ** (1.0 / 3.0)
    plus_cube = third * cube_u * inverse_cube
    minus_cube = third * cube_d * inverse_cube
    spin = 1.0 / (2.0 ** (4.0 / 3.0) - 2.0)
    weight = (plus * plus_cube + minus * minus_cube - 2.0) * spin
    by_weight = (4.0 / 3.0 * spin) * (plus_cube - minus_cube)
    unpol, unpol_root = pw_piece(root, square, PARAMS_UNPOL)
    pol, pol_root = pw_piece(root, square, PARAMS_POL)
    stiff, stiff_root = pw_piece(root, square, PARAMS_STIFF)
    stiff = stiff * (-1.0 / FZ_CURV)
    stiff_root = stiff_root * (-1.0 / FZ_CURV)
    zeta_two = zeta * zeta
    zeta_four = zeta_two * zeta_two
    gap = pol - unpol - stiff
    mixed = stiff + gap * zeta_four
    mixed_root = stiff_root + (pol_root - unpol_root - stiff_root) * zeta_four
    local = unpol + weight * mixed
    local_root = unpol_root + weight * mixed_root
    local_zeta = by_weight * mixed + weight * gap * (4.0 * zeta_two * zeta)
    phi = 0.5 * (plus_cube * plus_cube + minus_cube * minus_cube)
    by_phi = (2.0 ** (-1.0 / 3.0) / 3.0) * cube * (inverse_u - inverse_d)
    inverse_phi = 1.0 / phi
    phi_square = inverse_phi * inverse_phi
    inverse_gamma = phi_square * inverse_phi * (1.0 / GAMMA_C)
    gamma_phi = GAMMA_C * phi * phi * phi
    ratio = BETA_C / GAMMA_C
    expo = -local * inverse_gamma
    weight_a = ratio / (jnp.exp(expo) - 1.0)
    scale = math.pi / (16.0 * (3.0 * math.pi**2) ** (1.0 / 3.0))
    to_t = scale * phi_square * (inverse_square * inverse_cube) * (inverse_square * inverse_square)
    sigma = sigma_uu + 2.0 * sigma_ud + sigma_dd
    tee = sigma * to_t
    why = weight_a * tee
    numer = 1.0 + why
    denom = 1.0 + why * numer
    scaled = ratio * tee
    upper = denom + scaled * numer
    inverse = 1.0 / (denom * upper)
    gradient = gamma_phi * jnp.log(upper * upper * inverse)
    shared = gamma_phi * inverse
    by_tee = ratio * shared * (numer + why)
    by_a = shared * scaled * tee * why * (numer + 1.0)
    chain = by_a * weight_a * (1.0 + weight_a * (1.0 / ratio))
    by_local = 1.0 - chain * inverse_gamma
    tee_part = tee * by_tee
    phi_part = (3.0 * gradient - 3.0 * expo * chain - 2.0 * tee_part) * inverse_phi
    corr = local + gradient
    by_total = corr - (1.0 / 6.0) * root * local_root * by_local - (7.0 / 3.0) * tee_part
    by_zeta = by_local * local_zeta + phi_part * by_phi
    by_sigma = total * by_tee * to_t
    energy = energy_u + energy_d + total * corr
    return (
        energy,
        vx_u + by_total + by_zeta * minus,
        vx_d + by_total - by_zeta * plus,
        by_uu + by_sigma,
        2.0 * by_sigma,
        by_dd + by_sigma,
    )


def np_split(table):
    table = np.asarray(table, np.float32)
    high = table.astype(jnp.bfloat16)
    low = (table - high.astype(np.float32)).astype(jnp.bfloat16)
    return high, low


def y_tables(width_y, devices, scale):
    period = 2 * width_y
    count = period // devices
    half = count // 2
    slots = max(half, SUBLANES)
    device = np.arange(devices)[:, None]
    ky = device * count + np.arange(half)[None, :] + (device >= devices // 2)
    space = np.arange(width_y)
    angle = (ky[:, :, None] * space % period) * (2.0 * np.pi / period)
    both = np.stack([np.cos(angle), -np.sin(angle)], axis=1)
    both[0, 1, 0] = (-1.0) ** space
    weight = np.full((devices, 2, half, 1), 2.0)
    weight[0, :, 0] = 1.0
    pad = [(0, 0), (0, 0), (0, slots - half), (0, 0)]
    forward = np.pad(both, pad).reshape(devices * 2 * slots, width_y)
    back = np.pad(both * weight, pad).reshape(devices * 2 * slots, width_y)
    return *np_split(forward), *np_split(back.T * scale)


def x_tables(width_x):
    index = np.outer(np.arange(width_x), np.arange(width_x)) % (2 * width_x)
    angle = index * (np.pi / width_x)
    cos, sin = np.cos(angle), np.sin(angle)
    sin[:, 0] = (-1.0) ** np.arange(width_x)
    fore = np.concatenate([cos, sin], axis=1)
    back = np.concatenate([cos, sin.T], axis=0)
    return *np_split(fore), *np_split(back)


def stencil_matrix(size):
    table = np.zeros((size, size + 2 * REACH), np.float32)
    for row in range(size):
        for step, weight in enumerate(STENCIL_WHOLE, 1):
            table[row, row + REACH + step] = weight
            table[row, row + REACH - step] = -weight
    return table


def slope_tables(width_x, rows):
    wide = stencil_matrix(width_x)[:, REACH : REACH + width_x].T
    table = stencil_matrix(rows)
    inner = table[:, REACH : REACH + rows]
    below, above = table[:, :REACH], table[:, REACH + rows :]
    pad = np.zeros((rows, -(rows + 2 * REACH) % 16), np.float32)
    tall = np.concatenate([inner, above, below, pad], axis=1)
    tall = np.concatenate([tall] * 3, axis=1)
    tall = np.pad(tall, [(0, 0), (0, -tall.shape[1] % PACK)])
    return wide.astype(jnp.bfloat16), tall.astype(jnp.bfloat16)


def turn_table(width_x):
    table = np.zeros((width_x, width_x), np.float32)
    lanes = np.arange(width_x)
    table[(width_x - lanes) % width_x, lanes] = 1.0
    return table.astype(jnp.bfloat16)


def pack(tables):
    blocks, places, row = [], [], 0
    for table in tables:
        starts = []
        for column in range(0, table.shape[1], PACK):
            starts.append(row)
            blocks.append(table[:, column : column + PACK])
            row += table.shape[0]
        places.append((table.shape[0], tuple(starts)))
    return np.concatenate(blocks, axis=0), tuple(places)


def dot(left, right):
    return jnp.dot(left, right, preferred_element_type=jnp.float32)


def split(value):
    high = value.astype(jnp.bfloat16)
    low = (value - high.astype(jnp.float32)).astype(jnp.bfloat16)
    return high, low


def split_three(value):
    high = value.astype(jnp.bfloat16)
    rest = value - high.astype(jnp.float32)
    middle = rest.astype(jnp.bfloat16)
    low = (rest - middle.astype(jnp.float32)).astype(jnp.bfloat16)
    return high, middle, low


def dot_exact(value, table):
    high, middle, low = split_three(value)
    return dot(high, table) + (dot(middle, table) + dot(low, table))


def add(left, right):
    if left is None or right is None:
        return left if right is None else right
    return left[0] + right[0], left[1] + right[1]


def sub(left, right):
    if right is None:
        return left
    return left[0] - right[0], left[1] - right[1]


def turn(value, numer, denom, sign):
    if value is None:
        return None
    numer = numer * sign % denom
    eighth = numer * 8
    re, im = value
    if eighth % (2 * denom) == 0:
        quarter = eighth // (2 * denom)
        return ((re, im), (-im, re), (-re, -im), (im, -re))[quarter]
    if eighth % denom == 0:
        root = math.sqrt(0.5)
        plus, minus = root * (re + im), root * (re - im)
        return {1: (minus, plus), 3: (-plus, minus), 5: (-minus, -plus), 7: (plus, -minus)}[eighth // denom]
    cos = math.cos(2.0 * math.pi * numer / denom)
    sin = math.sin(2.0 * math.pi * numer / denom)
    return cos * re - sin * im, sin * re + cos * im


def small_dft(values, sign, first_half=False):
    count = len(values)
    if count == 1:
        return values
    even = small_dft(values[0::2], sign)
    odd = small_dft(values[1::2], sign)
    odd = [turn(value, k, count, sign) for k, value in enumerate(odd)]
    out = [add(e, o) for e, o in zip(even, odd)]
    if not first_half:
        out += [sub(e, o) for e, o in zip(even, odd)]
    return out


def mega_kernel(
    devices,
    group,
    half,
    places,
    *refs,
):
    dens_hbm, khat_hbm, table_hbm, hartree, v_all, sums, dens, khat, table = refs[:9]
    (
        spec_out,
        spec_in,
        halo_out,
        halo_in,
        main,
        grad_x,
        grad_y,
        grad_z,
        flux_z,
        flux_out,
        flux_in,
        v_own,
        edge_out,
        edge_in,
        k_raw,
        k_self,
        k_cross,
        z_in,
        z_mid,
        h_spec,
        x_in,
        back_out,
        back_in,
        partial,
        local_sems,
        spec_s,
        spec_r,
        back_s,
        back_r,
        part_s,
        part_r,
        main_s,
        main_r,
        relay_s,
        halo_s,
        halo_r,
        fz_s,
        fz_r,
        fy_s,
        fy_r,
        v_s,
        v_r,
        edge_s,
        edge_r,
    ) = refs[9:]
    me = lax.axis_index("gz")
    level, member = lax.div(me, group), lax.rem(me, group)
    levels = devices // group
    base = level * group
    width_y, width_x = dens.shape[1:]
    rows = width_y // group
    tiles = width_x // LANES
    depth = devices
    slots = spec_out.shape[1] // 2
    first_device, edge_device = 0, devices // 2
    cells = depth * width_y * width_x


    barrier = pltpu.get_barrier_semaphore()

    def greet(step, carry):
        pl.semaphore_signal(
            barrier, inc=1, device_id=(lax.rem(me + step, devices),), device_id_type=MESH
        )
        return carry

    lax.fori_loop(1, devices, greet, 0)

    cuts = (0, places[2][1][0], places[5][1][0], table.shape[0])
    pairs = [(dens_hbm, dens)]
    pairs += [
        (table_hbm.at[low:high], table.at[low:high]) for low, high in zip(cuts, cuts[1:])
    ]
    pairs.insert(2, (khat_hbm, khat))
    loads = [
        pltpu.make_async_copy(source, target, local_sems.at[i])
        for i, (source, target) in enumerate(pairs)
    ]
    for copy in loads:
        copy.start()

    def blocks(index):
        count, starts = places[index]
        return [table[start : start + count] for start in starts]

    def from_left(index, high, low):
        result = 0.0
        for k, (t_high, t_low) in enumerate(zip(blocks(index), blocks(index + 1))):
            part = slice(k * PACK, k * PACK + t_high.shape[1])
            upper, lower = high[part], low[part]
            result = result + (dot(t_high, upper) + (dot(t_high, lower) + dot(t_low, upper)))
        return result

    def from_right(index, high, low):
        return [
            dot(high, t_high) + (dot(low, t_high) + dot(high, t_low))
            for t_high, t_low in zip(blocks(index), blocks(index + 1))
        ]

    def remote(source, target, send, receive, peer):
        return pltpu.make_async_remote_copy(
            src_ref=source,
            dst_ref=target,
            send_sem=send,
            recv_sem=receive,
            device_id=(peer,),
            device_id_type=MESH,
        )


    loads[0].wait()
    sub_row = lax.broadcasted_iota(jnp.int32, (1, SUBLANES, width_x), 1)
    for b in range(group):
        above = dens[:, (b + 1) * rows : (b + 1) * rows + SUBLANES] if b < group - 1 else 0.0
        below = dens[:, b * rows - SUBLANES : b * rows] if b else 0.0
        halo_out[b] = jnp.where(sub_row < REACH, above, below)


    pl.semaphore_wait(barrier, devices - 1)


    upper = member >= REACH
    own_half = jnp.where(upper, REACH, 0)
    far_half = REACH - own_half
    near = jnp.where(upper, level + 1, level - 1)
    relay = jnp.where(upper, level - 1, level + 1)
    has_near = jnp.logical_and(near >= 0, near < levels)
    has_relay = jnp.logical_and(relay >= 0, relay < levels)

    def beyond(plane):
        return jnp.where(plane >= REACH, plane - (group - REACH), REACH + group + plane)

    def block(b):
        return pl.ds(pl.multiple_of(b * rows, rows), rows)

    def main_copy(b, peer, slot, which):
        return remote(
            dens.at[:, block(b)], main.at[:, slot], main_s.at[which], main_r.at[slot], peer
        )

    def halo_copy(b, peer, source):
        return remote(
            halo_out.at[b], halo_in.at[source], halo_s, halo_r, peer
        )

    def in_group(act):
        def body(step, carry):
            b = lax.rem(member + step, group)
            act(b, base + b)
            return carry

        lax.fori_loop(1, group, body, 0)

    def start_main(b, peer):
        main_copy(b, peer, REACH + member, 0).start()
        halo_copy(b, peer, member).start()

    def near_each(act):
        @pl.when(has_near)
        def _():
            def body(step, carry):
                b = own_half + lax.rem(member + step, REACH)
                act(main_copy(b, near * group + b, beyond(member), 1))
                return carry

            lax.fori_loop(0, REACH, body, 0)

    def relay_copy(step):
        plane = far_half + lax.rem(member + REACH - step, REACH)
        return plane, remote(
            main.at[:, REACH + plane],
            main.at[:, beyond(plane)],
            relay_s,
            main_r.at[beyond(plane)],
            relay * group + member,
        )

    near_each(lambda copy: copy.start())

    def start_far(step, carry):
        b = far_half + lax.rem(member + step, REACH)
        start_main(b, base + b)
        return carry

    def start_own(step, carry):
        b = own_half + lax.rem(member + step, REACH)
        start_main(b, base + b)
        return carry

    lax.fori_loop(0, REACH, start_far, 0)
    lax.fori_loop(1, REACH, start_own, 0)


    loads[1].wait()
    high, low = split(dens[0] + dens[1])
    spec_out[...] = from_left(0, high, low).reshape(spec_out.shape)

    loads[2].wait()

    @pl.when(me == edge_device)
    def _():
        edge_out[...] = khat[:, 0, :]
        remote(edge_out, edge_in, edge_s, edge_r, first_device).start()

    def spec_copy(peer, slot):
        return remote(
            spec_out.at[peer], spec_in.at[slot], spec_s, spec_r, peer
        )

    crossing = group * (levels - 1)

    def around(act, first=0, last=devices - 1):
        def body(index, carry):
            inner = index >= crossing
            away = lax.rem(lax.div(index, group), levels - 1)
            hop = lax.div(away + 1, 2)
            hop = levels // 2 + jnp.where(lax.rem(away, 2) == 0, hop, -hop)
            turn_by = jnp.where(inner, index - crossing + 1, lax.rem(index, group))
            hop = jnp.where(inner, 0, hop)
            act(lax.rem(level + hop, levels) * group + lax.rem(member + turn_by, group))
            return carry

        lax.fori_loop(first, last, body, 0)

    def start_spec(peer):
        spec_copy(peer, me).start()

    around(start_spec, last=EARLY)
    main[:, REACH + member] = dens[:, block(member)]
    halo_in[member] = halo_out[member]
    spec_in[me] = spec_out[me]

    zero_planes = jnp.zeros((2, REACH, rows, width_x), jnp.float32)

    @pl.when(level == 0)
    def _():
        main[:, :REACH] = zero_planes
        flux_z[:, :REACH] = zero_planes

    @pl.when(level == levels - 1)
    def _():
        main[:, REACH + group :] = zero_planes
        flux_z[:, REACH + group :] = zero_planes


    loads[3].wait()
    (t_turn,), (t_wide,), (t_tall,) = blocks(2), blocks(3), blocks(4)
    lower = me < edge_device
    planes_k = khat.shape[0]
    if slots > half:
        k_raw[...] = jnp.ones(k_raw.shape, jnp.float32)

    def pick(kz, carry):
        row = jnp.where(lower, khat[kz, :half], khat[kz, 1 : half + 1])
        for t in range(tiles):
            k_self[kz, t, :half] = row[:, t * LANES : (t + 1) * LANES]
        k_raw[kz, :half] = row[:, width_x:]
        if slots > half:
            for t in range(tiles):
                k_self[kz, t, half:] = jnp.ones((slots - half, LANES), jnp.float32)
        return carry

    lax.fori_loop(0, planes_k, pick, 0)
    turned = dot_exact(k_raw[...].reshape(planes_k * slots, width_x), t_turn)
    turned = turned.reshape(planes_k, slots, width_x)
    for t in range(tiles):
        k_self[:, tiles + t] = turned[:, :, t * LANES : (t + 1) * LANES]

    def clear(kz, carry):
        k_cross[kz] = jnp.zeros(k_cross.shape[1:], jnp.float32)
        return carry

    lax.fori_loop(0, planes_k, clear, 0)


    def finish_main(b, peer):
        main_copy(b, peer, REACH + b, 0).wait_recv()

    def finish_far(step, carry):
        plane, copy = relay_copy(step)
        finish_main(plane, base + plane)

        @pl.when(has_relay)
        def _():
            copy.start()

        return carry

    lax.fori_loop(0, REACH, finish_far, 0)
    around(start_spec, first=EARLY)

    def finish_own(step, carry):
        b = own_half + lax.rem(member + step, REACH)
        finish_main(b, base + b)
        return carry

    lax.fori_loop(1, REACH, finish_own, 0)
    mates = pl.ds(0, group - 1)
    remote(halo_out.at[mates], halo_in.at[mates], halo_s, halo_r, me).wait_recv()


    def slope_z(field, spin, plane):
        result = 0.0
        for step, weight in enumerate(STENCIL_WHOLE, 1):
            result = result + (weight * STENCIL_SCALE) * (
                field[spin, plane + REACH + step] - field[spin, plane + REACH - step]
            )
        return result

    pad_rows = -(rows + SUBLANES) % 16
    tall = 3 * (rows + SUBLANES + pad_rows)

    def slope_y(inner, outer):
        parts = [inner, outer]
        if pad_rows:
            parts.append(jnp.zeros((pad_rows, width_x), jnp.float32))
        stacked = jnp.concatenate(split_three(jnp.concatenate(parts, axis=0)), axis=0)
        return dot(t_tall[:, :tall], stacked) * STENCIL_SCALE

    def slope_x(field):
        value = field.reshape(group * rows, width_x)
        return (dot_exact(value, t_wide) * STENCIL_SCALE).reshape(group, rows, width_x)

    for spin in range(2):
        grad_x[spin] = slope_x(main[spin, REACH : REACH + group])

    def gradients(plane, carry):
        for spin in range(2):
            grad_y[spin, plane] = slope_y(main[spin, REACH + plane], halo_in[plane, spin])
        return carry

    lax.fori_loop(0, group, gradients, 0)

    def near_wait(first):
        def body(step, carry):
            main_copy(member, me, first + step, 1).wait_recv()
            return carry

        lax.fori_loop(0, REACH, body, 0)

    @pl.when(level > 0)
    def _():
        near_wait(0)

    @pl.when(level < levels - 1)
    def _():
        near_wait(REACH + group)


    def gradients_z(plane, carry):
        for spin in range(2):
            grad_z[spin, plane] = slope_z(main, spin, plane)
        return carry

    lax.fori_loop(0, group, gradients_z, 0)


    chunk = SUBLANES

    def point(index, acc):
        plane = lax.div(index, rows // chunk)
        at = pl.ds(pl.multiple_of(lax.rem(index, rows // chunk) * chunk, chunk), chunk)
        uz, uy, ux = grad_z[0, plane, at], grad_y[0, plane, at], grad_x[0, plane, at]
        dz, dy, dx = grad_z[1, plane, at], grad_y[1, plane, at], grad_x[1, plane, at]
        energy, d_up, d_down, d_uu, d_ud, d_dd = xc_point(
            main[0, REACH + plane, at],
            main[1, REACH + plane, at],
            uz * uz + uy * uy + ux * ux,
            uz * dz + uy * dy + ux * dx,
            dz * dz + dy * dy + dx * dx,
        )
        v_own[0, plane, at] = d_up
        v_own[1, plane, at] = d_down
        d_uu = 2.0 * d_uu
        d_dd = 2.0 * d_dd
        flux_z[0, REACH + plane, at] = d_uu * uz + d_ud * dz
        flux_z[1, REACH + plane, at] = d_dd * dz + d_ud * uz
        grad_y[0, plane, at] = d_uu * uy + d_ud * dy
        grad_y[1, plane, at] = d_dd * dy + d_ud * uy
        grad_x[0, plane, at] = d_uu * ux + d_ud * dx
        grad_x[1, plane, at] = d_dd * dx + d_ud * ux
        return acc + energy

    def flux_z_copy(side, peer):
        source = (slice(group, group + REACH), slice(REACH, 2 * REACH))[side]
        target = (slice(0, REACH), slice(REACH + group, 2 * REACH + group))[side]
        return remote(
            flux_z.at[:, source], flux_z.at[:, target], fz_s.at[side], fz_r.at[side], peer
        )

    def flux_y_copy(side, peer):
        return remote(flux_out, flux_in.at[side], fy_s.at[side], fy_r.at[side], peer)

    exists_up, exists_down = level < levels - 1, level > 0
    right, left = member < group - 1, member > 0

    steps = group * rows // chunk
    energy_acc = jnp.zeros((chunk, width_x), jnp.float32)
    energy_acc = lax.fori_loop(steps // 2, steps, point, energy_acc)

    @pl.when(exists_up)
    def _():
        flux_z_copy(0, me + group).start()

    energy_acc = lax.fori_loop(0, steps // 2, point, energy_acc)

    @pl.when(exists_down)
    def _():
        flux_z_copy(1, me - group).start()

    energy_xc = jnp.sum(energy_acc) * (1.0 / cells)

    for spin in range(2):
        flux_out[:, spin] = jnp.where(
            sub_row < REACH, grad_y[spin, :, :SUBLANES], grad_y[spin, :, rows - SUBLANES :]
        )

    @pl.when(right)
    def _():
        flux_y_copy(0, me + 1).start()

    @pl.when(left)
    def _():
        flux_y_copy(1, me - 1).start()


    @pl.when(me == first_device)
    def _():
        remote(edge_out, edge_in, edge_s, edge_r, edge_device).wait_recv()
        edge_out[:, :width_x] = edge_in[:, :width_x]
        edge_out[:, width_x:] = dot_exact(edge_in[:, width_x:], t_turn)
        top = lax.broadcasted_iota(jnp.int32, (slots, LANES), 0) == 0

        def mix(kz, carry):
            other = edge_out[pl.ds(kz, 1), :]
            for t in range(2 * tiles):
                mine = k_self[kz, t]
                theirs = other[:, t * LANES : (t + 1) * LANES]
                k_self[kz, t] = jnp.where(top, 0.5 * (mine + theirs), mine)
                k_cross[kz, t] = jnp.where(top, 0.5 * (mine - theirs), 0.0)
            return carry

        lax.fori_loop(0, planes_k, mix, 0)


    for spin in range(2):
        v_own[spin] = v_own[spin] - slope_x(grad_x[spin])


    loads[4].wait()
    others = pl.ds(0, devices - 1)
    remote(spec_out.at[others], spec_in.at[others], spec_s, spec_r, me).wait_recv()

    lane = lax.broadcasted_iota(jnp.int32, (1, 1, width_x), 2)
    first = lane == 0
    high, low = split(spec_in[...].reshape(depth * 2 * slots, width_x))
    wide = jnp.concatenate(from_right(5, high, low), axis=1)
    wide = wide.reshape(depth, 2, slots, 2 * width_x)
    cos_re, cos_im = wide[:, 0, :, :width_x], wide[:, 1, :, :width_x]
    sin_re, sin_im = wide[:, 0, :, width_x:], wide[:, 1, :, width_x:]
    fields = (
        (jnp.where(first, cos_re, cos_re + sin_im), jnp.where(first, cos_im, cos_im - sin_re)),
        (jnp.where(first, sin_re, cos_re - sin_im), jnp.where(first, sin_im, cos_im + sin_re)),
    )
    for sign in range(2):
        for part in range(2):
            for t in range(tiles):
                z_in[:, part, sign * tiles + t] = fields[sign][part][
                    :, :, t * LANES : (t + 1) * LANES
                ]


    n1, n2 = z_mid.shape[:2]
    full = n1 * n2

    def load(ref, *at):
        return ref[at[0], 0, at[1]], ref[at[0], 1, at[1]]

    def fore(col, carry):
        for j in range(n2):
            given = [load(z_in, n2 * i + j, col) for i in range(n1 // 2)]
            for k, value in enumerate(small_dft(given + [None] * (n1 // 2), -1)):
                re, im = turn(value, k * j, full, -1)
                z_mid[k, j, 0] = re
                z_mid[k, j, 1] = im
        for k in range(n1):
            given = [(z_mid[k, j, 0], z_mid[k, j, 1]) for j in range(n2)]
            for m, (re, im) in enumerate(small_dft(given, -1)):
                h_spec[k + n1 * m, 0, col] = re
                h_spec[k + n1 * m, 1, col] = im
        return carry

    lax.fori_loop(0, 2 * tiles, fore, 0)

    lane = lax.broadcasted_iota(jnp.int32, (slots, LANES), 1)

    def back(col, carry):
        other = lax.rem(col + tiles, 2 * tiles)
        alone = jnp.logical_and(lane == 0, lax.rem(col, tiles) == 0)
        for k in range(n1):
            given = []
            for m in range(n2):
                kz = k + n1 * m
                flip = (full - kz) % full
                re, im = load(h_spec, kz, col)
                own_re, own_im = load(h_spec, flip, col)
                far_re, far_im = load(h_spec, flip, other)
                far_re = jnp.where(alone, own_re, far_re)
                far_im = jnp.where(alone, own_im, far_im)
                direct, cross = k_self[kz, col], k_cross[kz, col]
                given.append((direct * re + cross * far_re, direct * im - cross * far_im))
            for j, value in enumerate(small_dft(given, 1)):
                re, im = turn(value, k * j, full, 1)
                z_mid[k, j, 0] = re
                z_mid[k, j, 1] = im
        for j in range(n2):
            given = [(z_mid[k, j, 0], z_mid[k, j, 1]) for k in range(n1)]
            for i, (re, im) in enumerate(small_dft(given, 1, first_half=True)):
                z_in[n2 * i + j, 0, col] = re
                z_in[n2 * i + j, 1, col] = im
        return carry

    lax.fori_loop(0, 2 * tiles, back, 0)

    for t in range(tiles):
        keep = lax.broadcasted_iota(jnp.int32, (1, 1, LANES), 2) + t * LANES == 0
        plus_re, plus_im = z_in[:, 0, t], z_in[:, 1, t]
        minus_re, minus_im = z_in[:, 0, tiles + t], z_in[:, 1, tiles + t]
        here = slice(t * LANES, (t + 1) * LANES)
        there = slice(width_x + t * LANES, width_x + (t + 1) * LANES)
        x_in[:, 0, :, here] = jnp.where(keep, plus_re, plus_re + minus_re)
        x_in[:, 1, :, here] = jnp.where(keep, plus_im, plus_im + minus_im)
        x_in[:, 0, :, there] = jnp.where(keep, minus_re, minus_im - plus_im)
        x_in[:, 1, :, there] = jnp.where(keep, minus_im, plus_re - minus_re)
    high, low = split(x_in[...].reshape(depth * 2 * slots, 2 * width_x))
    back_out[...] = jnp.concatenate(from_right(7, high, low), axis=1).reshape(back_out.shape)


    def back_copy(peer, slot):
        return remote(
            back_out.at[peer], back_in.at[slot], back_s, back_r, peer
        )

    around(lambda peer: back_copy(peer, me).start(), first=crossing)
    around(lambda peer: back_copy(peer, me).start(), last=crossing)
    back_in[me] = back_out[me]


    @pl.when(left)
    def _():
        flux_y_copy(0, me).wait_recv()

    @pl.when(right)
    def _():
        flux_y_copy(1, me).wait_recv()

    @pl.when(jnp.logical_not(left))
    def _():
        flux_in[0] = jnp.zeros(flux_in.shape[1:], jnp.float32)

    @pl.when(jnp.logical_not(right))
    def _():
        flux_in[1] = jnp.zeros(flux_in.shape[1:], jnp.float32)


    def divergence(plane, carry):
        for spin in range(2):
            outer = jnp.where(sub_row[0] < REACH, flux_in[1, plane, spin], flux_in[0, plane, spin])
            v_own[spin, plane] = v_own[spin, plane] - slope_y(grad_y[spin, plane], outer)
        return carry

    lax.fori_loop(0, group, divergence, 0)


    @pl.when(exists_down)
    def _():
        flux_z_copy(0, me).wait_recv()

    @pl.when(exists_up)
    def _():
        flux_z_copy(1, me).wait_recv()


    def divergence_z(plane, carry):
        for spin in range(2):
            v_own[spin, plane] = v_own[spin, plane] - slope_z(flux_z, spin, plane)
        return carry

    lax.fori_loop(0, group, divergence_z, 0)

    def v_copy(b, peer, source):
        return remote(
            v_own.at[:, b], v_all.at[:, block(source)], v_s, v_r, peer
        )

    in_group(lambda b, peer: v_copy(b, peer, member).start())
    v_all[:, block(member)] = v_own[:, member]


    acc = jnp.sum(spec_in[...] * back_out[...], axis=0)
    row = lax.broadcasted_iota(jnp.int32, acc.shape, 0)
    single = jnp.logical_and(me == first_device, lax.rem(row, slots) == 0)
    energy_h = jnp.sum(jnp.where(single, acc, 2.0 * acc)) * (0.5 / (8.0 * cells) / cells)
    lane = lax.broadcasted_iota(jnp.int32, partial.shape, 1)
    partial[...] = jnp.where(lane == 0, energy_xc, energy_h)

    def part_copy(peer, slot):
        return remote(partial, sums.at[slot], part_s, part_r, peer)

    around(lambda peer: part_copy(peer, me).start())
    sums[me] = partial[...]


    remote(back_out.at[others], back_in.at[others], back_s, back_r, me).wait_recv()

    high, low = split(back_in[...].reshape(depth * 2 * slots, width_x))
    hartree[...] = from_left(9, high, low)

    remote(v_own.at[:, mates], v_own.at[:, mates], v_s, v_r, me).wait_recv()

    remote(sums.at[others], sums.at[others], part_s, part_r, me).wait_recv()


    seven = main.at[:, mates]
    remote(seven, seven, main_s.at[0], main_r.at[0], me).wait_send()
    remote(halo_out.at[mates], halo_in.at[mates], halo_s, halo_r, me).wait_send()
    remote(seven, seven, v_s, v_r, me).wait_send()
    four = main.at[:, pl.ds(0, REACH)]

    @pl.when(has_near)
    def _():
        remote(four, four, main_s.at[1], main_r.at[0], me).wait_send()

    @pl.when(has_relay)
    def _():
        remote(four, four, relay_s, main_r.at[0], me).wait_send()

    remote(spec_out.at[others], spec_in.at[others], spec_s, spec_r, me).wait_send()
    remote(back_out.at[others], back_in.at[others], back_s, back_r, me).wait_send()
    remote(sums.at[others], sums.at[others], part_s, part_r, me).wait_send()

    @pl.when(exists_up)
    def _():
        flux_z_copy(0, me + group).wait_send()

    @pl.when(exists_down)
    def _():
        flux_z_copy(1, me - group).wait_send()

    @pl.when(right)
    def _():
        flux_y_copy(0, me + 1).wait_send()

    @pl.when(left)
    def _():
        flux_y_copy(1, me - 1).wait_send()

    @pl.when(me == edge_device)
    def _():
        remote(edge_out, edge_in, edge_s, edge_r, first_device).wait_send()


def join_kernel(hartree, v_all, sums, out, energies):
    out[0] = hartree[...] + v_all[0]
    out[1] = hartree[...] + v_all[1]
    both = jnp.sum(sums[...], axis=0)
    lane = lax.broadcasted_iota(jnp.int32, both.shape, 1)
    energies[0] = jnp.sum(jnp.where(lane == 0, both, 0.0))
    energies[1] = jnp.sum(jnp.where(lane == 1, both, 0.0))


def per_device(density, kernel_hat):
    planes, width_y, width_x = density.shape[1:]
    devices = lax.axis_size("gz")
    assert planes == 1
    group = 2 * REACH
    rows = width_y // group
    cells = devices * width_y * width_x
    count = kernel_hat.shape[1]
    half = count // 2
    slots = max(half, SUBLANES)
    tiles = width_x // LANES
    full = 2 * devices
    n1 = 1 << (full.bit_length() // 2)
    ty_high, ty_low, tb_high, tb_low = y_tables(width_y, devices, 1.0 / (8 * cells))
    tables = (
        ty_high,
        ty_low,
        turn_table(width_x),
        *slope_tables(width_x, rows),
        *x_tables(width_x),
        tb_high,
        tb_low,
    )
    packed, places = pack(tables)
    spec_shape = (devices, 2 * slots, width_x)
    tile_shape = (2, group, rows, width_x)
    tall_shape = (2, group + 2 * REACH, rows, width_x)
    f32 = functools.partial(pltpu.VMEM, dtype=jnp.float32)
    dma = pltpu.SemaphoreType.DMA
    scratch = [
        f32((2, width_y, width_x)),
        f32(kernel_hat.shape),
        pltpu.VMEM(packed.shape, packed.dtype),
        f32(spec_shape),
        f32(spec_shape),
        f32((group, 2, SUBLANES, width_x)),
        f32((group, 2, SUBLANES, width_x)),
        f32(tall_shape),
        f32(tile_shape),
        f32(tile_shape),
        f32(tile_shape),
        f32(tall_shape),
        f32((group, 2, SUBLANES, width_x)),
        f32((2, group, 2, SUBLANES, width_x)),
        f32(tile_shape),
        f32((full, 2 * width_x)),
        f32((full, 2 * width_x)),
        f32((full, slots, width_x)),
        f32((full, 2 * tiles, slots, LANES)),
        f32((full, 2 * tiles, slots, LANES)),
        f32((devices, 2, 2 * tiles, slots, LANES)),
        f32((n1, full // n1, 2, slots, LANES)),
        f32((full, 2, 2 * tiles, slots, LANES)),
        f32((devices, 2, slots, 2 * width_x)),
        f32(spec_shape),
        f32(spec_shape),
        f32((1, LANES)),
        dma((5,)),
        *[dma] * 6,
        dma((2,)),
        dma((group + 2 * REACH,)),
        *[dma] * 3,
        *[dma((2,))] * 4,
        *[dma] * 4,
    ]
    held = sum(math.prod(part.shape) for part in scratch if hasattr(part, "memory_space"))
    limit = max(VMEM_BYTES, min(VMEM_MOST, 8 * held))
    pieces = pl.pallas_call(
        functools.partial(mega_kernel, devices, group, half, places),
        out_shape=(
            jax.ShapeDtypeStruct((width_y, width_x), jnp.float32),
            jax.ShapeDtypeStruct((2, width_y, width_x), jnp.float32),
            jax.ShapeDtypeStruct((devices, 1, LANES), jnp.float32),
        ),
        in_specs=[HBM_SPEC] * 3,
        out_specs=(VMEM_SPEC,) * 3,
        scratch_shapes=scratch,
        compiler_params=pltpu.CompilerParams(
            collective_id=0, has_side_effects=True, vmem_limit_bytes=limit
        ),
        name="potential",
    )(density.reshape(2, width_y, width_x), kernel_hat, packed)
    potential, energies = pl.pallas_call(
        join_kernel,
        out_shape=(
            jax.ShapeDtypeStruct((2, width_y, width_x), jnp.float32),
            jax.ShapeDtypeStruct((2,), jnp.float32),
        ),
        in_specs=[VMEM_SPEC] * 3,
        out_specs=(VMEM_SPEC, pl.BlockSpec(memory_space=pltpu.SMEM)),
        compiler_params=pltpu.CompilerParams(vmem_limit_bytes=8 << 20),
        name="join",
    )(*pieces)
    return potential.reshape(density.shape), energies


def solution(mesh):
    placed = (P(None, "gz", None, None), P(None, "gz", None))
    return jax.shard_map(
        per_device,
        mesh=mesh,
        in_specs=placed,
        out_specs=(P(None, "gz", None, None), P()),
        check_vma=False,
    )
```

```python
import functools
import math

import jax
import jax.numpy as jnp
import numpy as np
from jax import lax
from jax.experimental import pallas as pl
from jax.experimental.pallas import tpu as pltpu
from jax.sharding import PartitionSpec as P

HGRID = 0.35
STENCIL_WHOLE = (672.0, -168.0, 32.0, -3.0)
STENCIL_SCALE = 1.0 / (840.0 * HGRID)
REACH = len(STENCIL_WHOLE)
KAPPA = 0.804
MU_X = 0.2195149727645171
BETA_C = 0.06672455060314922
GAMMA_C = 0.031090690869654894
FZ_CURV = 1.709921
PARAMS_UNPOL = (0.031091, 0.2137, 7.5957, 3.5876, 1.6382, 0.49294)
PARAMS_POL = (0.015545, 0.20548, 14.1189, 6.1977, 3.3662, 0.62517)
PARAMS_STIFF = (0.016887, 0.11125, 10.357, 3.6231, 0.88026, 0.49671)

MESH = pl.DeviceIdType.MESH
LANES = 128
SUBLANES = 8
PACK = 256
VMEM_SPEC = pl.BlockSpec(memory_space=pltpu.VMEM)
HBM_SPEC = pl.BlockSpec(memory_space=pltpu.HBM)
VMEM_BYTES = 53 * 1024 * 1024
VMEM_MOST = 63 * 1024 * 1024
EARLY = 12
KNOWN = 11


def exchange_spin(dens, cube, sigma):
    factor = -0.75 * (3.0 / math.pi) ** (1.0 / 3.0) * 2.0 ** (1.0 / 3.0)
    scale = (3.0 * math.pi**2) ** (2.0 / 3.0) * 2.0 ** (8.0 / 3.0)
    product = dens * cube
    weight = product * product
    bent = (MU_X / (KAPPA * scale)) * sigma
    inverse = 1.0 / (weight + bent)
    share = weight * inverse
    rest = KAPPA * bent * inverse
    enhance = 1.0 + rest
    energy = factor * product * enhance
    by_dens = factor * cube * ((4.0 / 3.0) * enhance - (8.0 / 3.0) * rest * share)
    square = dens * dens * inverse
    by_sigma = (factor * MU_X / scale) * square * square
    return energy, by_dens, by_sigma


def pw_piece(root, square, params):
    amp, alpha, b1, b2, b3, b4 = params
    doubled = 2.0 * amp
    series = root * (doubled * b1 + root * (doubled * b2 + root * (doubled * b3 + root * (doubled * b4))))
    slope = doubled * b1 + root * (
        2.0 * doubled * b2 + root * (3.0 * doubled * b3 + root * (4.0 * doubled * b4))
    )
    above = series + 1.0
    inverse = 1.0 / (series * above)
    logarithm = jnp.log(above * above * inverse)
    front = -doubled - (doubled * alpha) * square
    value = front * logarithm
    by_root = (-2.0 * doubled * alpha) * root * logarithm - front * slope * inverse
    return value, by_root


def xc_density(up, down):
    inverse_u = jnp.exp(jnp.log(up) * (-1.0 / 3.0))
    inverse_d = jnp.exp(jnp.log(down) * (-1.0 / 3.0))
    cube_u = up * inverse_u * inverse_u
    cube_d = down * inverse_d * inverse_d
    total = up + down
    sixth = jnp.exp(jnp.log(total) * (-1.0 / 6.0))
    inverse_cube = sixth * sixth
    wigner = (3.0 / (4.0 * math.pi)) ** (1.0 / 3.0)
    root = math.sqrt(wigner) * sixth
    square = wigner * inverse_cube
    inverse_square = inverse_cube * inverse_cube
    inverse_total = inverse_square * inverse_cube
    cube = total * inverse_square
    zeta = (up - down) * inverse_total
    plus = 1.0 + zeta
    minus = 1.0 - zeta
    third = 2.0 ** (1.0 / 3.0)
    plus_cube = third * cube_u * inverse_cube
    minus_cube = third * cube_d * inverse_cube
    spin = 1.0 / (2.0 ** (4.0 / 3.0) - 2.0)
    weight = (plus * plus_cube + minus * minus_cube - 2.0) * spin
    by_weight = (4.0 / 3.0 * spin) * (plus_cube - minus_cube)
    unpol, unpol_root = pw_piece(root, square, PARAMS_UNPOL)
    pol, pol_root = pw_piece(root, square, PARAMS_POL)
    stiff, stiff_root = pw_piece(root, square, PARAMS_STIFF)
    stiff = stiff * (-1.0 / FZ_CURV)
    stiff_root = stiff_root * (-1.0 / FZ_CURV)
    zeta_two = zeta * zeta
    zeta_four = zeta_two * zeta_two
    gap = pol - unpol - stiff
    mixed = stiff + gap * zeta_four
    mixed_root = stiff_root + (pol_root - unpol_root - stiff_root) * zeta_four
    local = unpol + weight * mixed
    local_root = unpol_root + weight * mixed_root
    local_zeta = by_weight * mixed + weight * gap * (4.0 * zeta_two * zeta)
    phi = 0.5 * (plus_cube * plus_cube + minus_cube * minus_cube)
    by_phi = (2.0 ** (-1.0 / 3.0) / 3.0) * cube * (inverse_u - inverse_d)
    inverse_phi = 1.0 / phi
    phi_square = inverse_phi * inverse_phi
    inverse_gamma = phi_square * inverse_phi * (1.0 / GAMMA_C)
    gamma_phi = GAMMA_C * phi * phi * phi
    ratio = BETA_C / GAMMA_C
    expo = -local * inverse_gamma
    weight_a = ratio / (jnp.exp(expo) - 1.0)
    scale = math.pi / (16.0 * (3.0 * math.pi**2) ** (1.0 / 3.0))
    to_t = scale * phi_square * (inverse_square * inverse_cube) * (inverse_square * inverse_square)
    slope = (1.0 / 6.0) * root * local_root
    return (
        cube_u, cube_d, zeta, local, slope, local_zeta, by_phi, inverse_phi, gamma_phi, weight_a, to_t
    )


def xc_gradient(up, down, given, sigma_uu, sigma_ud, sigma_dd):
    cube_u, cube_d, zeta, local, slope, local_zeta, by_phi, inverse_phi, gamma_phi, weight_a, to_t = given
    energy_u, vx_u, by_uu = exchange_spin(up, cube_u, sigma_uu)
    energy_d, vx_d, by_dd = exchange_spin(down, cube_d, sigma_dd)
    total = up + down
    ratio = BETA_C / GAMMA_C
    inverse_gamma = inverse_phi * inverse_phi * inverse_phi * (1.0 / GAMMA_C)
    expo = -local * inverse_gamma
    sigma = sigma_uu + 2.0 * sigma_ud + sigma_dd
    tee = sigma * to_t
    why = weight_a * tee
    numer = 1.0 + why
    denom = 1.0 + why * numer
    scaled = ratio * tee
    upper = denom + scaled * numer
    inverse = 1.0 / (denom * upper)
    gradient = gamma_phi * jnp.log(upper * upper * inverse)
    shared = gamma_phi * inverse
    by_tee = ratio * shared * (numer + why)
    by_a = shared * scaled * tee * why * (numer + 1.0)
    chain = by_a * weight_a * (1.0 + weight_a * (1.0 / ratio))
    by_local = 1.0 - chain * inverse_gamma
    tee_part = tee * by_tee
    phi_part = (3.0 * gradient - 3.0 * expo * chain - 2.0 * tee_part) * inverse_phi
    corr = local + gradient
    by_total = corr - slope * by_local - (7.0 / 3.0) * tee_part
    by_zeta = by_local * local_zeta + phi_part * by_phi
    by_sigma = total * by_tee * to_t
    energy = energy_u + energy_d + total * corr
    return (
        energy,
        vx_u + by_total + by_zeta * (1.0 - zeta),
        vx_d + by_total - by_zeta * (1.0 + zeta),
        by_uu + by_sigma,
        2.0 * by_sigma,
        by_dd + by_sigma,
    )


def np_split(table):
    table = np.asarray(table, np.float32)
    high = table.astype(jnp.bfloat16)
    low = (table - high.astype(np.float32)).astype(jnp.bfloat16)
    return high, low


def y_tables(width_y, devices, scale):
    period = 2 * width_y
    count = period // devices
    half = count // 2
    slots = max(half, SUBLANES)
    device = np.arange(devices)[:, None]
    ky = device * count + np.arange(half)[None, :] + (device >= devices // 2)
    space = np.arange(width_y)
    angle = (ky[:, :, None] * space % period) * (2.0 * np.pi / period)
    both = np.stack([np.cos(angle), -np.sin(angle)], axis=1)
    both[0, 1, 0] = (-1.0) ** space
    weight = np.full((devices, 2, half, 1), 2.0)
    weight[0, :, 0] = 1.0
    pad = [(0, 0), (0, 0), (0, slots - half), (0, 0)]
    forward = np.pad(both, pad).reshape(devices * 2 * slots, width_y)
    back = np.pad(both * weight, pad).reshape(devices * 2 * slots, width_y)
    return *np_split(forward), *np_split(back.T * scale)


def x_tables(width_x):
    index = np.outer(np.arange(width_x), np.arange(width_x)) % (2 * width_x)
    angle = index * (np.pi / width_x)
    cos, sin = np.cos(angle), np.sin(angle)
    sin[:, 0] = (-1.0) ** np.arange(width_x)
    fore = np.concatenate([cos, sin], axis=1)
    back = np.concatenate([cos, sin.T], axis=0)
    return *np_split(fore), *np_split(back)


def stencil_matrix(size):
    table = np.zeros((size, size + 2 * REACH), np.float32)
    for row in range(size):
        for step, weight in enumerate(STENCIL_WHOLE, 1):
            table[row, row + REACH + step] = weight
            table[row, row + REACH - step] = -weight
    return table


def slope_tables(width_x, rows):
    wide = stencil_matrix(width_x)[:, REACH : REACH + width_x].T
    table = stencil_matrix(rows)
    inner = table[:, REACH : REACH + rows]
    below, above = table[:, :REACH], table[:, REACH + rows :]
    pad = np.zeros((rows, -(rows + 2 * REACH) % 16), np.float32)
    tall = np.concatenate([inner, above, below, pad], axis=1)
    tall = np.concatenate([tall] * 3, axis=1)
    tall = np.pad(tall, [(0, 0), (0, -tall.shape[1] % PACK)])
    return wide.astype(jnp.bfloat16), tall.astype(jnp.bfloat16)


def turn_table(width_x):
    table = np.zeros((width_x, width_x), np.float32)
    lanes = np.arange(width_x)
    table[(width_x - lanes) % width_x, lanes] = 1.0
    return table.astype(jnp.bfloat16)


def pack(tables):
    blocks, places, row = [], [], 0
    for table in tables:
        starts = []
        for column in range(0, table.shape[1], PACK):
            starts.append(row)
            blocks.append(table[:, column : column + PACK])
            row += table.shape[0]
        places.append((table.shape[0], tuple(starts)))
    return np.concatenate(blocks, axis=0), tuple(places)


def dot(left, right):
    return jnp.dot(left, right, preferred_element_type=jnp.float32)


def split(value):
    high = value.astype(jnp.bfloat16)
    low = (value - high.astype(jnp.float32)).astype(jnp.bfloat16)
    return high, low


def split_three(value):
    high = value.astype(jnp.bfloat16)
    rest = value - high.astype(jnp.float32)
    middle = rest.astype(jnp.bfloat16)
    low = (rest - middle.astype(jnp.float32)).astype(jnp.bfloat16)
    return high, middle, low


def dot_exact(value, table):
    high, middle, low = split_three(value)
    return dot(high, table) + (dot(middle, table) + dot(low, table))


def add(left, right):
    if left is None or right is None:
        return left if right is None else right
    return left[0] + right[0], left[1] + right[1]


def sub(left, right):
    if right is None:
        return left
    return left[0] - right[0], left[1] - right[1]


def turn(value, numer, denom, sign):
    if value is None:
        return None
    numer = numer * sign % denom
    eighth = numer * 8
    re, im = value
    if eighth % (2 * denom) == 0:
        quarter = eighth // (2 * denom)
        return ((re, im), (-im, re), (-re, -im), (im, -re))[quarter]
    if eighth % denom == 0:
        root = math.sqrt(0.5)
        plus, minus = root * (re + im), root * (re - im)
        return {1: (minus, plus), 3: (-plus, minus), 5: (-minus, -plus), 7: (plus, -minus)}[eighth // denom]
    cos = math.cos(2.0 * math.pi * numer / denom)
    sin = math.sin(2.0 * math.pi * numer / denom)
    return cos * re - sin * im, sin * re + cos * im


def small_dft(values, sign, first_half=False):
    count = len(values)
    if count == 1:
        return values
    even = small_dft(values[0::2], sign)
    odd = small_dft(values[1::2], sign)
    odd = [turn(value, k, count, sign) for k, value in enumerate(odd)]
    out = [add(e, o) for e, o in zip(even, odd)]
    if not first_half:
        out += [sub(e, o) for e, o in zip(even, odd)]
    return out


def mega_kernel(
    devices,
    group,
    half,
    places,
    *refs,
):
    dens_hbm, khat_hbm, table_hbm, hartree, v_all, sums, dens, khat, table = refs[:9]
    (
        spec_out,
        spec_in,
        halo_out,
        halo_in,
        main,
        grad_x,
        grad_y,
        grad_z,
        known,
        flux_z,
        flux_out,
        flux_in,
        v_own,
        edge_out,
        edge_in,
        k_raw,
        k_self,
        k_cross,
        z_in,
        z_mid,
        h_spec,
        x_in,
        back_out,
        back_in,
        partial,
        local_sems,
        spec_s,
        spec_r,
        back_s,
        back_r,
        part_s,
        part_r,
        main_s,
        main_r,
        relay_s,
        halo_s,
        halo_r,
        fz_s,
        fz_r,
        fy_s,
        fy_r,
        v_s,
        v_r,
        edge_s,
        edge_r,
    ) = refs[9:]
    me = lax.axis_index("gz")
    level, member = lax.div(me, group), lax.rem(me, group)
    levels = devices // group
    base = level * group
    width_y, width_x = dens.shape[1:]
    rows = width_y // group
    tiles = width_x // LANES
    depth = devices
    slots = spec_out.shape[1] // 2
    first_device, edge_device = 0, devices // 2
    cells = depth * width_y * width_x

    barrier = pltpu.get_barrier_semaphore()

    def greet(step, carry):
        pl.semaphore_signal(
            barrier, inc=1, device_id=(lax.rem(me + step, devices),), device_id_type=MESH
        )
        return carry

    lax.fori_loop(1, devices, greet, 0)

    cuts = (0, places[2][1][0], places[5][1][0], table.shape[0])
    pairs = [(dens_hbm, dens)]
    pairs += [
        (table_hbm.at[low:high], table.at[low:high]) for low, high in zip(cuts, cuts[1:])
    ]
    pairs.insert(2, (khat_hbm, khat))
    loads = [
        pltpu.make_async_copy(source, target, local_sems.at[i])
        for i, (source, target) in enumerate(pairs)
    ]
    for copy in loads:
        copy.start()

    def blocks(index):
        count, starts = places[index]
        return [table[start : start + count] for start in starts]

    def from_left(index, high, low):
        result = 0.0
        for k, (t_high, t_low) in enumerate(zip(blocks(index), blocks(index + 1))):
            part = slice(k * PACK, k * PACK + t_high.shape[1])
            upper, lower = high[part], low[part]
            result = result + (dot(t_high, upper) + (dot(t_high, lower) + dot(t_low, upper)))
        return result

    def from_right(index, high, low):
        return [
            dot(high, t_high) + (dot(low, t_high) + dot(high, t_low))
            for t_high, t_low in zip(blocks(index), blocks(index + 1))
        ]

    def remote(source, target, send, receive, peer):
        return pltpu.make_async_remote_copy(
            src_ref=source,
            dst_ref=target,
            send_sem=send,
            recv_sem=receive,
            device_id=(peer,),
            device_id_type=MESH,
        )

    loads[0].wait()
    sub_row = lax.broadcasted_iota(jnp.int32, (1, SUBLANES, width_x), 1)
    for b in range(group):
        above = dens[:, (b + 1) * rows : (b + 1) * rows + SUBLANES] if b < group - 1 else 0.0
        below = dens[:, b * rows - SUBLANES : b * rows] if b else 0.0
        halo_out[b] = jnp.where(sub_row < REACH, above, below)

    pl.semaphore_wait(barrier, devices - 1)

    upper = member >= REACH
    own_half = jnp.where(upper, REACH, 0)
    far_half = REACH - own_half
    near = jnp.where(upper, level + 1, level - 1)
    relay = jnp.where(upper, level - 1, level + 1)
    has_near = jnp.logical_and(near >= 0, near < levels)
    has_relay = jnp.logical_and(relay >= 0, relay < levels)

    def beyond(plane):
        return jnp.where(plane >= REACH, plane - (group - REACH), REACH + group + plane)

    def block(b):
        return pl.ds(pl.multiple_of(b * rows, rows), rows)

    def main_copy(b, peer, slot, which):
        return remote(
            dens.at[:, block(b)], main.at[:, slot], main_s.at[which], main_r.at[slot], peer
        )

    def halo_copy(b, peer, source):
        return remote(
            halo_out.at[b], halo_in.at[source], halo_s, halo_r, peer
        )

    def in_group(act):
        def body(step, carry):
            b = lax.rem(member + step, group)
            act(b, base + b)
            return carry

        lax.fori_loop(1, group, body, 0)

    def start_main(b, peer):
        main_copy(b, peer, REACH + member, 0).start()
        halo_copy(b, peer, member).start()

    def near_each(act):
        @pl.when(has_near)
        def _():
            def body(step, carry):
                b = own_half + lax.rem(member + step, REACH)
                act(main_copy(b, near * group + b, beyond(member), 1))
                return carry

            lax.fori_loop(0, REACH, body, 0)

    def relay_copy(step):
        plane = far_half + lax.rem(member + REACH - step, REACH)
        return plane, remote(
            main.at[:, REACH + plane],
            main.at[:, beyond(plane)],
            relay_s,
            main_r.at[beyond(plane)],
            relay * group + member,
        )

    near_each(lambda copy: copy.start())

    def start_far(step, carry):
        b = far_half + lax.rem(member + step, REACH)
        start_main(b, base + b)
        return carry

    def start_own(step, carry):
        b = own_half + lax.rem(member + step, REACH)
        start_main(b, base + b)
        return carry

    lax.fori_loop(0, REACH, start_far, 0)
    lax.fori_loop(1, REACH, start_own, 0)

    loads[1].wait()
    high, low = split(dens[0] + dens[1])
    spec_out[...] = from_left(0, high, low).reshape(spec_out.shape)
    loads[2].wait()

    @pl.when(me == edge_device)
    def _():
        edge_out[...] = khat[:, 0, :]
        remote(edge_out, edge_in, edge_s, edge_r, first_device).start()

    def spec_copy(peer, slot):
        return remote(
            spec_out.at[peer], spec_in.at[slot], spec_s, spec_r, peer
        )

    crossing = group * (levels - 1)

    def around(act, first=0, last=devices - 1):
        def body(index, carry):
            inner = index >= crossing
            away = lax.rem(lax.div(index, group), levels - 1)
            hop = lax.div(away + 1, 2)
            hop = levels // 2 + jnp.where(lax.rem(away, 2) == 0, hop, -hop)
            turn_by = jnp.where(inner, index - crossing + 1, lax.rem(index, group))
            hop = jnp.where(inner, 0, hop)
            act(lax.rem(level + hop, levels) * group + lax.rem(member + turn_by, group))
            return carry

        lax.fori_loop(first, last, body, 0)

    def start_spec(peer):
        spec_copy(peer, me).start()

    around(start_spec, last=EARLY)
    main[:, REACH + member] = dens[:, block(member)]
    halo_in[member] = halo_out[member]
    spec_in[me] = spec_out[me]

    zero_planes = jnp.zeros((2, REACH, rows, width_x), jnp.float32)

    @pl.when(level == 0)
    def _():
        main[:, :REACH] = zero_planes
        flux_z[:, :REACH] = zero_planes

    @pl.when(level == levels - 1)
    def _():
        main[:, REACH + group :] = zero_planes
        flux_z[:, REACH + group :] = zero_planes

    loads[3].wait()
    (t_turn,), (t_wide,), (t_tall,) = blocks(2), blocks(3), blocks(4)
    lower = me < edge_device
    planes_k = khat.shape[0]
    if slots > half:
        k_raw[...] = jnp.ones(k_raw.shape, jnp.float32)

    def pick(kz, carry):
        row = jnp.where(lower, khat[kz, :half], khat[kz, 1 : half + 1])
        for t in range(tiles):
            k_self[kz, t, :half] = row[:, t * LANES : (t + 1) * LANES]
        k_raw[kz, :half] = row[:, width_x:]
        if slots > half:
            for t in range(tiles):
                k_self[kz, t, half:] = jnp.ones((slots - half, LANES), jnp.float32)
        return carry

    lax.fori_loop(0, planes_k, pick, 0)
    turned = dot_exact(k_raw[...].reshape(planes_k * slots, width_x), t_turn)
    turned = turned.reshape(planes_k, slots, width_x)
    for t in range(tiles):
        k_self[:, tiles + t] = turned[:, :, t * LANES : (t + 1) * LANES]

    def clear(kz, carry):
        k_cross[kz] = jnp.zeros(k_cross.shape[1:], jnp.float32)
        return carry

    lax.fori_loop(0, planes_k, clear, 0)

    def finish_main(b, peer):
        main_copy(b, peer, REACH + b, 0).wait_recv()

    def finish_far(step, carry):
        plane, copy = relay_copy(step)
        finish_main(plane, base + plane)

        @pl.when(has_relay)
        def _():
            copy.start()

        return carry

    lax.fori_loop(0, REACH, finish_far, 0)
    around(start_spec, first=EARLY)
    chunk = 2 * SUBLANES

    def density_part(plane):
        def body(index, carry):
            at = pl.ds(pl.multiple_of(index * chunk, chunk), chunk)
            parts = xc_density(main[0, REACH + plane, at], main[1, REACH + plane, at])
            for i, part in enumerate(parts):
                known[i, plane, at] = part
            return carry

        lax.fori_loop(0, rows // chunk, body, 0)

    def density_far(step, carry):
        density_part(far_half + step)
        return carry

    density_part(member)
    lax.fori_loop(0, REACH, density_far, 0)

    def finish_own(step, carry):
        b = own_half + lax.rem(member + step, REACH)
        finish_main(b, base + b)
        density_part(b)
        return carry

    lax.fori_loop(1, REACH, finish_own, 0)
    mates = pl.ds(0, group - 1)
    remote(halo_out.at[mates], halo_in.at[mates], halo_s, halo_r, me).wait_recv()

    def slope_z(field, spin, plane):
        result = 0.0
        for step, weight in enumerate(STENCIL_WHOLE, 1):
            result = result + (weight * STENCIL_SCALE) * (
                field[spin, plane + REACH + step] - field[spin, plane + REACH - step]
            )
        return result

    pad_rows = -(rows + SUBLANES) % 16
    tall = 3 * (rows + SUBLANES + pad_rows)

    def slope_y(inner, outer):
        parts = [inner, outer]
        if pad_rows:
            parts.append(jnp.zeros((pad_rows, width_x), jnp.float32))
        stacked = jnp.concatenate(split_three(jnp.concatenate(parts, axis=0)), axis=0)
        return dot(t_tall[:, :tall], stacked) * STENCIL_SCALE

    def slope_x(field):
        value = field.reshape(group * rows, width_x)
        return (dot_exact(value, t_wide) * STENCIL_SCALE).reshape(group, rows, width_x)

    for spin in range(2):
        grad_x[spin] = slope_x(main[spin, REACH : REACH + group])

    def gradients(plane, carry):
        for spin in range(2):
            grad_y[spin, plane] = slope_y(main[spin, REACH + plane], halo_in[plane, spin])
        return carry

    lax.fori_loop(0, group, gradients, 0)
    def near_wait(first):
        def body(step, carry):
            main_copy(member, me, first + step, 1).wait_recv()
            return carry

        lax.fori_loop(0, REACH, body, 0)

    @pl.when(level > 0)
    def _():
        near_wait(0)

    @pl.when(level < levels - 1)
    def _():
        near_wait(REACH + group)


    def gradients_z(plane, carry):
        for spin in range(2):
            grad_z[spin, plane] = slope_z(main, spin, plane)
        return carry

    lax.fori_loop(0, group, gradients_z, 0)


    def point(index, acc):
        plane = lax.div(index, rows // chunk)
        at = pl.ds(pl.multiple_of(lax.rem(index, rows // chunk) * chunk, chunk), chunk)
        uz, uy, ux = grad_z[0, plane, at], grad_y[0, plane, at], grad_x[0, plane, at]
        dz, dy, dx = grad_z[1, plane, at], grad_y[1, plane, at], grad_x[1, plane, at]
        energy, d_up, d_down, d_uu, d_ud, d_dd = xc_gradient(
            main[0, REACH + plane, at],
            main[1, REACH + plane, at],
            [known[i, plane, at] for i in range(KNOWN)],
            uz * uz + uy * uy + ux * ux,
            uz * dz + uy * dy + ux * dx,
            dz * dz + dy * dy + dx * dx,
        )
        v_own[0, plane, at] = d_up
        v_own[1, plane, at] = d_down
        d_uu = 2.0 * d_uu
        d_dd = 2.0 * d_dd
        flux_z[0, REACH + plane, at] = d_uu * uz + d_ud * dz
        flux_z[1, REACH + plane, at] = d_dd * dz + d_ud * uz
        grad_y[0, plane, at] = d_uu * uy + d_ud * dy
        grad_y[1, plane, at] = d_dd * dy + d_ud * uy
        grad_x[0, plane, at] = d_uu * ux + d_ud * dx
        grad_x[1, plane, at] = d_dd * dx + d_ud * ux
        return acc + energy

    def flux_z_copy(side, peer):
        source = (slice(group, group + REACH), slice(REACH, 2 * REACH))[side]
        target = (slice(0, REACH), slice(REACH + group, 2 * REACH + group))[side]
        return remote(
            flux_z.at[:, source], flux_z.at[:, target], fz_s.at[side], fz_r.at[side], peer
        )

    def flux_y_copy(side, peer):
        return remote(flux_out, flux_in.at[side], fy_s.at[side], fy_r.at[side], peer)

    exists_up, exists_down = level < levels - 1, level > 0
    right, left = member < group - 1, member > 0

    steps = group * rows // chunk
    energy_acc = jnp.zeros((chunk, width_x), jnp.float32)
    energy_acc = lax.fori_loop(steps // 2, steps, point, energy_acc)

    @pl.when(exists_up)
    def _():
        flux_z_copy(0, me + group).start()

    energy_acc = lax.fori_loop(0, steps // 2, point, energy_acc)

    @pl.when(exists_down)
    def _():
        flux_z_copy(1, me - group).start()

    energy_xc = jnp.sum(energy_acc) * (1.0 / cells)
    for spin in range(2):
        flux_out[:, spin] = jnp.where(
            sub_row < REACH, grad_y[spin, :, :SUBLANES], grad_y[spin, :, rows - SUBLANES :]
        )

    @pl.when(right)
    def _():
        flux_y_copy(0, me + 1).start()

    @pl.when(left)
    def _():
        flux_y_copy(1, me - 1).start()

    @pl.when(me == first_device)
    def _():
        remote(edge_out, edge_in, edge_s, edge_r, edge_device).wait_recv()
        edge_out[:, :width_x] = edge_in[:, :width_x]
        edge_out[:, width_x:] = dot_exact(edge_in[:, width_x:], t_turn)
        top = lax.broadcasted_iota(jnp.int32, (slots, LANES), 0) == 0

        def mix(kz, carry):
            other = edge_out[pl.ds(kz, 1), :]
            for t in range(2 * tiles):
                mine = k_self[kz, t]
                theirs = other[:, t * LANES : (t + 1) * LANES]
                k_self[kz, t] = jnp.where(top, 0.5 * (mine + theirs), mine)
                k_cross[kz, t] = jnp.where(top, 0.5 * (mine - theirs), 0.0)
            return carry

        lax.fori_loop(0, planes_k, mix, 0)

    for spin in range(2):
        v_own[spin] = v_own[spin] - slope_x(grad_x[spin])

    loads[4].wait()
    others = pl.ds(0, devices - 1)
    remote(spec_out.at[others], spec_in.at[others], spec_s, spec_r, me).wait_recv()
    lane = lax.broadcasted_iota(jnp.int32, (1, 1, width_x), 2)
    first = lane == 0
    high, low = split(spec_in[...].reshape(depth * 2 * slots, width_x))
    wide = jnp.concatenate(from_right(5, high, low), axis=1)
    wide = wide.reshape(depth, 2, slots, 2 * width_x)
    cos_re, cos_im = wide[:, 0, :, :width_x], wide[:, 1, :, :width_x]
    sin_re, sin_im = wide[:, 0, :, width_x:], wide[:, 1, :, width_x:]
    fields = (
        (jnp.where(first, cos_re, cos_re + sin_im), jnp.where(first, cos_im, cos_im - sin_re)),
        (jnp.where(first, sin_re, cos_re - sin_im), jnp.where(first, sin_im, cos_im + sin_re)),
    )
    for sign in range(2):
        for part in range(2):
            for t in range(tiles):
                z_in[:, part, sign * tiles + t] = fields[sign][part][
                    :, :, t * LANES : (t + 1) * LANES
                ]

    n1, n2 = z_mid.shape[:2]
    full = n1 * n2

    def load(ref, *at):
        return ref[at[0], 0, at[1]], ref[at[0], 1, at[1]]

    def fore(col, carry):
        for j in range(n2):
            given = [load(z_in, n2 * i + j, col) for i in range(n1 // 2)]
            for k, value in enumerate(small_dft(given + [None] * (n1 // 2), -1)):
                re, im = turn(value, k * j, full, -1)
                z_mid[k, j, 0] = re
                z_mid[k, j, 1] = im
        for k in range(n1):
            given = [(z_mid[k, j, 0], z_mid[k, j, 1]) for j in range(n2)]
            for m, (re, im) in enumerate(small_dft(given, -1)):
                h_spec[k + n1 * m, 0, col] = re
                h_spec[k + n1 * m, 1, col] = im
        return carry

    lax.fori_loop(0, 2 * tiles, fore, 0)
    lane = lax.broadcasted_iota(jnp.int32, (slots, LANES), 1)

    def back(col, carry):
        other = lax.rem(col + tiles, 2 * tiles)
        alone = jnp.logical_and(lane == 0, lax.rem(col, tiles) == 0)
        for k in range(n1):
            given = []
            for m in range(n2):
                kz = k + n1 * m
                flip = (full - kz) % full
                re, im = load(h_spec, kz, col)
                own_re, own_im = load(h_spec, flip, col)
                far_re, far_im = load(h_spec, flip, other)
                far_re = jnp.where(alone, own_re, far_re)
                far_im = jnp.where(alone, own_im, far_im)
                direct, cross = k_self[kz, col], k_cross[kz, col]
                given.append((direct * re + cross * far_re, direct * im - cross * far_im))
            for j, value in enumerate(small_dft(given, 1)):
                re, im = turn(value, k * j, full, 1)
                z_mid[k, j, 0] = re
                z_mid[k, j, 1] = im
        for j in range(n2):
            given = [(z_mid[k, j, 0], z_mid[k, j, 1]) for k in range(n1)]
            for i, (re, im) in enumerate(small_dft(given, 1, first_half=True)):
                z_in[n2 * i + j, 0, col] = re
                z_in[n2 * i + j, 1, col] = im
        return carry

    lax.fori_loop(0, 2 * tiles, back, 0)
    for t in range(tiles):
        keep = lax.broadcasted_iota(jnp.int32, (1, 1, LANES), 2) + t * LANES == 0
        plus_re, plus_im = z_in[:, 0, t], z_in[:, 1, t]
        minus_re, minus_im = z_in[:, 0, tiles + t], z_in[:, 1, tiles + t]
        here = slice(t * LANES, (t + 1) * LANES)
        there = slice(width_x + t * LANES, width_x + (t + 1) * LANES)
        x_in[:, 0, :, here] = jnp.where(keep, plus_re, plus_re + minus_re)
        x_in[:, 1, :, here] = jnp.where(keep, plus_im, plus_im + minus_im)
        x_in[:, 0, :, there] = jnp.where(keep, minus_re, minus_im - plus_im)
        x_in[:, 1, :, there] = jnp.where(keep, minus_im, plus_re - minus_re)
    high, low = split(x_in[...].reshape(depth * 2 * slots, 2 * width_x))
    back_out[...] = jnp.concatenate(from_right(7, high, low), axis=1).reshape(back_out.shape)

    def back_copy(peer, slot):
        return remote(
            back_out.at[peer], back_in.at[slot], back_s, back_r, peer
        )

    around(lambda peer: back_copy(peer, me).start(), last=crossing)
    around(lambda peer: back_copy(peer, me).start(), first=crossing)
    back_in[me] = back_out[me]

    @pl.when(left)
    def _():
        flux_y_copy(0, me).wait_recv()

    @pl.when(right)
    def _():
        flux_y_copy(1, me).wait_recv()

    @pl.when(jnp.logical_not(left))
    def _():
        flux_in[0] = jnp.zeros(flux_in.shape[1:], jnp.float32)

    @pl.when(jnp.logical_not(right))
    def _():
        flux_in[1] = jnp.zeros(flux_in.shape[1:], jnp.float32)

    def divergence(plane, carry):
        for spin in range(2):
            outer = jnp.where(sub_row[0] < REACH, flux_in[1, plane, spin], flux_in[0, plane, spin])
            v_own[spin, plane] = v_own[spin, plane] - slope_y(grad_y[spin, plane], outer)
        return carry

    lax.fori_loop(0, group, divergence, 0)

    @pl.when(exists_down)
    def _():
        flux_z_copy(0, me).wait_recv()

    @pl.when(exists_up)
    def _():
        flux_z_copy(1, me).wait_recv()

    def divergence_z(plane, carry):
        for spin in range(2):
            v_own[spin, plane] = v_own[spin, plane] - slope_z(flux_z, spin, plane)
        return carry

    lax.fori_loop(0, group, divergence_z, 0)
    def v_copy(b, peer, source):
        return remote(
            v_own.at[:, b], v_all.at[:, block(source)], v_s, v_r, peer
        )

    in_group(lambda b, peer: v_copy(b, peer, member).start())
    v_all[:, block(member)] = v_own[:, member]

    acc = jnp.sum(spec_in[...] * back_out[...], axis=0)
    row = lax.broadcasted_iota(jnp.int32, acc.shape, 0)
    single = jnp.logical_and(me == first_device, lax.rem(row, slots) == 0)
    energy_h = jnp.sum(jnp.where(single, acc, 2.0 * acc)) * (0.5 / (8.0 * cells) / cells)
    lane = lax.broadcasted_iota(jnp.int32, partial.shape, 1)
    partial[...] = jnp.where(lane == 0, energy_xc, energy_h)

    def part_copy(peer, slot):
        return remote(partial, sums.at[slot], part_s, part_r, peer)

    around(lambda peer: part_copy(peer, me).start())
    sums[me] = partial[...]


    remote(back_out.at[others], back_in.at[others], back_s, back_r, me).wait_recv()
    high, low = split(back_in[...].reshape(depth * 2 * slots, width_x))
    hartree[...] = from_left(9, high, low)
    remote(v_own.at[:, mates], v_own.at[:, mates], v_s, v_r, me).wait_recv()
    remote(sums.at[others], sums.at[others], part_s, part_r, me).wait_recv()

    seven = main.at[:, mates]
    remote(seven, seven, main_s.at[0], main_r.at[0], me).wait_send()
    remote(halo_out.at[mates], halo_in.at[mates], halo_s, halo_r, me).wait_send()
    remote(seven, seven, v_s, v_r, me).wait_send()
    four = main.at[:, pl.ds(0, REACH)]

    @pl.when(has_near)
    def _():
        remote(four, four, main_s.at[1], main_r.at[0], me).wait_send()

    @pl.when(has_relay)
    def _():
        remote(four, four, relay_s, main_r.at[0], me).wait_send()

    remote(spec_out.at[others], spec_in.at[others], spec_s, spec_r, me).wait_send()
    remote(back_out.at[others], back_in.at[others], back_s, back_r, me).wait_send()
    remote(sums.at[others], sums.at[others], part_s, part_r, me).wait_send()

    @pl.when(exists_up)
    def _():
        flux_z_copy(0, me + group).wait_send()

    @pl.when(exists_down)
    def _():
        flux_z_copy(1, me - group).wait_send()

    @pl.when(right)
    def _():
        flux_y_copy(0, me + 1).wait_send()

    @pl.when(left)
    def _():
        flux_y_copy(1, me - 1).wait_send()

    @pl.when(me == edge_device)
    def _():
        remote(edge_out, edge_in, edge_s, edge_r, first_device).wait_send()


def join_kernel(hartree, v_all, sums, out, energies):
    out[0] = hartree[...] + v_all[0]
    out[1] = hartree[...] + v_all[1]
    both = jnp.sum(sums[...], axis=0)
    lane = lax.broadcasted_iota(jnp.int32, both.shape, 1)
    energies[0] = jnp.sum(jnp.where(lane == 0, both, 0.0))
    energies[1] = jnp.sum(jnp.where(lane == 1, both, 0.0))


def per_device(density, kernel_hat):
    planes, width_y, width_x = density.shape[1:]
    devices = lax.axis_size("gz")
    assert planes == 1
    group = 2 * REACH
    rows = width_y // group
    cells = devices * width_y * width_x
    count = kernel_hat.shape[1]
    half = count // 2
    slots = max(half, SUBLANES)
    tiles = width_x // LANES
    full = 2 * devices
    n1 = 1 << (full.bit_length() // 2)
    ty_high, ty_low, tb_high, tb_low = y_tables(width_y, devices, 1.0 / (8 * cells))
    tables = (
        ty_high,
        ty_low,
        turn_table(width_x),
        *slope_tables(width_x, rows),
        *x_tables(width_x),
        tb_high,
        tb_low,
    )
    packed, places = pack(tables)
    spec_shape = (devices, 2 * slots, width_x)
    tile_shape = (2, group, rows, width_x)
    tall_shape = (2, group + 2 * REACH, rows, width_x)
    f32 = functools.partial(pltpu.VMEM, dtype=jnp.float32)
    dma = pltpu.SemaphoreType.DMA
    scratch = [
        f32((2, width_y, width_x)),
        f32(kernel_hat.shape),
        pltpu.VMEM(packed.shape, packed.dtype),
        f32(spec_shape),
        f32(spec_shape),
        f32((group, 2, SUBLANES, width_x)),
        f32((group, 2, SUBLANES, width_x)),
        f32(tall_shape),
        f32(tile_shape),
        f32(tile_shape),
        f32(tile_shape),
        f32((KNOWN, group, rows, width_x)),
        f32(tall_shape),
        f32((group, 2, SUBLANES, width_x)),
        f32((2, group, 2, SUBLANES, width_x)),
        f32(tile_shape),
        f32((full, 2 * width_x)),
        f32((full, 2 * width_x)),
        f32((full, slots, width_x)),
        f32((full, 2 * tiles, slots, LANES)),
        f32((full, 2 * tiles, slots, LANES)),
        f32((devices, 2, 2 * tiles, slots, LANES)),
        f32((n1, full // n1, 2, slots, LANES)),
        f32((full, 2, 2 * tiles, slots, LANES)),
        f32((devices, 2, slots, 2 * width_x)),
        f32(spec_shape),
        f32(spec_shape),
        f32((1, LANES)),
        dma((5,)),
        *[dma] * 6,
        dma((2,)),
        dma((group + 2 * REACH,)),
        *[dma] * 3,
        *[dma((2,))] * 4,
        *[dma] * 4,
    ]
    held = sum(math.prod(part.shape) for part in scratch if hasattr(part, "memory_space"))
    limit = max(VMEM_BYTES, min(VMEM_MOST, 8 * held))
    pieces = pl.pallas_call(
        functools.partial(mega_kernel, devices, group, half, places),
        out_shape=(
            jax.ShapeDtypeStruct((width_y, width_x), jnp.float32),
            jax.ShapeDtypeStruct((2, width_y, width_x), jnp.float32),
            jax.ShapeDtypeStruct((devices, 1, LANES), jnp.float32),
        ),
        in_specs=[HBM_SPEC] * 3,
        out_specs=(VMEM_SPEC,) * 3,
        scratch_shapes=scratch,
        compiler_params=pltpu.CompilerParams(
            collective_id=0, has_side_effects=True, vmem_limit_bytes=limit
        ),
        name="potential",
    )(density.reshape(2, width_y, width_x), kernel_hat, packed)
    potential, energies = pl.pallas_call(
        join_kernel,
        out_shape=(
            jax.ShapeDtypeStruct((2, width_y, width_x), jnp.float32),
            jax.ShapeDtypeStruct((2,), jnp.float32),
        ),
        in_specs=[VMEM_SPEC] * 3,
        out_specs=(VMEM_SPEC, pl.BlockSpec(memory_space=pltpu.SMEM)),
        compiler_params=pltpu.CompilerParams(vmem_limit_bytes=8 << 20),
        name="join",
    )(*pieces)
    return potential.reshape(density.shape), energies


def solution(mesh):
    placed = (P(None, "gz", None, None), P(None, "gz", None))
    return jax.shard_map(
        per_device,
        mesh=mesh,
        in_specs=placed,
        out_specs=(P(None, "gz", None, None), P()),
        check_vma=False,
    )
```

```python
import functools
import math

import jax
import jax.numpy as jnp
import numpy as np
from jax import lax
from jax.experimental import pallas as pl
from jax.experimental.pallas import tpu as pltpu
from jax.sharding import PartitionSpec as P

HGRID = 0.35
STENCIL_WHOLE = (672.0, -168.0, 32.0, -3.0)
STENCIL_SCALE = 1.0 / (840.0 * HGRID)
REACH = len(STENCIL_WHOLE)
KAPPA = 0.804
MU_X = 0.2195149727645171
BETA_C = 0.06672455060314922
GAMMA_C = 0.031090690869654894
FZ_CURV = 1.709921
PARAMS_UNPOL = (0.031091, 0.2137, 7.5957, 3.5876, 1.6382, 0.49294)
PARAMS_POL = (0.015545, 0.20548, 14.1189, 6.1977, 3.3662, 0.62517)
PARAMS_STIFF = (0.016887, 0.11125, 10.357, 3.6231, 0.88026, 0.49671)

MESH = pl.DeviceIdType.MESH
LANES = 128
SUBLANES = 8
PACK = 256
VMEM_SPEC = pl.BlockSpec(memory_space=pltpu.VMEM)
HBM_SPEC = pl.BlockSpec(memory_space=pltpu.HBM)
VMEM_BYTES = 53 * 1024 * 1024
VMEM_MOST = 63 * 1024 * 1024
EARLY = 12
KNOWN = 11


def exchange_spin(dens, cube, sigma):
    factor = -0.75 * (3.0 / math.pi) ** (1.0 / 3.0) * 2.0 ** (1.0 / 3.0)
    scale = (3.0 * math.pi**2) ** (2.0 / 3.0) * 2.0 ** (8.0 / 3.0)
    product = dens * cube
    weight = product * product
    bent = (MU_X / (KAPPA * scale)) * sigma
    inverse = 1.0 / (weight + bent)
    share = weight * inverse
    rest = KAPPA * bent * inverse
    enhance = 1.0 + rest
    energy = factor * product * enhance
    by_dens = factor * cube * ((4.0 / 3.0) * enhance - (8.0 / 3.0) * rest * share)
    square = dens * dens * inverse
    by_sigma = (factor * MU_X / scale) * square * square
    return energy, by_dens, by_sigma


def pw_piece(root, square, params):
    amp, alpha, b1, b2, b3, b4 = params
    doubled = 2.0 * amp
    series = root * (doubled * b1 + root * (doubled * b2 + root * (doubled * b3 + root * (doubled * b4))))
    slope = doubled * b1 + root * (
        2.0 * doubled * b2 + root * (3.0 * doubled * b3 + root * (4.0 * doubled * b4))
    )
    above = series + 1.0
    inverse = 1.0 / (series * above)
    logarithm = jnp.log(above * above * inverse)
    front = -doubled - (doubled * alpha) * square
    value = front * logarithm
    by_root = (-2.0 * doubled * alpha) * root * logarithm - front * slope * inverse
    return value, by_root


def xc_density(up, down):
    inverse_u = jnp.exp(jnp.log(up) * (-1.0 / 3.0))
    inverse_d = jnp.exp(jnp.log(down) * (-1.0 / 3.0))
    cube_u = up * inverse_u * inverse_u
    cube_d = down * inverse_d * inverse_d
    total = up + down
    sixth = jnp.exp(jnp.log(total) * (-1.0 / 6.0))
    inverse_cube = sixth * sixth
    wigner = (3.0 / (4.0 * math.pi)) ** (1.0 / 3.0)
    root = math.sqrt(wigner) * sixth
    square = wigner * inverse_cube
    inverse_square = inverse_cube * inverse_cube
    inverse_total = inverse_square * inverse_cube
    cube = total * inverse_square
    zeta = (up - down) * inverse_total
    plus = 1.0 + zeta
    minus = 1.0 - zeta
    third = 2.0 ** (1.0 / 3.0)
    plus_cube = third * cube_u * inverse_cube
    minus_cube = third * cube_d * inverse_cube
    spin = 1.0 / (2.0 ** (4.0 / 3.0) - 2.0)
    weight = (plus * plus_cube + minus * minus_cube - 2.0) * spin
    by_weight = (4.0 / 3.0 * spin) * (plus_cube - minus_cube)
    unpol, unpol_root = pw_piece(root, square, PARAMS_UNPOL)
    pol, pol_root = pw_piece(root, square, PARAMS_POL)
    stiff, stiff_root = pw_piece(root, square, PARAMS_STIFF)
    stiff = stiff * (-1.0 / FZ_CURV)
    stiff_root = stiff_root * (-1.0 / FZ_CURV)
    zeta_two = zeta * zeta
    zeta_four = zeta_two * zeta_two
    gap = pol - unpol - stiff
    mixed = stiff + gap * zeta_four
    mixed_root = stiff_root + (pol_root - unpol_root - stiff_root) * zeta_four
    local = unpol + weight * mixed
    local_root = unpol_root + weight * mixed_root
    local_zeta = by_weight * mixed + weight * gap * (4.0 * zeta_two * zeta)
    phi = 0.5 * (plus_cube * plus_cube + minus_cube * minus_cube)
    by_phi = (2.0 ** (-1.0 / 3.0) / 3.0) * cube * (inverse_u - inverse_d)
    inverse_phi = 1.0 / phi
    phi_square = inverse_phi * inverse_phi
    inverse_gamma = phi_square * inverse_phi * (1.0 / GAMMA_C)
    gamma_phi = GAMMA_C * phi * phi * phi
    ratio = BETA_C / GAMMA_C
    expo = -local * inverse_gamma
    weight_a = ratio / (jnp.exp(expo) - 1.0)
    scale = math.pi / (16.0 * (3.0 * math.pi**2) ** (1.0 / 3.0))
    to_t = scale * phi_square * (inverse_square * inverse_cube) * (inverse_square * inverse_square)
    slope = (1.0 / 6.0) * root * local_root
    return (
        cube_u, cube_d, zeta, local, slope, local_zeta, by_phi, inverse_phi, gamma_phi, weight_a, to_t
    )


def xc_gradient(up, down, given, sigma_uu, sigma_ud, sigma_dd):
    cube_u, cube_d, zeta, local, slope, local_zeta, by_phi, inverse_phi, gamma_phi, weight_a, to_t = given
    energy_u, vx_u, by_uu = exchange_spin(up, cube_u, sigma_uu)
    energy_d, vx_d, by_dd = exchange_spin(down, cube_d, sigma_dd)
    total = up + down
    ratio = BETA_C / GAMMA_C
    inverse_gamma = inverse_phi * inverse_phi * inverse_phi * (1.0 / GAMMA_C)
    expo = -local * inverse_gamma
    sigma = sigma_uu + 2.0 * sigma_ud + sigma_dd
    tee = sigma * to_t
    why = weight_a * tee
    numer = 1.0 + why
    denom = 1.0 + why * numer
    scaled = ratio * tee
    upper = denom + scaled * numer
    inverse = 1.0 / (denom * upper)
    gradient = gamma_phi * jnp.log(upper * upper * inverse)
    shared = gamma_phi * inverse
    by_tee = ratio * shared * (numer + why)
    by_a = shared * scaled * tee * why * (numer + 1.0)
    chain = by_a * weight_a * (1.0 + weight_a * (1.0 / ratio))
    by_local = 1.0 - chain * inverse_gamma
    tee_part = tee * by_tee
    phi_part = (3.0 * gradient - 3.0 * expo * chain - 2.0 * tee_part) * inverse_phi
    corr = local + gradient
    by_total = corr - slope * by_local - (7.0 / 3.0) * tee_part
    by_zeta = by_local * local_zeta + phi_part * by_phi
    by_sigma = total * by_tee * to_t
    energy = energy_u + energy_d + total * corr
    return (
        energy,
        vx_u + by_total + by_zeta * (1.0 - zeta),
        vx_d + by_total - by_zeta * (1.0 + zeta),
        by_uu + by_sigma,
        2.0 * by_sigma,
        by_dd + by_sigma,
    )


def np_split(table):
    table = np.asarray(table, np.float32)
    high = table.astype(jnp.bfloat16)
    low = (table - high.astype(np.float32)).astype(jnp.bfloat16)
    return high, low


def y_tables(width_y, devices, scale):
    period = 2 * width_y
    count = period // devices
    half = count // 2
    slots = max(half, SUBLANES)
    device = np.arange(devices)[:, None]
    ky = device * count + np.arange(half)[None, :] + (device >= devices // 2)
    space = np.arange(width_y)
    angle = (ky[:, :, None] * space % period) * (2.0 * np.pi / period)
    both = np.stack([np.cos(angle), -np.sin(angle)], axis=1)
    both[0, 1, 0] = (-1.0) ** space
    weight = np.full((devices, 2, half, 1), 2.0)
    weight[0, :, 0] = 1.0
    pad = [(0, 0), (0, 0), (0, slots - half), (0, 0)]
    forward = np.pad(both, pad).reshape(devices * 2 * slots, width_y)
    back = np.pad(both * weight, pad).reshape(devices * 2 * slots, width_y)
    return *np_split(forward), *np_split(back.T * scale)


def x_tables(width_x):
    index = np.outer(np.arange(width_x), np.arange(width_x)) % (2 * width_x)
    angle = index * (np.pi / width_x)
    cos, sin = np.cos(angle), np.sin(angle)
    sin[:, 0] = (-1.0) ** np.arange(width_x)
    fore = np.concatenate([cos, sin], axis=1)
    back = np.concatenate([cos, sin.T], axis=0)
    return *np_split(fore), *np_split(back)


def stencil_matrix(size):
    table = np.zeros((size, size + 2 * REACH), np.float32)
    for row in range(size):
        for step, weight in enumerate(STENCIL_WHOLE, 1):
            table[row, row + REACH + step] = weight
            table[row, row + REACH - step] = -weight
    return table


def slope_tables(width_x, rows):
    wide = stencil_matrix(width_x)[:, REACH : REACH + width_x].T
    table = stencil_matrix(rows)
    inner = table[:, REACH : REACH + rows]
    below, above = table[:, :REACH], table[:, REACH + rows :]
    pad = np.zeros((rows, -(rows + 2 * REACH) % 16), np.float32)
    tall = np.concatenate([inner, above, below, pad], axis=1)
    tall = np.concatenate([tall] * 3, axis=1)
    tall = np.pad(tall, [(0, 0), (0, -tall.shape[1] % PACK)])
    return wide.astype(jnp.bfloat16), tall.astype(jnp.bfloat16)


def turn_table(width_x):
    table = np.zeros((width_x, width_x), np.float32)
    lanes = np.arange(width_x)
    table[(width_x - lanes) % width_x, lanes] = 1.0
    return table.astype(jnp.bfloat16)


def pack(tables):
    blocks, places, row = [], [], 0
    for table in tables:
        starts = []
        for column in range(0, table.shape[1], PACK):
            starts.append(row)
            blocks.append(table[:, column : column + PACK])
            row += table.shape[0]
        places.append((table.shape[0], tuple(starts)))
    return np.concatenate(blocks, axis=0), tuple(places)


def dot(left, right):
    return jnp.dot(left, right, preferred_element_type=jnp.float32)


def split(value):
    high = value.astype(jnp.bfloat16)
    low = (value - high.astype(jnp.float32)).astype(jnp.bfloat16)
    return high, low


def split_three(value):
    high = value.astype(jnp.bfloat16)
    rest = value - high.astype(jnp.float32)
    middle = rest.astype(jnp.bfloat16)
    low = (rest - middle.astype(jnp.float32)).astype(jnp.bfloat16)
    return high, middle, low


def dot_exact(value, table):
    high, middle, low = split_three(value)
    return dot(high, table) + (dot(middle, table) + dot(low, table))


def add(left, right):
    if left is None or right is None:
        return left if right is None else right
    return left[0] + right[0], left[1] + right[1]


def sub(left, right):
    if right is None:
        return left
    return left[0] - right[0], left[1] - right[1]


def turn(value, numer, denom, sign):
    if value is None:
        return None
    numer = numer * sign % denom
    eighth = numer * 8
    re, im = value
    if eighth % (2 * denom) == 0:
        quarter = eighth // (2 * denom)
        return ((re, im), (-im, re), (-re, -im), (im, -re))[quarter]
    if eighth % denom == 0:
        root = math.sqrt(0.5)
        plus, minus = root * (re + im), root * (re - im)
        return {1: (minus, plus), 3: (-plus, minus), 5: (-minus, -plus), 7: (plus, -minus)}[eighth // denom]
    cos = math.cos(2.0 * math.pi * numer / denom)
    sin = math.sin(2.0 * math.pi * numer / denom)
    return cos * re - sin * im, sin * re + cos * im


def small_dft(values, sign, first_half=False):
    count = len(values)
    if count == 1:
        return values
    even = small_dft(values[0::2], sign)
    odd = small_dft(values[1::2], sign)
    odd = [turn(value, k, count, sign) for k, value in enumerate(odd)]
    out = [add(e, o) for e, o in zip(even, odd)]
    if not first_half:
        out += [sub(e, o) for e, o in zip(even, odd)]
    return out


def mega_kernel(
    devices,
    group,
    half,
    places,
    *refs,
):
    dens_hbm, khat_hbm, table_hbm, hartree, v_all, sums, dens, khat, table = refs[:9]
    (
        spec_out,
        spec_in,
        halo_out,
        halo_in,
        main,
        grad_x,
        grad_y,
        grad_z,
        known,
        flux_z,
        flux_out,
        flux_in,
        v_own,
        edge_out,
        edge_in,
        k_raw,
        k_self,
        k_cross,
        z_in,
        z_mid,
        h_spec,
        x_in,
        back_out,
        back_in,
        partial,
        local_sems,
        spec_s,
        spec_r,
        back_s,
        back_r,
        part_s,
        part_r,
        main_s,
        main_r,
        relay_s,
        halo_s,
        halo_r,
        fz_s,
        fz_r,
        fy_s,
        fy_r,
        v_s,
        v_r,
        edge_s,
        edge_r,
    ) = refs[9:]
    me = lax.axis_index("gz")
    level, member = lax.div(me, group), lax.rem(me, group)
    levels = devices // group
    base = level * group
    width_y, width_x = dens.shape[1:]
    rows = width_y // group
    tiles = width_x // LANES
    depth = devices
    slots = spec_out.shape[1] // 2
    first_device, edge_device = 0, devices // 2
    cells = depth * width_y * width_x

    barrier = pltpu.get_barrier_semaphore()

    def greet(step, carry):
        pl.semaphore_signal(
            barrier, inc=1, device_id=(lax.rem(me + step, devices),), device_id_type=MESH
        )
        return carry

    lax.fori_loop(1, devices, greet, 0)

    cuts = (0, places[2][1][0], places[5][1][0], table.shape[0])
    pairs = [(dens_hbm, dens)]
    pairs += [
        (table_hbm.at[low:high], table.at[low:high]) for low, high in zip(cuts, cuts[1:])
    ]
    pairs.insert(2, (khat_hbm, khat))
    loads = [
        pltpu.make_async_copy(source, target, local_sems.at[i])
        for i, (source, target) in enumerate(pairs)
    ]
    for copy in loads:
        copy.start()

    def blocks(index):
        count, starts = places[index]
        return [table[start : start + count] for start in starts]

    def from_left(index, high, low):
        result = 0.0
        for k, (t_high, t_low) in enumerate(zip(blocks(index), blocks(index + 1))):
            part = slice(k * PACK, k * PACK + t_high.shape[1])
            upper, lower = high[part], low[part]
            result = result + (dot(t_high, upper) + (dot(t_high, lower) + dot(t_low, upper)))
        return result

    def from_right(index, high, low):
        return [
            dot(high, t_high) + (dot(low, t_high) + dot(high, t_low))
            for t_high, t_low in zip(blocks(index), blocks(index + 1))
        ]

    def remote(source, target, send, receive, peer):
        return pltpu.make_async_remote_copy(
            src_ref=source,
            dst_ref=target,
            send_sem=send,
            recv_sem=receive,
            device_id=(peer,),
            device_id_type=MESH,
        )

    loads[0].wait()
    sub_row = lax.broadcasted_iota(jnp.int32, (1, SUBLANES, width_x), 1)
    for b in range(group):
        above = dens[:, (b + 1) * rows : (b + 1) * rows + SUBLANES] if b < group - 1 else 0.0
        below = dens[:, b * rows - SUBLANES : b * rows] if b else 0.0
        halo_out[b] = jnp.where(sub_row < REACH, above, below)

    pl.semaphore_wait(barrier, devices - 1)

    upper = member >= REACH
    own_half = jnp.where(upper, REACH, 0)
    far_half = REACH - own_half
    near = jnp.where(upper, level + 1, level - 1)
    relay = jnp.where(upper, level - 1, level + 1)
    has_near = jnp.logical_and(near >= 0, near < levels)
    has_relay = jnp.logical_and(relay >= 0, relay < levels)

    def beyond(plane):
        return jnp.where(plane >= REACH, plane - (group - REACH), REACH + group + plane)

    def block(b):
        return pl.ds(pl.multiple_of(b * rows, rows), rows)

    def main_copy(b, peer, slot, which):
        return remote(
            dens.at[:, block(b)], main.at[:, slot], main_s.at[which], main_r.at[slot], peer
        )

    def halo_copy(b, peer, source):
        return remote(
            halo_out.at[b], halo_in.at[source], halo_s, halo_r, peer
        )

    def in_group(act):
        def body(step, carry):
            b = lax.rem(member + step, group)
            act(b, base + b)
            return carry

        lax.fori_loop(1, group, body, 0)

    def start_main(b, peer):
        main_copy(b, peer, REACH + member, 0).start()
        halo_copy(b, peer, member).start()

    def near_each(act):
        @pl.when(has_near)
        def _():
            def body(step, carry):
                b = own_half + lax.rem(member + step, REACH)
                act(main_copy(b, near * group + b, beyond(member), 1))
                return carry

            lax.fori_loop(0, REACH, body, 0)

    def relay_copy(step):
        plane = far_half + lax.rem(member + REACH - step, REACH)
        return plane, remote(
            main.at[:, REACH + plane],
            main.at[:, beyond(plane)],
            relay_s,
            main_r.at[beyond(plane)],
            relay * group + member,
        )

    near_each(lambda copy: copy.start())

    def start_far(step, carry):
        b = far_half + lax.rem(member + step, REACH)
        start_main(b, base + b)
        return carry

    def start_own(step, carry):
        b = own_half + lax.rem(member + step, REACH)
        start_main(b, base + b)
        return carry

    lax.fori_loop(0, REACH, start_far, 0)
    lax.fori_loop(1, REACH, start_own, 0)

    loads[1].wait()
    high, low = split(dens[0] + dens[1])
    spec_out[...] = from_left(0, high, low).reshape(spec_out.shape)

    def spec_copy(peer, slot):
        return remote(
            spec_out.at[peer], spec_in.at[slot], spec_s, spec_r, peer
        )

    crossing = group * (levels - 1)

    def around(act, first=0, last=devices - 1):
        def body(index, carry):
            inner = index >= crossing
            away = lax.rem(lax.div(index, group), levels - 1)
            hop = lax.div(away + 1, 2)
            hop = levels // 2 + jnp.where(lax.rem(away, 2) == 0, hop, -hop)
            turn_by = jnp.where(inner, index - crossing + 1, lax.rem(index, group))
            hop = jnp.where(inner, 0, hop)
            act(lax.rem(level + hop, levels) * group + lax.rem(member + turn_by, group))
            return carry

        lax.fori_loop(first, last, body, 0)

    def start_spec(peer):
        spec_copy(peer, me).start()

    around(start_spec, last=EARLY)
    loads[2].wait()

    @pl.when(me == edge_device)
    def _():
        edge_out[...] = khat[:, 0, :]
        remote(edge_out, edge_in, edge_s, edge_r, first_device).start()
    main[:, REACH + member] = dens[:, block(member)]
    halo_in[member] = halo_out[member]
    spec_in[me] = spec_out[me]

    zero_planes = jnp.zeros((2, REACH, rows, width_x), jnp.float32)

    @pl.when(level == 0)
    def _():
        main[:, :REACH] = zero_planes
        flux_z[:, :REACH] = zero_planes

    @pl.when(level == levels - 1)
    def _():
        main[:, REACH + group :] = zero_planes
        flux_z[:, REACH + group :] = zero_planes

    loads[3].wait()
    (t_turn,), (t_wide,), (t_tall,) = blocks(2), blocks(3), blocks(4)
    lower = me < edge_device
    planes_k = khat.shape[0]
    if slots > half:
        k_raw[...] = jnp.ones(k_raw.shape, jnp.float32)

    def pick(kz, carry):
        row = jnp.where(lower, khat[kz, :half], khat[kz, 1 : half + 1])
        for t in range(tiles):
            k_self[kz, t, :half] = row[:, t * LANES : (t + 1) * LANES]
        k_raw[kz, :half] = row[:, width_x:]
        if slots > half:
            for t in range(tiles):
                k_self[kz, t, half:] = jnp.ones((slots - half, LANES), jnp.float32)
        return carry

    lax.fori_loop(0, planes_k, pick, 0)
    turned = dot_exact(k_raw[...].reshape(planes_k * slots, width_x), t_turn)
    turned = turned.reshape(planes_k, slots, width_x)
    for t in range(tiles):
        k_self[:, tiles + t] = turned[:, :, t * LANES : (t + 1) * LANES]

    def clear(kz, carry):
        k_cross[kz] = jnp.zeros(k_cross.shape[1:], jnp.float32)
        return carry

    lax.fori_loop(0, planes_k, clear, 0)

    def finish_main(b, peer):
        main_copy(b, peer, REACH + b, 0).wait_recv()

    def finish_far(step, carry):
        plane, copy = relay_copy(step)
        finish_main(plane, base + plane)

        @pl.when(has_relay)
        def _():
            copy.start()

        return carry

    lax.fori_loop(0, REACH, finish_far, 0)
    around(start_spec, first=EARLY)
    chunk = 2 * SUBLANES

    def density_part(plane):
        def body(index, carry):
            at = pl.ds(pl.multiple_of(index * chunk, chunk), chunk)
            parts = xc_density(main[0, REACH + plane, at], main[1, REACH + plane, at])
            for i, part in enumerate(parts):
                known[i, plane, at] = part
            return carry

        lax.fori_loop(0, rows // chunk, body, 0)

    def density_far(step, carry):
        density_part(far_half + step)
        return carry

    density_part(member)
    lax.fori_loop(0, REACH, density_far, 0)

    def finish_own(step, carry):
        b = own_half + lax.rem(member + step, REACH)
        finish_main(b, base + b)
        density_part(b)
        return carry

    lax.fori_loop(1, REACH, finish_own, 0)
    mates = pl.ds(0, group - 1)
    remote(halo_out.at[mates], halo_in.at[mates], halo_s, halo_r, me).wait_recv()

    def slope_z(field, spin, plane):
        result = 0.0
        for step, weight in enumerate(STENCIL_WHOLE, 1):
            result = result + (weight * STENCIL_SCALE) * (
                field[spin, plane + REACH + step] - field[spin, plane + REACH - step]
            )
        return result

    pad_rows = -(rows + SUBLANES) % 16
    tall = 3 * (rows + SUBLANES + pad_rows)

    def slope_y(inner, outer):
        parts = [inner, outer]
        if pad_rows:
            parts.append(jnp.zeros((pad_rows, width_x), jnp.float32))
        stacked = jnp.concatenate(split_three(jnp.concatenate(parts, axis=0)), axis=0)
        return dot(t_tall[:, :tall], stacked) * STENCIL_SCALE

    def slope_x(field):
        value = field.reshape(group * rows, width_x)
        return (dot_exact(value, t_wide) * STENCIL_SCALE).reshape(group, rows, width_x)

    for spin in range(2):
        grad_x[spin] = slope_x(main[spin, REACH : REACH + group])

    def gradients(plane, carry):
        for spin in range(2):
            grad_y[spin, plane] = slope_y(main[spin, REACH + plane], halo_in[plane, spin])
        return carry

    lax.fori_loop(0, group, gradients, 0)
    def near_wait(first):
        def body(step, carry):
            main_copy(member, me, first + step, 1).wait_recv()
            return carry

        lax.fori_loop(0, REACH, body, 0)

    @pl.when(level > 0)
    def _():
        near_wait(0)

    @pl.when(level < levels - 1)
    def _():
        near_wait(REACH + group)


    def gradients_z(plane, carry):
        for spin in range(2):
            grad_z[spin, plane] = slope_z(main, spin, plane)
        return carry

    lax.fori_loop(0, group, gradients_z, 0)


    def point(index, acc):
        plane = lax.div(index, rows // chunk)
        at = pl.ds(pl.multiple_of(lax.rem(index, rows // chunk) * chunk, chunk), chunk)
        uz, uy, ux = grad_z[0, plane, at], grad_y[0, plane, at], grad_x[0, plane, at]
        dz, dy, dx = grad_z[1, plane, at], grad_y[1, plane, at], grad_x[1, plane, at]
        energy, d_up, d_down, d_uu, d_ud, d_dd = xc_gradient(
            main[0, REACH + plane, at],
            main[1, REACH + plane, at],
            [known[i, plane, at] for i in range(KNOWN)],
            uz * uz + uy * uy + ux * ux,
            uz * dz + uy * dy + ux * dx,
            dz * dz + dy * dy + dx * dx,
        )
        v_own[0, plane, at] = d_up
        v_own[1, plane, at] = d_down
        d_uu = 2.0 * d_uu
        d_dd = 2.0 * d_dd
        flux_z[0, REACH + plane, at] = d_uu * uz + d_ud * dz
        flux_z[1, REACH + plane, at] = d_dd * dz + d_ud * uz
        grad_y[0, plane, at] = d_uu * uy + d_ud * dy
        grad_y[1, plane, at] = d_dd * dy + d_ud * uy
        grad_x[0, plane, at] = d_uu * ux + d_ud * dx
        grad_x[1, plane, at] = d_dd * dx + d_ud * ux
        return acc + energy

    def flux_z_copy(side, peer):
        source = (slice(group, group + REACH), slice(REACH, 2 * REACH))[side]
        target = (slice(0, REACH), slice(REACH + group, 2 * REACH + group))[side]
        return remote(
            flux_z.at[:, source], flux_z.at[:, target], fz_s.at[side], fz_r.at[side], peer
        )

    def flux_y_copy(side, peer):
        return remote(flux_out, flux_in.at[side], fy_s.at[side], fy_r.at[side], peer)

    exists_up, exists_down = level < levels - 1, level > 0
    right, left = member < group - 1, member > 0

    steps = group * rows // chunk
    energy_acc = jnp.zeros((chunk, width_x), jnp.float32)
    energy_acc = lax.fori_loop(steps // 2, steps, point, energy_acc)

    @pl.when(exists_up)
    def _():
        flux_z_copy(0, me + group).start()

    energy_acc = lax.fori_loop(0, steps // 2, point, energy_acc)

    @pl.when(exists_down)
    def _():
        flux_z_copy(1, me - group).start()

    energy_xc = jnp.sum(energy_acc) * (1.0 / cells)
    for spin in range(2):
        flux_out[:, spin] = jnp.where(
            sub_row < REACH, grad_y[spin, :, :SUBLANES], grad_y[spin, :, rows - SUBLANES :]
        )

    @pl.when(right)
    def _():
        flux_y_copy(0, me + 1).start()

    @pl.when(left)
    def _():
        flux_y_copy(1, me - 1).start()

    @pl.when(me == first_device)
    def _():
        remote(edge_out, edge_in, edge_s, edge_r, edge_device).wait_recv()
        edge_out[:, :width_x] = edge_in[:, :width_x]
        edge_out[:, width_x:] = dot_exact(edge_in[:, width_x:], t_turn)
        top = lax.broadcasted_iota(jnp.int32, (slots, LANES), 0) == 0

        def mix(kz, carry):
            other = edge_out[pl.ds(kz, 1), :]
            for t in range(2 * tiles):
                mine = k_self[kz, t]
                theirs = other[:, t * LANES : (t + 1) * LANES]
                k_self[kz, t] = jnp.where(top, 0.5 * (mine + theirs), mine)
                k_cross[kz, t] = jnp.where(top, 0.5 * (mine - theirs), 0.0)
            return carry

        lax.fori_loop(0, planes_k, mix, 0)

    for spin in range(2):
        v_own[spin] = v_own[spin] - slope_x(grad_x[spin])

    loads[4].wait()
    others = pl.ds(0, devices - 1)
    remote(spec_out.at[others], spec_in.at[others], spec_s, spec_r, me).wait_recv()
    lane = lax.broadcasted_iota(jnp.int32, (1, 1, width_x), 2)
    first = lane == 0
    high, low = split(spec_in[...].reshape(depth * 2 * slots, width_x))
    wide = jnp.concatenate(from_right(5, high, low), axis=1)
    wide = wide.reshape(depth, 2, slots, 2 * width_x)
    cos_re, cos_im = wide[:, 0, :, :width_x], wide[:, 1, :, :width_x]
    sin_re, sin_im = wide[:, 0, :, width_x:], wide[:, 1, :, width_x:]
    fields = (
        (jnp.where(first, cos_re, cos_re + sin_im), jnp.where(first, cos_im, cos_im - sin_re)),
        (jnp.where(first, sin_re, cos_re - sin_im), jnp.where(first, sin_im, cos_im + sin_re)),
    )
    for sign in range(2):
        for part in range(2):
            for t in range(tiles):
                z_in[:, part, sign * tiles + t] = fields[sign][part][
                    :, :, t * LANES : (t + 1) * LANES
                ]

    n1, n2 = z_mid.shape[:2]
    full = n1 * n2

    def load(ref, *at):
        return ref[at[0], 0, at[1]], ref[at[0], 1, at[1]]

    def fore(col, carry):
        for j in range(n2):
            given = [load(z_in, n2 * i + j, col) for i in range(n1 // 2)]
            for k, value in enumerate(small_dft(given + [None] * (n1 // 2), -1)):
                re, im = turn(value, k * j, full, -1)
                z_mid[k, j, 0] = re
                z_mid[k, j, 1] = im
        for k in range(n1):
            given = [(z_mid[k, j, 0], z_mid[k, j, 1]) for j in range(n2)]
            for m, (re, im) in enumerate(small_dft(given, -1)):
                h_spec[k + n1 * m, 0, col] = re
                h_spec[k + n1 * m, 1, col] = im
        return carry

    lax.fori_loop(0, 2 * tiles, fore, 0)
    lane = lax.broadcasted_iota(jnp.int32, (slots, LANES), 1)

    def back(col, carry):
        other = lax.rem(col + tiles, 2 * tiles)
        alone = jnp.logical_and(lane == 0, lax.rem(col, tiles) == 0)
        for k in range(n1):
            given = []
            for m in range(n2):
                kz = k + n1 * m
                flip = (full - kz) % full
                re, im = load(h_spec, kz, col)
                own_re, own_im = load(h_spec, flip, col)
                far_re, far_im = load(h_spec, flip, other)
                far_re = jnp.where(alone, own_re, far_re)
                far_im = jnp.where(alone, own_im, far_im)
                direct, cross = k_self[kz, col], k_cross[kz, col]
                given.append((direct * re + cross * far_re, direct * im - cross * far_im))
            for j, value in enumerate(small_dft(given, 1)):
                re, im = turn(value, k * j, full, 1)
                z_mid[k, j, 0] = re
                z_mid[k, j, 1] = im
        for j in range(n2):
            given = [(z_mid[k, j, 0], z_mid[k, j, 1]) for k in range(n1)]
            for i, (re, im) in enumerate(small_dft(given, 1, first_half=True)):
                z_in[n2 * i + j, 0, col] = re
                z_in[n2 * i + j, 1, col] = im
        return carry

    lax.fori_loop(0, 2 * tiles, back, 0)
    for t in range(tiles):
        keep = lax.broadcasted_iota(jnp.int32, (1, 1, LANES), 2) + t * LANES == 0
        plus_re, plus_im = z_in[:, 0, t], z_in[:, 1, t]
        minus_re, minus_im = z_in[:, 0, tiles + t], z_in[:, 1, tiles + t]
        here = slice(t * LANES, (t + 1) * LANES)
        there = slice(width_x + t * LANES, width_x + (t + 1) * LANES)
        x_in[:, 0, :, here] = jnp.where(keep, plus_re, plus_re + minus_re)
        x_in[:, 1, :, here] = jnp.where(keep, plus_im, plus_im + minus_im)
        x_in[:, 0, :, there] = jnp.where(keep, minus_re, minus_im - plus_im)
        x_in[:, 1, :, there] = jnp.where(keep, minus_im, plus_re - minus_re)
    high, low = split(x_in[...].reshape(depth * 2 * slots, 2 * width_x))
    back_out[...] = jnp.concatenate(from_right(7, high, low), axis=1).reshape(back_out.shape)

    def back_copy(peer, slot):
        return remote(
            back_out.at[peer], back_in.at[slot], back_s, back_r, peer
        )

    around(lambda peer: back_copy(peer, me).start(), last=crossing)
    around(lambda peer: back_copy(peer, me).start(), first=crossing)
    back_in[me] = back_out[me]

    @pl.when(left)
    def _():
        flux_y_copy(0, me).wait_recv()

    @pl.when(right)
    def _():
        flux_y_copy(1, me).wait_recv()

    @pl.when(jnp.logical_not(left))
    def _():
        flux_in[0] = jnp.zeros(flux_in.shape[1:], jnp.float32)

    @pl.when(jnp.logical_not(right))
    def _():
        flux_in[1] = jnp.zeros(flux_in.shape[1:], jnp.float32)

    def divergence(plane, carry):
        for spin in range(2):
            outer = jnp.where(sub_row[0] < REACH, flux_in[1, plane, spin], flux_in[0, plane, spin])
            v_own[spin, plane] = v_own[spin, plane] - slope_y(grad_y[spin, plane], outer)
        return carry

    lax.fori_loop(0, group, divergence, 0)

    @pl.when(exists_down)
    def _():
        flux_z_copy(0, me).wait_recv()

    @pl.when(exists_up)
    def _():
        flux_z_copy(1, me).wait_recv()

    def divergence_z(plane, carry):
        for spin in range(2):
            v_own[spin, plane] = v_own[spin, plane] - slope_z(flux_z, spin, plane)
        return carry

    lax.fori_loop(0, group, divergence_z, 0)
    def v_copy(b, peer, source):
        return remote(
            v_own.at[:, b], v_all.at[:, block(source)], v_s, v_r, peer
        )

    in_group(lambda b, peer: v_copy(b, peer, member).start())
    v_all[:, block(member)] = v_own[:, member]

    acc = jnp.sum(spec_in[...] * back_out[...], axis=0)
    row = lax.broadcasted_iota(jnp.int32, acc.shape, 0)
    single = jnp.logical_and(me == first_device, lax.rem(row, slots) == 0)
    energy_h = jnp.sum(jnp.where(single, acc, 2.0 * acc)) * (0.5 / (8.0 * cells) / cells)
    lane = lax.broadcasted_iota(jnp.int32, partial.shape, 1)
    partial[...] = jnp.where(lane == 0, energy_xc, energy_h)

    def part_copy(peer, slot):
        return remote(partial, sums.at[slot], part_s, part_r, peer)

    around(lambda peer: part_copy(peer, me).start())
    sums[me] = partial[...]


    remote(back_out.at[others], back_in.at[others], back_s, back_r, me).wait_recv()
    high, low = split(back_in[...].reshape(depth * 2 * slots, width_x))
    hartree[...] = from_left(9, high, low)
    remote(v_own.at[:, mates], v_own.at[:, mates], v_s, v_r, me).wait_recv()
    remote(sums.at[others], sums.at[others], part_s, part_r, me).wait_recv()

    seven = main.at[:, mates]
    remote(seven, seven, main_s.at[0], main_r.at[0], me).wait_send()
    remote(halo_out.at[mates], halo_in.at[mates], halo_s, halo_r, me).wait_send()
    remote(seven, seven, v_s, v_r, me).wait_send()
    four = main.at[:, pl.ds(0, REACH)]

    @pl.when(has_near)
    def _():
        remote(four, four, main_s.at[1], main_r.at[0], me).wait_send()

    @pl.when(has_relay)
    def _():
        remote(four, four, relay_s, main_r.at[0], me).wait_send()

    remote(spec_out.at[others], spec_in.at[others], spec_s, spec_r, me).wait_send()
    remote(back_out.at[others], back_in.at[others], back_s, back_r, me).wait_send()
    remote(sums.at[others], sums.at[others], part_s, part_r, me).wait_send()

    @pl.when(exists_up)
    def _():
        flux_z_copy(0, me + group).wait_send()

    @pl.when(exists_down)
    def _():
        flux_z_copy(1, me - group).wait_send()

    @pl.when(right)
    def _():
        flux_y_copy(0, me + 1).wait_send()

    @pl.when(left)
    def _():
        flux_y_copy(1, me - 1).wait_send()

    @pl.when(me == edge_device)
    def _():
        remote(edge_out, edge_in, edge_s, edge_r, first_device).wait_send()


def join_kernel(hartree, v_all, sums, out, energies):
    out[0] = hartree[...] + v_all[0]
    out[1] = hartree[...] + v_all[1]
    both = jnp.sum(sums[...], axis=0)
    lane = lax.broadcasted_iota(jnp.int32, both.shape, 1)
    energies[0] = jnp.sum(jnp.where(lane == 0, both, 0.0))
    energies[1] = jnp.sum(jnp.where(lane == 1, both, 0.0))


def per_device(density, kernel_hat):
    planes, width_y, width_x = density.shape[1:]
    devices = lax.axis_size("gz")
    assert planes == 1
    group = 2 * REACH
    rows = width_y // group
    cells = devices * width_y * width_x
    count = kernel_hat.shape[1]
    half = count // 2
    slots = max(half, SUBLANES)
    tiles = width_x // LANES
    full = 2 * devices
    n1 = 1 << (full.bit_length() // 2)
    ty_high, ty_low, tb_high, tb_low = y_tables(width_y, devices, 1.0 / (8 * cells))
    tables = (
        ty_high,
        ty_low,
        turn_table(width_x),
        *slope_tables(width_x, rows),
        *x_tables(width_x),
        tb_high,
        tb_low,
    )
    packed, places = pack(tables)
    spec_shape = (devices, 2 * slots, width_x)
    tile_shape = (2, group, rows, width_x)
    tall_shape = (2, group + 2 * REACH, rows, width_x)
    f32 = functools.partial(pltpu.VMEM, dtype=jnp.float32)
    dma = pltpu.SemaphoreType.DMA
    scratch = [
        f32((2, width_y, width_x)),
        f32(kernel_hat.shape),
        pltpu.VMEM(packed.shape, packed.dtype),
        f32(spec_shape),
        f32(spec_shape),
        f32((group, 2, SUBLANES, width_x)),
        f32((group, 2, SUBLANES, width_x)),
        f32(tall_shape),
        f32(tile_shape),
        f32(tile_shape),
        f32(tile_shape),
        f32((KNOWN, group, rows, width_x)),
        f32(tall_shape),
        f32((group, 2, SUBLANES, width_x)),
        f32((2, group, 2, SUBLANES, width_x)),
        f32(tile_shape),
        f32((full, 2 * width_x)),
        f32((full, 2 * width_x)),
        f32((full, slots, width_x)),
        f32((full, 2 * tiles, slots, LANES)),
        f32((full, 2 * tiles, slots, LANES)),
        f32((devices, 2, 2 * tiles, slots, LANES)),
        f32((n1, full // n1, 2, slots, LANES)),
        f32((full, 2, 2 * tiles, slots, LANES)),
        f32((devices, 2, slots, 2 * width_x)),
        f32(spec_shape),
        f32(spec_shape),
        f32((1, LANES)),
        dma((5,)),
        *[dma] * 6,
        dma((2,)),
        dma((group + 2 * REACH,)),
        *[dma] * 3,
        *[dma((2,))] * 4,
        *[dma] * 4,
    ]
    held = sum(math.prod(part.shape) for part in scratch if hasattr(part, "memory_space"))
    limit = max(VMEM_BYTES, min(VMEM_MOST, 8 * held))
    pieces = pl.pallas_call(
        functools.partial(mega_kernel, devices, group, half, places),
        out_shape=(
            jax.ShapeDtypeStruct((width_y, width_x), jnp.float32),
            jax.ShapeDtypeStruct((2, width_y, width_x), jnp.float32),
            jax.ShapeDtypeStruct((devices, 1, LANES), jnp.float32),
        ),
        in_specs=[HBM_SPEC] * 3,
        out_specs=(VMEM_SPEC,) * 3,
        scratch_shapes=scratch,
        compiler_params=pltpu.CompilerParams(
            collective_id=0, has_side_effects=True, vmem_limit_bytes=limit
        ),
        name="potential",
    )(density.reshape(2, width_y, width_x), kernel_hat, packed)
    potential, energies = pl.pallas_call(
        join_kernel,
        out_shape=(
            jax.ShapeDtypeStruct((2, width_y, width_x), jnp.float32),
            jax.ShapeDtypeStruct((2,), jnp.float32),
        ),
        in_specs=[VMEM_SPEC] * 3,
        out_specs=(VMEM_SPEC, pl.BlockSpec(memory_space=pltpu.SMEM)),
        compiler_params=pltpu.CompilerParams(vmem_limit_bytes=8 << 20),
        name="join",
    )(*pieces)
    return potential.reshape(density.shape), energies


def solution(mesh):
    placed = (P(None, "gz", None, None), P(None, "gz", None))
    return jax.shard_map(
        per_device,
        mesh=mesh,
        in_specs=placed,
        out_specs=(P(None, "gz", None, None), P()),
        check_vma=False,
    )
```
